8 devices in a mesh: grp: 1 (over z), comp: 2 (over y), row: 4 (over x, core).
Axes of the slice: x: 2, y: 2, z: 1, core: 2. Of those that a mesh axis runs over, the one named last changes fastest.
Arguments:
- points: bfloat16 [8192, 1024], P(('grp', 'row'))
- mu_init: float32 [2, 1024, 512], P(None, ('grp', 'comp'))
- logpi_init: float32 [2, 1024], P(None, ('grp', 'comp'))
- inv_temp: float32 [3], replicated
Outputs:
- output 1: float32 [2, 1024, 512], P(None, ('grp', 'comp'))
- output 2: float32 [2, 1024], P(None, ('grp', 'comp'))
- output 3: float32 [2, 8192], P(None, ('grp', 'row'))
All inputs are finite; a program needn't handle non-finite values.
Results may differ from the reference program's by a relative error of at most 0.001.
Values are sent between devices in bfloat16 or wider.
A program may use at most 1 GiB of HBM per device.

```python
import jax
import jax.numpy as jnp
from jax import lax

POINTS = 8192
DIM = 1024
HALF = 512
COMPS = 1024
SWEEPS = 3
CLUSTERS = 16
BLOCK = 256

EPS_COUNT = 1e-6
PRIOR_ALPHA = 1e-3


def setup_inputs(seed: int = 0, part: int = 0) -> dict:
    base_key = jax.random.key(seed)
    part_key = jax.random.fold_in(base_key, part)
    key_c, key_x, key_j, key_m, key_w = jax.random.split(part_key, 5)
    key_b = jax.random.fold_in(base_key, 1000)
    centers = jax.random.normal(key_c, (2, CLUSTERS, HALF), jnp.float32)
    source = (jnp.arange(POINTS) * CLUSTERS) // POINTS
    noise_x = jax.random.normal(key_x, (2, POINTS, HALF), jnp.float32)
    pts_pair = centers[:, source, :] + 0.7 * noise_x
    points = jnp.transpose(pts_pair, (1, 0, 2)).reshape(POINTS, DIM).astype(jnp.bfloat16)
    pick_ids = jax.random.randint(key_j, (2, COMPS), 0, CLUSTERS)
    noise_m = jax.random.normal(key_m, (2, COMPS, HALF), jnp.float32)
    mu_init = centers[jnp.arange(2)[:, None], pick_ids] + 0.5 * noise_m
    raw_logit = jax.random.normal(key_w, (2, COMPS), jnp.float32)
    logpi_init = raw_logit - jax.nn.logsumexp(raw_logit, axis=1, keepdims=True)
    inv_temp = (0.5 + 1.5 * jax.random.uniform(key_b, (SWEEPS,), jnp.float32)) / HALF
    return {"points": points, "mu_init": mu_init, "logpi_init": logpi_init, "inv_temp": inv_temp}


def reference(points, mu_init, logpi_init, inv_temp):
    x_blocks = points.astype(jnp.float32).reshape(POINTS // BLOCK, BLOCK, 2, HALF)
    x_blocks = jnp.transpose(x_blocks, (0, 2, 1, 3))
    sq_blocks = jnp.sum(x_blocks * x_blocks, axis=3)

    def one_sweep(carry_in, beta_t):
        mean_vecs, log_wts = carry_in
        mu_round = mean_vecs.astype(jnp.bfloat16).astype(jnp.float32)
        mu_sq = jnp.sum(mean_vecs * mean_vecs, axis=2)

        def point_block(acc_pair, block_in):
            x_block, sq_norm = block_in
            cross_dot = jnp.einsum("snh,skh->snk", x_block, mu_round)
            logits = log_wts[:, None, :] - beta_t * (sq_norm[:, :, None] - 2.0 * cross_dot + mu_sq[:, None, :])
            row_max = jnp.max(logits, axis=2)
            shifted = jnp.exp(logits - row_max[:, :, None])
            row_sum = jnp.sum(shifted, axis=2)
            resp_f = shifted / row_sum[:, :, None]
            log_norm = row_max + jnp.log(row_sum)
            resp_round = resp_f.astype(jnp.bfloat16).astype(jnp.float32)
            stat_part = jnp.einsum("snk,snh->skh", resp_round, x_block)
            count_acc, stat_acc = acc_pair
            return (count_acc + jnp.sum(resp_f, axis=1), stat_acc + stat_part), log_norm

        zero_acc = (jnp.zeros((2, COMPS), jnp.float32), jnp.zeros((2, COMPS, HALF), jnp.float32))
        (counts, stat_sum), norm_blocks = lax.scan(point_block, zero_acc, (x_blocks, sq_blocks))
        new_means = stat_sum / (counts[:, :, None] + EPS_COUNT)
        new_logw = jnp.log((counts + PRIOR_ALPHA) / (POINTS + COMPS * PRIOR_ALPHA))
        return (new_means, new_logw), norm_blocks

    (mean_vecs, log_wts), norm_all = lax.scan(one_sweep, (mu_init, logpi_init), inv_temp)
    log_norm = jnp.transpose(norm_all[-1], (1, 0, 2)).reshape(2, POINTS)
    return mean_vecs, log_wts, log_norm
```

```python
import jax
import jax.numpy as jnp
from jax import lax
from jax.experimental import pallas as pl
from jax.experimental.pallas import tpu as pltpu
from jax.sharding import PartitionSpec as P

EPS_COUNT = 1e-6
PRIOR_ALPHA = 1e-3

F32 = jnp.float32
BF16 = jnp.bfloat16
MESH = pl.DeviceIdType.MESH

SWEEPS = 3
HALF = 512
SHARD = 2048
ROWS = 8192
KC = 256
BLK = 256
NBLK = ROWS // BLK
GRP = 4
NGRP = NBLK // GRP
NCH = 16
Z = SHARD // 2 // NCH
OWN = 2 * SHARD
NQ = 4
QC = KC // NQ


def body(x_hbm, mu_hbm, lp_in, beta_ref,
         mu_out, lp_out, lse_out,
         xb, p_ref, rb, s_ref, nacc, mu_f, mu2, sqmu, lpb, sqx, lse_ref,
         st_own, st_rem, xin, lpbuf, lse_snd, lse_rcv,
         loc_sem, xs, xr, ys, yr, ds, dr, own_s, own_r,
         st_s, st_r, lps, lpr, ls_s, ls_r, fxs, fxr, fds, fdr, frs, frr, fl):
    comp = lax.axis_index("comp")
    row = lax.axis_index("row")
    side = row // 2
    core = row % 2
    sib = {"row": side * 2 + (1 - core)}
    ypt = {"comp": 1 - comp}
    ydg = {"comp": 1 - comp, "row": side * 2 + (1 - core)}
    xpt = {"row": (1 - side) * 2 + core}
    xdg = {"row": (1 - side) * 2 + (1 - core)}
    peers = (sib, ypt, ydg)

    barrier = pltpu.get_barrier_semaphore()
    for dev in (xpt, sib, ypt, ydg, xdg):
        pl.semaphore_signal(barrier, inc=1, device_id=dev, device_id_type=MESH)

    def remote(src, dst, ssem, rsem, dev):
        return pltpu.make_async_remote_copy(
            src_ref=src, dst_ref=dst, send_sem=ssem, recv_sem=rsem,
            device_id=dev, device_id_type=MESH)

    fit_cols = pl.ds(pl.multiple_of(side * HALF, HALF), HALF)
    oth_cols = pl.ds(pl.multiple_of((1 - side) * HALF, HALF), HALF)
    cbase = pl.multiple_of(core * KC, KC)

    def own_rows(c):
        return xb.at[pl.ds(pl.multiple_of(c * SHARD, SHARD), SHARD), :]

    ld_x = pltpu.make_async_copy(x_hbm.at[:, fit_cols], own_rows(core), loc_sem.at[0])
    ld_mu = pltpu.make_async_copy(mu_hbm.at[side, pl.ds(cbase, KC), :], mu_f, loc_sem.at[1])
    ld_mu.start()
    ld_x.start()

    def place(g, c, half, n):
        return xb.at[pl.ds(pl.multiple_of(OWN + g * (4 * Z) + c * (2 * Z) + half * Z, Z), n), :]

    def x_copy(g):
        src = x_hbm.at[pl.ds(pl.multiple_of(comp * (SHARD // 2) + g * Z, Z), Z), oth_cols]
        return remote(src, place(g, core, comp, Z), xs.at[g], xr.at[g], xpt)

    def y_copy(g):
        ref = place(g, core, comp, Z)
        return remote(ref, ref, ys.at[g], yr.at[g], ypt)

    def d_copy(g):
        ref = place(g, core, 0, 2 * Z)
        return remote(ref, ref, ds.at[g], dr.at[g], sib)

    own_copy = remote(x_hbm.at[:, fit_cols], own_rows(core), own_s, own_r, sib)

    pl.semaphore_wait(barrier, 5)
    own_copy.start()

    @pl.loop(0, NCH)
    def _(g):
        x_copy(g).start()

    def bc(row_vec):
        return jnp.transpose(jnp.broadcast_to(row_vec, (128, KC)))

    def set_means(mu):
        mu2[...] = mu.astype(BF16) * jnp.asarray(-2.0, BF16)
        sq = jnp.sum(mu * mu, axis=1, keepdims=True)
        sqmu[...] = jnp.broadcast_to(sq, (KC, 128))

    lpb[...] = bc(lp_in[pl.ds(side, 1), pl.ds(cbase, KC)])
    ld_mu.wait()
    set_means(mu_f[...])

    def point_sq(b):
        xf = xb[pl.ds(pl.multiple_of(b * BLK, BLK), BLK), :].astype(F32)
        sq = xf * xf
        part = (sq[:, 0:128] + sq[:, 128:256]) + (sq[:, 256:384] + sq[:, 384:512])
        rowv = jnp.sum(jnp.transpose(part), axis=0, keepdims=True)
        sqx[:, pl.ds(pl.multiple_of(b * BLK, BLK), BLK)] = rowv

    def estep(b, beta, par):
        xblk = xb[pl.ds(pl.multiple_of(b * BLK, BLK), BLK), :]
        a2 = lax.dot_general(mu2[...], xblk, (((1,), (1,)), ((), ())),
                             preferred_element_type=F32)
        sq = sqx[:, pl.ds(pl.multiple_of(b * BLK, BLK), BLK)]
        grp = b // GRP
        j = b % GRP
        for h in range(BLK // 128):
            cols = slice(h * 128, (h + 1) * 128)
            t = (a2[:, cols] + sq[:, cols]) + sqmu[...]
            logit = lpb[...] - beta * t
            m = jnp.max(logit, axis=0, keepdims=True)
            e = jnp.exp(logit - m)
            r = jnp.sum(e, axis=0, keepdims=True)
            p_ref[b, :, cols] = e
            st_own[par, grp, 0, j, :, cols] = m
            st_own[par, grp, 1, j, :, cols] = r

    def st_copy(grp, par, i):
        return remote(st_own.at[par, grp], st_rem.at[par, i, grp],
                      st_s.at[i, grp], st_r.at[par, i, grp], peers[i])

    def send_stats(grp, par):
        for i in range(3):
            st_copy(grp, par, i).start()

    def mstep(grp, par, first):
        for i in range(3):
            st_copy(grp, par, i).wait_recv()
            st_copy(grp, par, i).wait_send()
        st = [st_own[par, grp]] + [st_rem[par, i, grp] for i in range(3)]
        ms = [s[0] for s in st]
        rs = [s[1] for s in st]
        m = jnp.maximum(jnp.maximum(ms[0], ms[1]), jnp.maximum(ms[2], ms[3]))
        es = [jnp.exp(v - m) for v in ms]
        tot = (rs[0] * es[0] + rs[1] * es[1]) + (rs[2] * es[2] + rs[3] * es[3])
        scale = es[0] / tot
        lse = m + jnp.log(tot)
        cnt = None
        for j in range(GRP):
            lse_ref[:, pl.ds(pl.multiple_of((grp * GRP + j) * BLK, BLK), BLK)] = lse[j]
            rj = p_ref[grp * GRP + j] * scale[j]
            part = rj[:, 0:128] + rj[:, 128:256]
            cnt = part if cnt is None else cnt + part
            rb[:, j * BLK:(j + 1) * BLK] = rj.astype(BF16)
        nacc[...] += cnt
        rows = pl.ds(pl.multiple_of(grp * (GRP * BLK), GRP * BLK), GRP * BLK)
        s_ref[...] += jnp.dot(rb[...], xb[rows, :], preferred_element_type=F32)

    def zero_sums():
        nacc[...] = jnp.zeros_like(nacc)
        s_ref[...] = jnp.zeros_like(s_ref)

    def finish_sweep():
        n = jnp.sum(nacc[...], axis=1, keepdims=True)
        mu = s_ref[...] / (n + EPS_COUNT)
        mu_f[...] = mu
        lp = jnp.log((n + PRIOR_ALPHA) / (ROWS + 4 * KC * PRIOR_ALPHA))
        lpb[...] = jnp.broadcast_to(lp, (KC, 128))
        set_means(mu)

    zero_sums()
    beta0 = beta_ref[0]

    def first_blocks(c):
        @pl.loop(0, SHARD // BLK)
        def _(k):
            b = c * (SHARD // BLK) + k
            point_sq(b)
            estep(b, beta0, 0)

            @pl.when(k % GRP == GRP - 1)
            def _():
                send_stats(b // GRP, 0)

    ld_x.wait()
    first_blocks(core)
    own_copy.wait_recv()
    first_blocks(1 - core)

    @pl.loop(0, NCH + 4)
    def _(it):
        @pl.when(it < NCH)
        def _():
            x_copy(it).wait_recv()
            y_copy(it).start()

        @pl.when((it >= 3) & (it < NCH + 3))
        def _():
            y_copy(it - 3).wait_recv()
            d_copy(it - 3).start()

        @pl.when(it >= 4)
        def _():
            d_copy(it - 4).wait_recv()
            b = NBLK // 2 + it - 4
            point_sq(b)
            estep(b, beta0, 0)

            @pl.when(it % GRP == GRP - 1)
            def _():
                send_stats(b // GRP, 0)

        @pl.when((it < NCH) & (it % 4 == 2))
        def _():
            mstep(it // 4, 0, True)

        @pl.when((it >= 9) & (it % 4 == 1))
        def _():
            mstep(NGRP // 2 + (it - 9) // 4, 0, True)

    mstep(NGRP - 1, 0, True)
    finish_sweep()
    own_copy.wait_send()

    @pl.loop(0, NCH)
    def _(g):
        x_copy(g).wait_send()
        y_copy(g).wait_send()
        d_copy(g).wait_send()

    @pl.loop(1, SWEEPS)
    def _(t):
        par = t % 2
        beta = beta_ref[t]
        zero_sums()

        @pl.loop(0, NBLK)
        def _(b):
            estep(b, beta, par)

            @pl.when(b % GRP == GRP - 1)
            def _():
                send_stats(b // GRP, par)

        @pl.loop(0, NGRP)
        def _(grp):
            mstep(grp, par, False)

        finish_sweep()

    def fx_copy(q):
        rows = pl.ds(q * QC, QC)
        return remote(mu_f.at[rows, :], xin.at[rows, :], fxs.at[q], fxr.at[q], xpt)

    def out_rows(s, q, n):
        return mu_out.at[s, pl.ds(cbase + q * QC, n), :]

    def relay(q):
        return remote(xin.at[pl.ds(q * QC, QC), :], out_rows(1 - side, q, QC),
                      frs.at[q], frr.at[q], sib)

    def keep(q):
        return pltpu.make_async_copy(xin.at[pl.ds(q * QC, QC), :], out_rows(1 - side, q, QC),
                                     fl.at[1 + q])

    for q in range(NQ):
        fx_copy(q).start()
    to_sib = remote(mu_f, out_rows(side, 0, KC), fds, fdr, sib)
    to_sib.start()
    mine = pltpu.make_async_copy(mu_f, out_rows(side, 0, KC), fl.at[0])
    mine.start()

    slot = side * 2 + core
    lp_row = jnp.transpose(lpb[...])[0:1, :]
    lpbuf[slot] = lp_row
    lp_devs = (sib, xpt, xdg)

    def lp_copy(i):
        return remote(lpbuf.at[slot], lpbuf.at[slot], lps.at[i], lpr.at[i], lp_devs[i])

    halves = ([], [])
    for g in range(NCH):
        piece = lse_ref[:, pl.ds(pl.multiple_of(OWN + g * (4 * Z) + core * (2 * Z), 128), 128)]
        halves[0].append(piece[:, 0:Z])
        halves[1].append(piece[:, Z:2 * Z])
    lse_snd[...] = jnp.concatenate(halves[0] + halves[1], axis=1)
    lse_out[pl.ds(side, 1), :] = lse_ref[:, pl.ds(pl.multiple_of(core * SHARD, SHARD), SHARD)]
    lse_copy = remote(lse_snd, lse_rcv, ls_s, ls_r, xpt)
    lse_copy.start()
    for i in range(3):
        lp_copy(i).start()

    for q in range(NQ):
        fx_copy(q).wait_recv()
        relay(q).start()
        keep(q).start()

    lse_copy.wait()
    lse_out[pl.ds(1 - side, 1), :] = lse_rcv[...]
    for i in range(3):
        lp_copy(i).wait()
    for s in range(2):
        for c in range(2):
            lp_out[s:s + 1, c * KC:(c + 1) * KC] = lpbuf[s * 2 + c]
    mine.wait()
    to_sib.wait()
    for q in range(NQ):
        keep(q).wait()
        relay(q).wait()
        fx_copy(q).wait_send()


def solution(mesh):
    def local_fit(x_local, mu_init, logpi_init, inv_temp):
        dma = pltpu.SemaphoreType.DMA
        vmem = pl.BlockSpec(memory_space=pltpu.VMEM)
        hbm = pl.BlockSpec(memory_space=pl.ANY)
        return pl.pallas_call(
            body,
            out_shape=(
                jax.ShapeDtypeStruct(mu_init.shape, F32),
                jax.ShapeDtypeStruct(logpi_init.shape, F32),
                jax.ShapeDtypeStruct((2, x_local.shape[0]), F32),
            ),
            in_specs=[hbm, hbm, vmem, pl.BlockSpec(memory_space=pltpu.SMEM)],
            out_specs=(hbm, vmem, vmem),
            scratch_shapes=[
                pltpu.VMEM((ROWS, HALF), BF16),
                pltpu.VMEM((NBLK, KC, BLK), F32),
                pltpu.VMEM((KC, GRP * BLK), BF16),
                pltpu.VMEM((KC, HALF), F32),
                pltpu.VMEM((KC, 128), F32),
                pltpu.VMEM((KC, HALF), F32),
                pltpu.VMEM((KC, HALF), BF16),
                pltpu.VMEM((KC, 128), F32),
                pltpu.VMEM((KC, 128), F32),
                pltpu.VMEM((1, ROWS), F32),
                pltpu.VMEM((1, ROWS), F32),
                pltpu.VMEM((2, NGRP, 2, GRP, 1, BLK), F32),
                pltpu.VMEM((2, 3, NGRP, 2, GRP, 1, BLK), F32),
                pltpu.VMEM((KC, HALF), F32),
                pltpu.VMEM((4, 1, KC), F32),
                pltpu.VMEM((1, SHARD), F32),
                pltpu.VMEM((1, SHARD), F32),
                dma((2,)),
                dma((NCH,)), dma((NCH,)),
                dma((NCH,)), dma((NCH,)),
                dma((NCH,)), dma((NCH,)),
                dma, dma,
                dma((3, NGRP)), dma((2, 3, NGRP)),
                dma((3,)), dma((3,)),
                dma, dma,
                dma((NQ,)), dma((NQ,)),
                dma, dma,
                dma((NQ,)), dma((NQ,)),
                dma((NQ + 1,)),
            ],
            compiler_params=pltpu.CompilerParams(
                collective_id=0, has_side_effects=True,
                vmem_limit_bytes=56 * 1024 * 1024),
        )(x_local, mu_init, logpi_init, inv_temp)

    return jax.shard_map(
        local_fit,
        mesh=mesh,
        in_specs=(P(("grp", "row"), None), P(None, ("grp", "comp"), None), P(None, ("grp", "comp")), P()),
        out_specs=(P(None, ("grp", "comp"), None), P(None, ("grp", "comp")), P(None, ("grp", "row"))),
        check_vma=False,
    )
```

```python
import jax
import jax.numpy as jnp
from jax import lax
from jax.experimental import pallas as pl
from jax.experimental.pallas import tpu as pltpu
from jax.sharding import PartitionSpec as P

EPS_COUNT = 1e-6
PRIOR_ALPHA = 1e-3

F32 = jnp.float32
BF16 = jnp.bfloat16
MESH = pl.DeviceIdType.MESH

SWEEPS = 3
HALF = 512
SHARD = 2048
ROWS = 8192
KC = 256
BLK = 256
NBLK = ROWS // BLK
GRP = 4
NGRP = NBLK // GRP
NCH = 16
Z = SHARD // 2 // NCH
NOWN = 4
PIECE = SHARD // NOWN
OWN = 2 * SHARD
NQ = 4
QC = KC // NQ


def body(x_hbm, mu_hbm, lp_in, beta_ref,
         mu_out, lp_out, lse_out,
         xb, xt_ref, p_ref, a0, a1, rb0, rb1, s_ref, nacc, mu_f, mu2, sqmu, lpb, sqx, lse_ref,
         st_own, st_rem, xin, lpbuf, lse_snd, lse_rcv,
         loc_sem, xs, xr, ys, yr, ds, dr, own_s, own_r,
         st_s, st_r, lps, lpr, ls_s, ls_r, fxs, fxr, fds, fdr, frs, frr, fl):
    comp = lax.axis_index("comp")
    row = lax.axis_index("row")
    side = row // 2
    core = row % 2
    sib = {"row": side * 2 + (1 - core)}
    ypt = {"comp": 1 - comp}
    ydg = {"comp": 1 - comp, "row": side * 2 + (1 - core)}
    xpt = {"row": (1 - side) * 2 + core}
    xdg = {"row": (1 - side) * 2 + (1 - core)}
    peers = (sib, ypt, ydg)

    barrier = pltpu.get_barrier_semaphore()
    for dev in (xpt, sib, ypt, ydg, xdg):
        pl.semaphore_signal(barrier, inc=1, device_id=dev, device_id_type=MESH)

    def remote(src, dst, ssem, rsem, dev):
        return pltpu.make_async_remote_copy(
            src_ref=src, dst_ref=dst, send_sem=ssem, recv_sem=rsem,
            device_id=dev, device_id_type=MESH)

    fit_cols = pl.ds(pl.multiple_of(side * HALF, HALF), HALF)
    oth_cols = pl.ds(pl.multiple_of((1 - side) * HALF, HALF), HALF)
    cbase = pl.multiple_of(core * KC, KC)

    def own_rows(c):
        return xb.at[pl.ds(pl.multiple_of(c * SHARD, SHARD), SHARD), :]

    ld_x = pltpu.make_async_copy(x_hbm.at[:, fit_cols], own_rows(core), loc_sem.at[0])
    ld_mu = pltpu.make_async_copy(mu_hbm.at[side, pl.ds(cbase, KC), :], mu_f, loc_sem.at[1])
    ld_mu.start()
    ld_x.start()

    def place(g, c, half, n):
        return xb.at[pl.ds(pl.multiple_of(OWN + g * (4 * Z) + c * (2 * Z) + half * Z, Z), n), :]

    def x_copy(g):
        src = x_hbm.at[pl.ds(pl.multiple_of(comp * (SHARD // 2) + g * Z, Z), Z), oth_cols]
        return remote(src, place(g, core, comp, Z), xs.at[g], xr.at[g], xpt)

    def y_copy(g):
        ref = place(g, core, comp, Z)
        return remote(ref, ref, ys.at[g], yr.at[g], ypt)

    def d_copy(g):
        ref = place(g, core, 0, 2 * Z)
        return remote(ref, ref, ds.at[g], dr.at[g], sib)

    def own_copy(k):
        src = x_hbm.at[pl.ds(pl.multiple_of(k * PIECE, PIECE), PIECE), fit_cols]
        dst = xb.at[pl.ds(pl.multiple_of(core * SHARD + k * PIECE, PIECE), PIECE), :]
        return remote(src, dst, own_s.at[k], own_r.at[k], sib)

    pl.semaphore_wait(barrier, 5)
    for k in range(NOWN):
        own_copy(k).start()

    @pl.loop(0, NCH)
    def _(g):
        x_copy(g).start()

    def bc(row_vec):
        return jnp.transpose(jnp.broadcast_to(row_vec, (128, KC)))

    def set_means(mu):
        mu2[...] = mu.astype(BF16) * jnp.asarray(-2.0, BF16)
        sq = jnp.sum(mu * mu, axis=1, keepdims=True)
        sqmu[...] = jnp.broadcast_to(sq, (KC, 128))

    lpb[...] = bc(lp_in[pl.ds(side, 1), pl.ds(cbase, KC)])
    ld_mu.wait()
    set_means(mu_f[...])

    def prep(b):
        xt = jnp.transpose(xb[pl.ds(pl.multiple_of(b * BLK, BLK), BLK), :])
        xt_ref[b] = xt
        xf = xt.astype(F32)
        sqx[b] = jnp.sum(xf * xf, axis=0, keepdims=True)

    def cross(b, a_ref):
        a_ref[...] = jnp.dot(mu2[...], xt_ref[b], preferred_element_type=F32)

    def soft(b, a_ref, beta, par):
        sq = sqx[b]
        grp = b // GRP
        j = b % GRP
        for h in range(BLK // 128):
            cols = slice(h * 128, (h + 1) * 128)
            t = (a_ref[:, cols] + sq[:, cols]) + sqmu[...]
            logit = lpb[...] - beta * t
            m = jnp.max(logit, axis=0, keepdims=True)
            e = jnp.exp(logit - m)
            r = jnp.sum(e, axis=0, keepdims=True)
            p_ref[b, :, cols] = e
            st_own[par, grp, 0, j, :, cols] = m
            st_own[par, grp, 1, j, :, cols] = r

    def st_copy(grp, par, i):
        return remote(st_own.at[par, grp], st_rem.at[par, i, grp],
                      st_s.at[i, grp], st_r.at[par, i, grp], peers[i])

    def send_stats(grp, par):
        for i in range(3):
            st_copy(grp, par, i).start()

    def wait_stats(grp, par):
        for i in range(3):
            st_copy(grp, par, i).wait_recv()
            st_copy(grp, par, i).wait_send()

    def resp(grp, par, rb):
        st = [st_own[par, grp]] + [st_rem[par, i, grp] for i in range(3)]
        ms = [s[0] for s in st]
        rs = [s[1] for s in st]
        m = jnp.maximum(jnp.maximum(ms[0], ms[1]), jnp.maximum(ms[2], ms[3]))
        es = [jnp.exp(v - m) for v in ms]
        tot = (rs[0] * es[0] + rs[1] * es[1]) + (rs[2] * es[2] + rs[3] * es[3])
        scale = es[0] / tot
        lse = m + jnp.log(tot)
        cnt = nacc[...]
        for j in range(GRP):
            lse_ref[:, pl.ds(pl.multiple_of((grp * GRP + j) * BLK, BLK), BLK)] = lse[j]
            rj = p_ref[grp * GRP + j] * scale[j]
            cnt = cnt + (rj[:, 0:128] + rj[:, 128:256])
            rb[:, j * BLK:(j + 1) * BLK] = rj.astype(BF16)
        nacc[...] = cnt

    def gather(grp, rb):
        rows = pl.ds(pl.multiple_of(grp * (GRP * BLK), GRP * BLK), GRP * BLK)
        s_ref[...] += jnp.dot(rb[...], xb[rows, :], preferred_element_type=F32)

    def mstep(grp, par):
        wait_stats(grp, par)
        resp(grp, par, rb0)
        gather(grp, rb0)

    def zero_sums():
        nacc[...] = jnp.zeros_like(nacc)
        s_ref[...] = jnp.zeros_like(s_ref)

    def finish_sweep():
        n = jnp.sum(nacc[...], axis=1, keepdims=True)
        mu = s_ref[...] / (n + EPS_COUNT)
        mu_f[...] = mu
        lp = jnp.log((n + PRIOR_ALPHA) / (ROWS + 4 * KC * PRIOR_ALPHA))
        lpb[...] = jnp.broadcast_to(lp, (KC, 128))
        set_means(mu)

    zero_sums()
    beta0 = beta_ref[0]

    def first_block(b):
        prep(b)
        cross(b, a0)
        soft(b, a0, beta0, 0)

        @pl.when(b % GRP == GRP - 1)
        def _():
            send_stats(b // GRP, 0)

    ld_x.wait()

    @pl.loop(0, NCH + 4)
    def _(it):
        @pl.when(it < NCH)
        def _():
            x_copy(it).wait_recv()
            y_copy(it).start()

        @pl.when((it >= 3) & (it < NCH + 3))
        def _():
            y_copy(it - 3).wait_recv()
            d_copy(it - 3).start()

        @pl.when((it < NCH) & (it // 8 != core) & (it % 2 == 0))
        def _():
            own_copy((it % 8) // 2).wait_recv()

        @pl.when(it < NCH)
        def _():
            first_block(it)

        @pl.when(it >= 4)
        def _():
            d_copy(it - 4).wait_recv()
            first_block(NBLK // 2 + it - 4)

        @pl.when((it >= 6) & (it % 4 == 2))
        def _():
            mstep((it - 6) // 4, 0)

        @pl.when((it >= 9) & (it % 4 == 1))
        def _():
            mstep(NGRP // 2 + (it - 9) // 4, 0)

    mstep(NGRP - 1, 0)
    finish_sweep()
    for k in range(NOWN):
        own_copy(k).wait_send()

    @pl.loop(0, NCH)
    def _(g):
        x_copy(g).wait_send()
        y_copy(g).wait_send()
        d_copy(g).wait_send()

    @pl.loop(1, SWEEPS)
    def _(t):
        par = t % 2
        beta = beta_ref[t]
        zero_sums()
        cross(0, a0)

        @pl.loop(0, NBLK // 2)
        def _(i):
            b = 2 * i
            cross(b + 1, a1)
            soft(b, a0, beta, par)
            cross((b + 2) % NBLK, a0)
            soft(b + 1, a1, beta, par)

            @pl.when(i % 2 == 1)
            def _():
                send_stats(i // 2, par)

        wait_stats(0, par)
        resp(0, par, rb0)

        @pl.loop(0, NGRP // 2 - 1)
        def _(i):
            g = 2 * i
            wait_stats(g + 1, par)
            resp(g + 1, par, rb1)
            gather(g, rb0)
            wait_stats(g + 2, par)
            resp(g + 2, par, rb0)
            gather(g + 1, rb1)

        wait_stats(NGRP - 1, par)
        resp(NGRP - 1, par, rb1)
        gather(NGRP - 2, rb0)
        gather(NGRP - 1, rb1)
        finish_sweep()

    def fx_copy(q):
        rows = pl.ds(q * QC, QC)
        return remote(mu_f.at[rows, :], xin.at[rows, :], fxs.at[q], fxr.at[q], xpt)

    def out_rows(s, q, n):
        return mu_out.at[s, pl.ds(cbase + q * QC, n), :]

    def relay(q):
        return remote(xin.at[pl.ds(q * QC, QC), :], out_rows(1 - side, q, QC),
                      frs.at[q], frr.at[q], sib)

    def keep(q):
        return pltpu.make_async_copy(xin.at[pl.ds(q * QC, QC), :], out_rows(1 - side, q, QC),
                                     fl.at[1 + q])

    for q in range(NQ):
        fx_copy(q).start()
    to_sib = remote(mu_f, out_rows(side, 0, KC), fds, fdr, sib)
    to_sib.start()
    mine = pltpu.make_async_copy(mu_f, out_rows(side, 0, KC), fl.at[0])
    mine.start()

    slot = side * 2 + core
    lp_row = jnp.transpose(lpb[...])[0:1, :]
    lpbuf[slot] = lp_row
    lp_devs = (sib, xpt, xdg)

    def lp_copy(i):
        return remote(lpbuf.at[slot], lpbuf.at[slot], lps.at[i], lpr.at[i], lp_devs[i])

    halves = ([], [])
    for g in range(NCH):
        piece = lse_ref[:, pl.ds(pl.multiple_of(OWN + g * (4 * Z) + core * (2 * Z), 128), 128)]
        halves[0].append(piece[:, 0:Z])
        halves[1].append(piece[:, Z:2 * Z])
    lse_snd[...] = jnp.concatenate(halves[0] + halves[1], axis=1)
    lse_out[pl.ds(side, 1), :] = lse_ref[:, pl.ds(pl.multiple_of(core * SHARD, SHARD), SHARD)]
    lse_copy = remote(lse_snd, lse_rcv, ls_s, ls_r, xpt)
    lse_copy.start()
    for i in range(3):
        lp_copy(i).start()

    for q in range(NQ):
        fx_copy(q).wait_recv()
        relay(q).start()
        keep(q).start()

    lse_copy.wait()
    lse_out[pl.ds(1 - side, 1), :] = lse_rcv[...]
    for i in range(3):
        lp_copy(i).wait()
    for s in range(2):
        for c in range(2):
            lp_out[s:s + 1, c * KC:(c + 1) * KC] = lpbuf[s * 2 + c]
    mine.wait()
    to_sib.wait()
    for q in range(NQ):
        keep(q).wait()
        relay(q).wait()
        fx_copy(q).wait_send()


def solution(mesh):
    def local_fit(x_local, mu_init, logpi_init, inv_temp):
        dma = pltpu.SemaphoreType.DMA
        vmem = pl.BlockSpec(memory_space=pltpu.VMEM)
        hbm = pl.BlockSpec(memory_space=pl.ANY)
        return pl.pallas_call(
            body,
            out_shape=(
                jax.ShapeDtypeStruct(mu_init.shape, F32),
                jax.ShapeDtypeStruct(logpi_init.shape, F32),
                jax.ShapeDtypeStruct((2, x_local.shape[0]), F32),
            ),
            in_specs=[hbm, hbm, vmem, pl.BlockSpec(memory_space=pltpu.SMEM)],
            out_specs=(hbm, vmem, vmem),
            scratch_shapes=[
                pltpu.VMEM((ROWS, HALF), BF16),
                pltpu.VMEM((NBLK, HALF, BLK), BF16),
                pltpu.VMEM((NBLK, KC, BLK), F32),
                pltpu.VMEM((KC, BLK), F32), pltpu.VMEM((KC, BLK), F32),
                pltpu.VMEM((KC, GRP * BLK), BF16),
                pltpu.VMEM((KC, GRP * BLK), BF16),
                pltpu.VMEM((KC, HALF), F32),
                pltpu.VMEM((KC, 128), F32),
                pltpu.VMEM((KC, HALF), F32),
                pltpu.VMEM((KC, HALF), BF16),
                pltpu.VMEM((KC, 128), F32),
                pltpu.VMEM((KC, 128), F32),
                pltpu.VMEM((NBLK, 1, BLK), F32),
                pltpu.VMEM((1, ROWS), F32),
                pltpu.VMEM((2, NGRP, 2, GRP, 1, BLK), F32),
                pltpu.VMEM((2, 3, NGRP, 2, GRP, 1, BLK), F32),
                pltpu.VMEM((KC, HALF), F32),
                pltpu.VMEM((4, 1, KC), F32),
                pltpu.VMEM((1, SHARD), F32),
                pltpu.VMEM((1, SHARD), F32),
                dma((2,)),
                dma((NCH,)), dma((NCH,)),
                dma((NCH,)), dma((NCH,)),
                dma((NCH,)), dma((NCH,)),
                dma((NOWN,)), dma((NOWN,)),
                dma((3, NGRP)), dma((2, 3, NGRP)),
                dma((3,)), dma((3,)),
                dma, dma,
                dma((NQ,)), dma((NQ,)),
                dma, dma,
                dma((NQ,)), dma((NQ,)),
                dma((NQ + 1,)),
            ],
            compiler_params=pltpu.CompilerParams(
                collective_id=0, has_side_effects=True,
                vmem_limit_bytes=56 * 1024 * 1024),
        )(x_local, mu_init, logpi_init, inv_temp)

    return jax.shard_map(
        local_fit,
        mesh=mesh,
        in_specs=(P(("grp", "row"), None), P(None, ("grp", "comp"), None), P(None, ("grp", "comp")), P()),
        out_specs=(P(None, ("grp", "comp"), None), P(None, ("grp", "comp")), P(None, ("grp", "row"))),
        check_vma=False,
    )
```

```python
import jax
import jax.numpy as jnp
from jax import lax
from jax.experimental import pallas as pl
from jax.experimental.pallas import tpu as pltpu
from jax.sharding import PartitionSpec as P

EPS_COUNT = 1e-6
PRIOR_ALPHA = 1e-3

F32 = jnp.float32
BF16 = jnp.bfloat16
MESH = pl.DeviceIdType.MESH

SWEEPS = 3
HALF = 512
SHARD = 2048
ROWS = 8192
KC = 256
BLK = 256
NBLK = ROWS // BLK
GRP = 4
NGRP = NBLK // GRP
NCH = 16
Z = SHARD // 2 // NCH
NOWN = 4
PIECE = SHARD // NOWN
OWN = 2 * SHARD
NQ = 4
QC = KC // NQ


def body(x_hbm, mu_hbm, lp_in, beta_ref,
         mu_out, lp_out, lse_out,
         xb, xt_ref, p_ref, a0, a1, rb0, rb1, s_ref, nacc, mu_f, mu2, sqmu, lpb, sqx, lse_ref,
         st_own, st_rem, lpbuf, lse_snd, lse_rcv,
         loc_sem, xs, xr, ys, yr, ds, dr, own_s, own_r,
         st_s, st_r, lps, lpr, ls_s, ls_r, fxs, fxr, fds, fdr, frs, frr):
    comp = lax.axis_index("comp")
    row = lax.axis_index("row")
    side = row // 2
    core = row % 2
    sib = {"row": side * 2 + (1 - core)}
    ypt = {"comp": 1 - comp}
    ydg = {"comp": 1 - comp, "row": side * 2 + (1 - core)}
    xpt = {"row": (1 - side) * 2 + core}
    xdg = {"row": (1 - side) * 2 + (1 - core)}
    peers = (sib, ypt, ydg)

    barrier = pltpu.get_barrier_semaphore()
    for dev in (xpt, sib, ypt, ydg, xdg):
        pl.semaphore_signal(barrier, inc=1, device_id=dev, device_id_type=MESH)

    def remote(src, dst, ssem, rsem, dev):
        return pltpu.make_async_remote_copy(
            src_ref=src, dst_ref=dst, send_sem=ssem, recv_sem=rsem,
            device_id=dev, device_id_type=MESH)

    fit_cols = pl.ds(pl.multiple_of(side * HALF, HALF), HALF)
    oth_cols = pl.ds(pl.multiple_of((1 - side) * HALF, HALF), HALF)
    cbase = pl.multiple_of(core * KC, KC)

    def own_rows(c):
        return xb.at[pl.ds(pl.multiple_of(c * SHARD, SHARD), SHARD), :]

    ld_x = pltpu.make_async_copy(x_hbm.at[:, fit_cols], own_rows(core), loc_sem.at[0])
    ld_mu = pltpu.make_async_copy(mu_hbm.at[side, pl.ds(cbase, KC), :], mu_f, loc_sem.at[1])
    ld_mu.start()
    ld_x.start()

    def place(g, c, half, n):
        return xb.at[pl.ds(pl.multiple_of(OWN + g * (4 * Z) + c * (2 * Z) + half * Z, Z), n), :]

    def x_copy(g):
        src = x_hbm.at[pl.ds(pl.multiple_of(comp * (SHARD // 2) + g * Z, Z), Z), oth_cols]
        return remote(src, place(g, core, comp, Z), xs.at[g], xr.at[g], xpt)

    def y_copy(g):
        ref = place(g, core, comp, Z)
        return remote(ref, ref, ys.at[g], yr.at[g], ypt)

    def d_copy(g):
        ref = place(g, core, 0, 2 * Z)
        return remote(ref, ref, ds.at[g], dr.at[g], sib)

    def own_copy(k):
        src = x_hbm.at[pl.ds(pl.multiple_of(k * PIECE, PIECE), PIECE), fit_cols]
        dst = xb.at[pl.ds(pl.multiple_of(core * SHARD + k * PIECE, PIECE), PIECE), :]
        return remote(src, dst, own_s.at[k], own_r.at[k], sib)

    pl.semaphore_wait(barrier, 5)
    for k in range(NOWN):
        own_copy(k).start()

    @pl.loop(0, NCH)
    def _(g):
        x_copy(g).start()

    def bc(row_vec):
        return jnp.transpose(jnp.broadcast_to(row_vec, (128, KC)))

    def set_means(mu):
        mu2[...] = mu.astype(BF16) * jnp.asarray(-2.0, BF16)
        sq = jnp.sum(mu * mu, axis=1, keepdims=True)
        sqmu[...] = jnp.broadcast_to(sq, (KC, 128))

    lpb[...] = bc(lp_in[pl.ds(side, 1), pl.ds(cbase, KC)])
    ld_mu.wait()
    set_means(mu_f[...])

    def prep(b):
        xt = jnp.transpose(xb[pl.ds(pl.multiple_of(b * BLK, BLK), BLK), :])
        xt_ref[b] = xt
        xf = xt.astype(F32)
        sqx[b] = jnp.sum(xf * xf, axis=0, keepdims=True)

    def cross(b, a_ref):
        a_ref[...] = jnp.dot(mu2[...], xt_ref[b], preferred_element_type=F32)

    def soft(b, a_ref, beta, par):
        sq = sqx[b]
        grp = b // GRP
        j = b % GRP
        for h in range(BLK // 128):
            cols = slice(h * 128, (h + 1) * 128)
            t = (a_ref[:, cols] + sq[:, cols]) + sqmu[...]
            logit = lpb[...] - beta * t
            m = jnp.max(logit, axis=0, keepdims=True)
            e = jnp.exp(logit - m)
            r = jnp.sum(e, axis=0, keepdims=True)
            p_ref[b, :, cols] = e
            st_own[par, grp, 0, j, :, cols] = m
            st_own[par, grp, 1, j, :, cols] = r

    def st_copy(grp, par, i):
        return remote(st_own.at[par, grp], st_rem.at[par, i, grp],
                      st_s.at[i, grp], st_r.at[par, i, grp], peers[i])

    def send_stats(grp, par):
        for i in range(3):
            st_copy(grp, par, i).start()

    def wait_stats(grp, par):
        for i in range(3):
            st_copy(grp, par, i).wait_recv()
            st_copy(grp, par, i).wait_send()

    def resp(grp, par, rb):
        st = [st_own[par, grp]] + [st_rem[par, i, grp] for i in range(3)]
        ms = [s[0] for s in st]
        rs = [s[1] for s in st]
        m = jnp.maximum(jnp.maximum(ms[0], ms[1]), jnp.maximum(ms[2], ms[3]))
        es = [jnp.exp(v - m) for v in ms]
        tot = (rs[0] * es[0] + rs[1] * es[1]) + (rs[2] * es[2] + rs[3] * es[3])
        scale = es[0] / tot
        lse = m + jnp.log(tot)
        cnt = nacc[...]
        for j in range(GRP):
            lse_ref[:, pl.ds(pl.multiple_of((grp * GRP + j) * BLK, BLK), BLK)] = lse[j]
            rj = p_ref[grp * GRP + j] * scale[j]
            cnt = cnt + (rj[:, 0:128] + rj[:, 128:256])
            rb[:, j * BLK:(j + 1) * BLK] = rj.astype(BF16)
        nacc[...] = cnt

    def gather(grp, rb):
        rows = pl.ds(pl.multiple_of(grp * (GRP * BLK), GRP * BLK), GRP * BLK)
        s_ref[...] += jnp.dot(rb[...], xb[rows, :], preferred_element_type=F32)

    def mstep(grp, par):
        wait_stats(grp, par)
        resp(grp, par, rb0)
        gather(grp, rb0)

    def zero_sums():
        nacc[...] = jnp.zeros_like(nacc)
        s_ref[...] = jnp.zeros_like(s_ref)

    def finish_sweep():
        n = jnp.sum(nacc[...], axis=1, keepdims=True)
        mu = s_ref[...] / (n + EPS_COUNT)
        mu_f[...] = mu
        lp = jnp.log((n + PRIOR_ALPHA) / (ROWS + 4 * KC * PRIOR_ALPHA))
        lpb[...] = jnp.broadcast_to(lp, (KC, 128))
        set_means(mu)

    zero_sums()
    beta0 = beta_ref[0]

    def first_block(b):
        prep(b)
        cross(b, a0)
        soft(b, a0, beta0, 0)

        @pl.when(b % GRP == GRP - 1)
        def _():
            send_stats(b // GRP, 0)

    ld_x.wait()

    @pl.loop(0, NCH + 4)
    def _(it):
        @pl.when(it < NCH)
        def _():
            x_copy(it).wait_recv()
            y_copy(it).start()

        @pl.when((it >= 3) & (it < NCH + 3))
        def _():
            y_copy(it - 3).wait_recv()
            d_copy(it - 3).start()

        @pl.when((it < NCH) & (it // 8 != core) & (it % 2 == 0))
        def _():
            own_copy((it % 8) // 2).wait_recv()

        @pl.when(it < NCH)
        def _():
            first_block(it)

        @pl.when(it >= 4)
        def _():
            d_copy(it - 4).wait_recv()
            first_block(NBLK // 2 + it - 4)

        @pl.when((it >= 10) & (it % 4 == 2))
        def _():
            mstep((it - 10) // 4, 0)

        @pl.when((it >= 13) & (it % 4 == 1))
        def _():
            mstep(NGRP // 2 + (it - 13) // 4, 0)

    mstep(NGRP // 2 - 1, 0)
    mstep(NGRP - 2, 0)
    mstep(NGRP - 1, 0)
    finish_sweep()
    for k in range(NOWN):
        own_copy(k).wait_send()

    @pl.loop(0, NCH)
    def _(g):
        x_copy(g).wait_send()
        y_copy(g).wait_send()
        d_copy(g).wait_send()

    @pl.loop(1, SWEEPS)
    def _(t):
        par = t % 2
        beta = beta_ref[t]
        zero_sums()
        cross(0, a0)

        @pl.loop(0, NBLK // 2)
        def _(i):
            b = 2 * i
            cross(b + 1, a1)
            soft(b, a0, beta, par)
            cross((b + 2) % NBLK, a0)
            soft(b + 1, a1, beta, par)

            @pl.when(i % 2 == 1)
            def _():
                send_stats(i // 2, par)

        wait_stats(0, par)
        resp(0, par, rb0)

        @pl.loop(0, NGRP // 2 - 1)
        def _(i):
            g = 2 * i
            wait_stats(g + 1, par)
            resp(g + 1, par, rb1)
            gather(g, rb0)
            wait_stats(g + 2, par)
            resp(g + 2, par, rb0)
            gather(g + 1, rb1)

        wait_stats(NGRP - 1, par)
        resp(NGRP - 1, par, rb1)
        gather(NGRP - 2, rb0)
        gather(NGRP - 1, rb1)
        finish_sweep()

    def block(s, q, n):
        return mu_out.at[s, pl.ds(cbase + q * QC, n), :]

    def fx_copy(q):
        ref = block(side, q, QC)
        return remote(ref, ref, fxs.at[q], fxr.at[q], xpt)

    def relay(q):
        ref = block(1 - side, q, QC)
        return remote(ref, ref, frs.at[q], frr.at[q], sib)

    mu_out[side, pl.ds(cbase, KC), :] = mu_f[...]
    to_sib = remote(block(side, 0, KC), block(side, 0, KC), fds, fdr, sib)

    slot = side * 2 + core
    lpbuf[slot] = jnp.transpose(lpb[...])[0:1, :]
    lp_devs = (sib, xpt, xdg)

    def lp_copy(i):
        return remote(lpbuf.at[slot], lpbuf.at[slot], lps.at[i], lpr.at[i], lp_devs[i])

    for q in range(NQ):
        fx_copy(q).start()
    to_sib.start()

    halves = ([], [])
    for g in range(NCH):
        piece = lse_ref[:, pl.ds(pl.multiple_of(OWN + g * (4 * Z) + core * (2 * Z), 128), 128)]
        halves[0].append(piece[:, 0:Z])
        halves[1].append(piece[:, Z:2 * Z])
    lse_snd[...] = jnp.concatenate(halves[0] + halves[1], axis=1)
    lse_out[pl.ds(side, 1), :] = lse_ref[:, pl.ds(pl.multiple_of(core * SHARD, SHARD), SHARD)]
    lse_copy = remote(lse_snd, lse_rcv, ls_s, ls_r, xpt)
    lse_copy.start()
    for i in range(3):
        lp_copy(i).start()
    lse_copy.wait()
    lse_out[pl.ds(1 - side, 1), :] = lse_rcv[...]
    for i in range(3):
        lp_copy(i).wait()
    for s in range(2):
        for c in range(2):
            lp_out[s:s + 1, c * KC:(c + 1) * KC] = lpbuf[s * 2 + c]

    for q in range(NQ):
        fx_copy(q).wait_recv()
        relay(q).start()

    to_sib.wait()
    for q in range(NQ):
        relay(q).wait()
        fx_copy(q).wait_send()


def solution(mesh):
    def local_fit(x_local, mu_init, logpi_init, inv_temp):
        dma = pltpu.SemaphoreType.DMA
        vmem = pl.BlockSpec(memory_space=pltpu.VMEM)
        hbm = pl.BlockSpec(memory_space=pltpu.HBM)
        outs = [jax.ShapeDtypeStruct(mu_init.shape, F32),
                jax.ShapeDtypeStruct(logpi_init.shape, F32),
                jax.ShapeDtypeStruct((2, x_local.shape[0]), F32)]
        res = pl.pallas_call(
            body,
            out_shape=tuple(pltpu.VMEM(o.shape, o.dtype) for o in outs),
            in_specs=[hbm, hbm, vmem, pl.BlockSpec(memory_space=pltpu.SMEM)],
            out_specs=(vmem, vmem, vmem),
            scratch_shapes=[
                pltpu.VMEM((ROWS, HALF), BF16),
                pltpu.VMEM((NBLK, HALF, BLK), BF16),
                pltpu.VMEM((NBLK, KC, BLK), F32),
                pltpu.VMEM((KC, BLK), F32), pltpu.VMEM((KC, BLK), F32),
                pltpu.VMEM((KC, GRP * BLK), BF16),
                pltpu.VMEM((KC, GRP * BLK), BF16),
                pltpu.VMEM((KC, HALF), F32),
                pltpu.VMEM((KC, 128), F32),
                pltpu.VMEM((KC, HALF), F32),
                pltpu.VMEM((KC, HALF), BF16),
                pltpu.VMEM((KC, 128), F32),
                pltpu.VMEM((KC, 128), F32),
                pltpu.VMEM((NBLK, 1, BLK), F32),
                pltpu.VMEM((1, ROWS), F32),
                pltpu.VMEM((2, NGRP, 2, GRP, 1, BLK), F32),
                pltpu.VMEM((2, 3, NGRP, 2, GRP, 1, BLK), F32),
                pltpu.VMEM((4, 1, KC), F32),
                pltpu.VMEM((1, SHARD), F32),
                pltpu.VMEM((1, SHARD), F32),
                dma((2,)),
                dma((NCH,)), dma((NCH,)),
                dma((NCH,)), dma((NCH,)),
                dma((NCH,)), dma((NCH,)),
                dma((NOWN,)), dma((NOWN,)),
                dma((3, NGRP)), dma((2, 3, NGRP)),
                dma((3,)), dma((3,)),
                dma, dma,
                dma((NQ,)), dma((NQ,)),
                dma, dma,
                dma((NQ,)), dma((NQ,)),
            ],
            compiler_params=pltpu.CompilerParams(
                collective_id=0, has_side_effects=True,
                vmem_limit_bytes=56 * 1024 * 1024),
        )(x_local, mu_init, logpi_init, inv_temp)
        return tuple(res)

    return jax.shard_map(
        local_fit,
        mesh=mesh,
        in_specs=(P(("grp", "row"), None), P(None, ("grp", "comp"), None), P(None, ("grp", "comp")), P()),
        out_specs=(P(None, ("grp", "comp"), None), P(None, ("grp", "comp")), P(None, ("grp", "row"))),
        check_vma=False,
    )
```

```python
import jax
import jax.numpy as jnp
from jax import lax
from jax.experimental import pallas as pl
from jax.experimental.pallas import tpu as pltpu
from jax.sharding import PartitionSpec as P

EPS_COUNT = 1e-6
PRIOR_ALPHA = 1e-3

F32 = jnp.float32
BF16 = jnp.bfloat16
MESH = pl.DeviceIdType.MESH

SWEEPS = 3
HALF = 512
SHARD = 2048
ROWS = 8192
KC = 256
BLK = 256
NBLK = ROWS // BLK
GRP = 4
NGRP = NBLK // GRP
NCH = 16
Z = SHARD // 2 // NCH
NOWN = 4
PIECE = SHARD // NOWN
OWN = 2 * SHARD
NQ = 4
QC = KC // NQ


def body(x_hbm, mu_hbm, lp_in, beta_ref,
         mu_out, lp_out, lse_out,
         xb, xt_ref, p_ref, a0, a1, rb0, rb1, s_ref, nacc, mu_f, mu2, sqmu, lpb, sqx, mx_ref, lse_ref,
         st_own, st_rem, lpbuf, lse_snd, lse_rcv,
         loc_sem, xs, xr, ys, yr, ds, dr, own_s, own_r,
         st_s, st_r, lps, lpr, ls_s, ls_r, fxs, fxr, fds, fdr, frs, frr):
    comp = lax.axis_index("comp")
    row = lax.axis_index("row")
    side = row // 2
    core = row % 2
    sib = {"row": side * 2 + (1 - core)}
    ypt = {"comp": 1 - comp}
    ydg = {"comp": 1 - comp, "row": side * 2 + (1 - core)}
    xpt = {"row": (1 - side) * 2 + core}
    xdg = {"row": (1 - side) * 2 + (1 - core)}
    peers = (sib, ypt, ydg)

    barrier = pltpu.get_barrier_semaphore()
    for dev in (xpt, sib, ypt, ydg, xdg):
        pl.semaphore_signal(barrier, inc=1, device_id=dev, device_id_type=MESH)

    def remote(src, dst, ssem, rsem, dev):
        return pltpu.make_async_remote_copy(
            src_ref=src, dst_ref=dst, send_sem=ssem, recv_sem=rsem,
            device_id=dev, device_id_type=MESH)

    fit_cols = pl.ds(pl.multiple_of(side * HALF, HALF), HALF)
    oth_cols = pl.ds(pl.multiple_of((1 - side) * HALF, HALF), HALF)
    cbase = pl.multiple_of(core * KC, KC)

    def own_rows(c):
        return xb.at[pl.ds(pl.multiple_of(c * SHARD, SHARD), SHARD), :]

    ld_x = pltpu.make_async_copy(x_hbm.at[:, fit_cols], own_rows(core), loc_sem.at[0])
    ld_mu = pltpu.make_async_copy(mu_hbm.at[side, pl.ds(cbase, KC), :], mu_f, loc_sem.at[1])
    ld_mu.start()
    ld_x.start()

    def place(g, c, half, n):
        return xb.at[pl.ds(pl.multiple_of(OWN + g * (4 * Z) + c * (2 * Z) + half * Z, Z), n), :]

    def x_copy(g):
        extra = g // NCH
        g0 = g - extra
        half = comp + extra * (1 - 2 * comp)
        src = x_hbm.at[pl.ds(pl.multiple_of(half * (SHARD // 2) + g0 * Z, Z), Z), oth_cols]
        return remote(src, place(g0, core, half, Z), xs, xr.at[g], xpt)

    def y_copy(g):
        ref = place(g, core, comp, Z)
        return remote(ref, ref, ys, yr.at[g], ypt)

    def d_copy(g):
        ref = place(g, core, 0, 2 * Z)
        return remote(ref, ref, ds, dr.at[g], sib)

    def own_copy(k):
        src = x_hbm.at[pl.ds(pl.multiple_of(k * PIECE, PIECE), PIECE), fit_cols]
        dst = xb.at[pl.ds(pl.multiple_of(core * SHARD + k * PIECE, PIECE), PIECE), :]
        return remote(src, dst, own_s, own_r.at[k], sib)

    pl.semaphore_wait(barrier, 5)
    for k in range(NOWN):
        own_copy(k).start()

    @pl.loop(0, NCH + 1)
    def _(g):
        x_copy(g).start()

    def bc(row_vec):
        return jnp.transpose(jnp.broadcast_to(row_vec, (128, KC)))

    def set_means(mu):
        mu2[...] = mu.astype(BF16) * jnp.asarray(-2.0, BF16)
        sq = jnp.sum(mu * mu, axis=1, keepdims=True)
        sqmu[...] = jnp.broadcast_to(sq, (KC, 128))

    lpb[...] = bc(lp_in[pl.ds(side, 1), pl.ds(cbase, KC)])
    ld_mu.wait()
    set_means(mu_f[...])

    def prep(b):
        xt = jnp.transpose(xb[pl.ds(pl.multiple_of(b * BLK, BLK), BLK), :])
        xt_ref[b] = xt
        xf = xt.astype(F32)
        sqx[b] = jnp.sum(xf * xf, axis=0, keepdims=True)

    def cross(b, a_ref):
        a_ref[...] = jnp.dot(mu2[...], xt_ref[b], preferred_element_type=F32)

    def soft(b, a_ref, beta, par):
        sq = sqx[b]
        grp = b // GRP
        j = b % GRP
        for h in range(BLK // 128):
            cols = slice(h * 128, (h + 1) * 128)
            t = (a_ref[:, cols] + sq[:, cols]) + sqmu[...]
            logit = lpb[...] - beta * t
            m = jnp.max(logit, axis=0, keepdims=True)
            e = jnp.exp(logit - m)
            r = jnp.sum(e, axis=0, keepdims=True)
            p_ref[b, :, cols] = e
            mx_ref[b, :, cols] = m
            st_own[par, grp, j, :, cols] = m + jnp.log(r)

    def st_copy(grp, par, i):
        return remote(st_own.at[par, grp], st_rem.at[par, grp, i],
                      st_s.at[grp], st_r.at[par, grp], peers[i])

    def send_stats(grp, par):
        for i in range(3):
            st_copy(grp, par, i).start()

    def wait_stats(grp, par):
        three = st_rem.at[par, grp]
        both = remote(three, three, st_s.at[grp], st_r.at[par, grp], sib)
        both.wait_recv()
        both.wait_send()

    def resp(grp, par, rb):
        st = [st_own[par, grp]] + [st_rem[par, grp, i] for i in range(3)]
        top = jnp.maximum(jnp.maximum(st[0], st[1]), jnp.maximum(st[2], st[3]))
        es = [jnp.exp(v - top) for v in st]
        tot = (es[0] + es[1]) + (es[2] + es[3])
        lse = top + jnp.log(tot)
        first = pl.multiple_of(grp * GRP, GRP)
        scale = jnp.exp(mx_ref[pl.ds(first, GRP)] - top) / tot
        cnt = nacc[...]
        for j in range(GRP):
            lse_ref[:, pl.ds(pl.multiple_of((grp * GRP + j) * BLK, BLK), BLK)] = lse[j]
            rj = p_ref[grp * GRP + j] * scale[j]
            cnt = cnt + (rj[:, 0:128] + rj[:, 128:256])
            rb[:, j * BLK:(j + 1) * BLK] = rj.astype(BF16)
        nacc[...] = cnt

    def gather(grp, rb):
        rows = pl.ds(pl.multiple_of(grp * (GRP * BLK), GRP * BLK), GRP * BLK)
        s_ref[...] += jnp.dot(rb[...], xb[rows, :], preferred_element_type=F32)

    def mstep(grp, par):
        wait_stats(grp, par)
        resp(grp, par, rb0)
        gather(grp, rb0)

    def zero_sums():
        nacc[...] = jnp.zeros_like(nacc)
        s_ref[...] = jnp.zeros_like(s_ref)

    def finish_sweep():
        n = jnp.sum(nacc[...], axis=1, keepdims=True)
        mu = s_ref[...] / (n + EPS_COUNT)
        mu_f[...] = mu
        lp = jnp.log((n + PRIOR_ALPHA) / (ROWS + 4 * KC * PRIOR_ALPHA))
        lpb[...] = jnp.broadcast_to(lp, (KC, 128))
        set_means(mu)

    zero_sums()
    beta0 = beta_ref[0]

    def first_block(b):
        prep(b)
        cross(b, a0)
        soft(b, a0, beta0, 0)

        @pl.when(b % GRP == GRP - 1)
        def _():
            send_stats(b // GRP, 0)

    ld_x.wait()

    @pl.loop(0, NCH + 4)
    def _(it):
        @pl.when(it < NCH - 1)
        def _():
            x_copy(it).wait_recv()
            y_copy(it).start()

        @pl.when((it >= 3) & (it < NCH + 2))
        def _():
            y_copy(it - 3).wait_recv()
            d_copy(it - 3).start()

        @pl.when(it == NCH + 2)
        def _():
            x_copy(NCH - 1).wait_recv()
            x_copy(NCH).wait_recv()
            d_copy(NCH - 1).start()

        @pl.when((it < NCH) & (it // 8 != core) & (it % 2 == 0))
        def _():
            own_copy((it % 8) // 2).wait_recv()

        @pl.when(it < NCH)
        def _():
            first_block(it)

        @pl.when(it >= 4)
        def _():
            d_copy(it - 4).wait_recv()
            first_block(NBLK // 2 + it - 4)

        @pl.when((it >= 8) & (it < NCH + 4) & (it % 4 == 0))
        def _():
            mstep((it - 8) // 4, 0)

        @pl.when((it >= 14) & (it % 4 == 2))
        def _():
            mstep(NGRP // 2 + (it - 14) // 4, 0)

    mstep(NGRP // 2 - 1, 0)
    mstep(NGRP - 2, 0)
    mstep(NGRP - 1, 0)
    finish_sweep()

    def all_sent(n, sem):
        ref = xb.at[pl.ds(0, n), :]
        remote(ref, ref, sem, own_r.at[0], sib).wait_send()

    all_sent(SHARD, own_s)
    all_sent((NCH + 1) * Z, xs)
    all_sent((NCH - 1) * Z, ys)
    all_sent(NCH * 2 * Z, ds)

    @pl.loop(1, SWEEPS)
    def _(t):
        par = t % 2
        beta = beta_ref[t]
        zero_sums()
        cross(0, a0)

        @pl.loop(0, NBLK // 2)
        def _(i):
            b = 2 * i
            cross(b + 1, a1)
            soft(b, a0, beta, par)
            cross((b + 2) % NBLK, a0)
            soft(b + 1, a1, beta, par)

            @pl.when(i % 2 == 1)
            def _():
                send_stats(i // 2, par)

        wait_stats(0, par)
        resp(0, par, rb0)

        @pl.loop(0, NGRP // 2 - 1)
        def _(i):
            g = 2 * i
            wait_stats(g + 1, par)
            resp(g + 1, par, rb1)
            gather(g, rb0)
            wait_stats(g + 2, par)
            resp(g + 2, par, rb0)
            gather(g + 1, rb1)

        wait_stats(NGRP - 1, par)
        resp(NGRP - 1, par, rb1)
        gather(NGRP - 2, rb0)
        gather(NGRP - 1, rb1)
        finish_sweep()

    def block(s, q, n):
        return mu_out.at[s, pl.ds(cbase + q * QC, n), :]

    def fx_copy(q):
        ref = block(side, q, QC)
        return remote(ref, ref, fxs, fxr.at[q], xpt)

    def relay(q):
        ref = block(1 - side, q, QC)
        return remote(ref, ref, frs, frr, sib)

    mu_out[side, pl.ds(cbase, KC), :] = mu_f[...]
    to_sib = remote(block(side, 0, KC), block(side, 0, KC), fds, fdr, sib)

    slot = side * 2 + core
    lpbuf[slot] = jnp.transpose(lpb[...])[0:1, :]
    lp_devs = (sib, xpt, xdg)

    def lp_copy(i):
        return remote(lpbuf.at[slot], lpbuf.at[slot], lps, lpr, lp_devs[i])


    halves = ([], [])
    for g in range(NCH):
        piece = lse_ref[:, pl.ds(pl.multiple_of(OWN + g * (4 * Z) + core * (2 * Z), 128), 128)]
        halves[0].append(piece[:, 0:Z])
        halves[1].append(piece[:, Z:2 * Z])
    lse_snd[...] = jnp.concatenate(halves[0] + halves[1], axis=1)
    lse_out[pl.ds(side, 1), :] = lse_ref[:, pl.ds(pl.multiple_of(core * SHARD, SHARD), SHARD)]
    lse_copy = remote(lse_snd, lse_rcv, ls_s, ls_r, xpt)
    lse_copy.start()
    for i in range(3):
        lp_copy(i).start()
    for q in range(NQ):
        fx_copy(q).start()
    to_sib.start()
    lse_copy.wait()
    lse_out[pl.ds(1 - side, 1), :] = lse_rcv[...]
    remote(lpbuf.at[pl.ds(0, 3)], lpbuf.at[pl.ds(0, 3)], lps, lpr, sib).wait()
    for s in range(2):
        for c in range(2):
            lp_out[s:s + 1, c * KC:(c + 1) * KC] = lpbuf[s * 2 + c]

    for q in range(NQ):
        fx_copy(q).wait_recv()
        relay(q).start()

    to_sib.wait()
    remote(block(1 - side, 0, KC), block(1 - side, 0, KC), frs, frr, sib).wait()
    remote(block(side, 0, KC), block(side, 0, KC), fxs, frr, xpt).wait_send()


def solution(mesh):
    def local_fit(x_local, mu_init, logpi_init, inv_temp):
        dma = pltpu.SemaphoreType.DMA
        vmem = pl.BlockSpec(memory_space=pltpu.VMEM)
        hbm = pl.BlockSpec(memory_space=pltpu.HBM)
        outs = [jax.ShapeDtypeStruct(mu_init.shape, F32),
                jax.ShapeDtypeStruct(logpi_init.shape, F32),
                jax.ShapeDtypeStruct((2, x_local.shape[0]), F32)]
        res = pl.pallas_call(
            body,
            out_shape=tuple(pltpu.VMEM(o.shape, o.dtype) for o in outs),
            in_specs=[hbm, hbm, vmem, pl.BlockSpec(memory_space=pltpu.SMEM)],
            out_specs=(vmem, vmem, vmem),
            scratch_shapes=[
                pltpu.VMEM((ROWS, HALF), BF16),
                pltpu.VMEM((NBLK, HALF, BLK), BF16),
                pltpu.VMEM((NBLK, KC, BLK), F32),
                pltpu.VMEM((KC, BLK), F32), pltpu.VMEM((KC, BLK), F32),
                pltpu.VMEM((KC, GRP * BLK), BF16),
                pltpu.VMEM((KC, GRP * BLK), BF16),
                pltpu.VMEM((KC, HALF), F32),
                pltpu.VMEM((KC, 128), F32),
                pltpu.VMEM((KC, HALF), F32),
                pltpu.VMEM((KC, HALF), BF16),
                pltpu.VMEM((KC, 128), F32),
                pltpu.VMEM((KC, 128), F32),
                pltpu.VMEM((NBLK, 1, BLK), F32),
                pltpu.VMEM((NBLK, 1, BLK), F32),
                pltpu.VMEM((1, ROWS), F32),
                pltpu.VMEM((2, NGRP, GRP, 1, BLK), F32),
                pltpu.VMEM((2, NGRP, 3, GRP, 1, BLK), F32),
                pltpu.VMEM((4, 1, KC), F32),
                pltpu.VMEM((1, SHARD), F32),
                pltpu.VMEM((1, SHARD), F32),
                dma((2,)),
                dma, dma((NCH + 1,)),
                dma, dma((NCH - 1,)),
                dma, dma((NCH,)),
                dma, dma((NOWN,)),
                dma((NGRP,)), dma((2, NGRP)),
                dma, dma,
                dma, dma,
                dma, dma((NQ,)),
                dma, dma,
                dma, dma,
            ],
            compiler_params=pltpu.CompilerParams(
                collective_id=0, has_side_effects=True,
                vmem_limit_bytes=56 * 1024 * 1024),
        )(x_local, mu_init, logpi_init, inv_temp)
        return tuple(res)

    return jax.shard_map(
        local_fit,
        mesh=mesh,
        in_specs=(P(("grp", "row"), None), P(None, ("grp", "comp"), None), P(None, ("grp", "comp")), P()),
        out_specs=(P(None, ("grp", "comp"), None), P(None, ("grp", "comp")), P(None, ("grp", "row"))),
        check_vma=False,
    )
```

```python
import jax
import jax.numpy as jnp
from jax import lax
from jax.experimental import pallas as pl
from jax.experimental.pallas import tpu as pltpu
from jax.sharding import PartitionSpec as P

EPS_COUNT = 1e-6
PRIOR_ALPHA = 1e-3

F32 = jnp.float32
BF16 = jnp.bfloat16
MESH = pl.DeviceIdType.MESH

SWEEPS = 3
HALF = 512
SHARD = 2048
ROWS = 8192
KC = 256
BLK = 256
NBLK = ROWS // BLK
GRP = 4
NGRP = NBLK // GRP
NCH = 16
Z = SHARD // 2 // NCH
NOWN = 4
PIECE = SHARD // NOWN
OWN = 2 * SHARD
NQ = 4
QC = KC // NQ


def body(x_hbm, mu_hbm, lp_in, beta_ref,
         mu_out, lp_out, lse_out,
         xb, xt_ref, p_ref, a0, a1, rb0, rb1, s_ref, nacc, mu_f, mu2, sqmu, lpb, sqx, mx_ref, lse_ref,
         st_own, st_rem, lpbuf, lse_snd, lse_rcv,
         loc_sem, xs, xr, ys, yr, ds, dr, own_s, own_r,
         st_s, st_r, lps, lpr, ls_s, ls_r, fxs, fxr, fds, fdr, frs, frr):
    comp = lax.axis_index("comp")
    row = lax.axis_index("row")
    side = row // 2
    core = row % 2
    sib = {"row": side * 2 + (1 - core)}
    ypt = {"comp": 1 - comp}
    ydg = {"comp": 1 - comp, "row": side * 2 + (1 - core)}
    xpt = {"row": (1 - side) * 2 + core}
    xdg = {"row": (1 - side) * 2 + (1 - core)}
    peers = (sib, ypt, ydg)

    barrier = pltpu.get_barrier_semaphore()
    for dev in (xpt, sib, ypt, ydg, xdg):
        pl.semaphore_signal(barrier, inc=1, device_id=dev, device_id_type=MESH)

    def remote(src, dst, ssem, rsem, dev):
        return pltpu.make_async_remote_copy(
            src_ref=src, dst_ref=dst, send_sem=ssem, recv_sem=rsem,
            device_id=dev, device_id_type=MESH)

    fit_cols = pl.ds(pl.multiple_of(side * HALF, HALF), HALF)
    oth_cols = pl.ds(pl.multiple_of((1 - side) * HALF, HALF), HALF)
    cbase = pl.multiple_of(core * KC, KC)

    def own_rows(c):
        return xb.at[pl.ds(pl.multiple_of(c * SHARD, SHARD), SHARD), :]

    ld_x = pltpu.make_async_copy(x_hbm.at[:, fit_cols], own_rows(core), loc_sem.at[0])
    ld_mu = pltpu.make_async_copy(mu_hbm.at[side, pl.ds(cbase, KC), :], mu_f, loc_sem.at[1])
    ld_mu.start()
    ld_x.start()

    def place(g, c, half, n):
        return xb.at[pl.ds(pl.multiple_of(OWN + g * (4 * Z) + c * (2 * Z) + half * Z, Z), n), :]

    def x_copy(g):
        extra = g // NCH
        g0 = g - extra
        half = comp + extra * (1 - 2 * comp)
        src = x_hbm.at[pl.ds(pl.multiple_of(half * (SHARD // 2) + g0 * Z, Z), Z), oth_cols]
        return remote(src, place(g0, core, half, Z), xs, xr.at[g], xpt)

    def y_copy(g):
        ref = place(g, core, comp, Z)
        return remote(ref, ref, ys, yr.at[g], ypt)

    def d_copy(g):
        ref = place(g, core, 0, 2 * Z)
        return remote(ref, ref, ds, dr.at[g], sib)

    def own_copy(k):
        src = x_hbm.at[pl.ds(pl.multiple_of(k * PIECE, PIECE), PIECE), fit_cols]
        dst = xb.at[pl.ds(pl.multiple_of(core * SHARD + k * PIECE, PIECE), PIECE), :]
        return remote(src, dst, own_s, own_r.at[k], sib)

    pl.semaphore_wait(barrier, 5)
    for k in range(NOWN):
        own_copy(k).start()

    @pl.loop(0, NCH + 1)
    def _(g):
        x_copy(g).start()

    def bc(row_vec):
        return jnp.transpose(jnp.broadcast_to(row_vec, (128, KC)))

    def set_means(mu):
        mu2[...] = mu.astype(BF16) * jnp.asarray(-2.0, BF16)
        sq = jnp.sum(mu * mu, axis=1, keepdims=True)
        sqmu[...] = jnp.broadcast_to(sq, (KC, 128))

    lpb[...] = bc(lp_in[pl.ds(side, 1), pl.ds(cbase, KC)])
    ld_mu.wait()
    set_means(mu_f[...])

    def prep(b):
        xt = jnp.transpose(xb[pl.ds(pl.multiple_of(b * BLK, BLK), BLK), :])
        xt_ref[b] = xt
        xf = xt.astype(F32)
        sqx[b] = jnp.sum(xf * xf, axis=0, keepdims=True)

    def cross(b, a_ref):
        a_ref[...] = jnp.dot(mu2[...], xt_ref[b], preferred_element_type=F32)

    def soft(b, a_ref, beta, par):
        sq = sqx[b]
        grp = b // GRP
        j = b % GRP
        for h in range(BLK // 128):
            cols = slice(h * 128, (h + 1) * 128)
            t = (a_ref[:, cols] + sq[:, cols]) + sqmu[...]
            logit = lpb[...] - beta * t
            m = jnp.max(logit, axis=0, keepdims=True)
            e = jnp.exp(logit - m)
            r = jnp.sum(e, axis=0, keepdims=True)
            p_ref[b, :, cols] = e
            mx_ref[b, :, cols] = m
            st_own[par, grp, j, :, cols] = m + jnp.log(r)

    def st_copy(grp, par, i):
        return remote(st_own.at[par, grp], st_rem.at[par, grp, i],
                      st_s.at[grp], st_r.at[par, grp], peers[i])

    def send_stats(grp, par):
        for i in range(3):
            st_copy(grp, par, i).start()

    def wait_stats(grp, par):
        three = st_rem.at[par, grp]
        both = remote(three, three, st_s.at[grp], st_r.at[par, grp], sib)
        both.wait_recv()
        both.wait_send()

    def resp(grp, par, rb):
        st = [st_own[par, grp]] + [st_rem[par, grp, i] for i in range(3)]
        top = jnp.maximum(jnp.maximum(st[0], st[1]), jnp.maximum(st[2], st[3]))
        es = [jnp.exp(v - top) for v in st]
        tot = (es[0] + es[1]) + (es[2] + es[3])
        lse = top + jnp.log(tot)
        first = pl.multiple_of(grp * GRP, GRP)
        scale = jnp.exp(mx_ref[pl.ds(first, GRP)] - top) / tot
        cnt = nacc[...]
        for j in range(GRP):
            lse_ref[:, pl.ds(pl.multiple_of((grp * GRP + j) * BLK, BLK), BLK)] = lse[j]
            rj = p_ref[grp * GRP + j] * scale[j]
            cnt = cnt + (rj[:, 0:128] + rj[:, 128:256])
            rb[:, j * BLK:(j + 1) * BLK] = rj.astype(BF16)
        nacc[...] = cnt

    def gather(grp, rb):
        rows = pl.ds(pl.multiple_of(grp * (GRP * BLK), GRP * BLK), GRP * BLK)
        s_ref[...] += jnp.dot(rb[...], xb[rows, :], preferred_element_type=F32)

    def mstep(grp, par):
        wait_stats(grp, par)
        resp(grp, par, rb0)
        gather(grp, rb0)

    def zero_sums():
        nacc[...] = jnp.zeros_like(nacc)
        s_ref[...] = jnp.zeros_like(s_ref)

    def finish_sweep():
        n = jnp.sum(nacc[...], axis=1, keepdims=True)
        mu = s_ref[...] / (n + EPS_COUNT)
        mu_f[...] = mu
        lp = jnp.log((n + PRIOR_ALPHA) / (ROWS + 4 * KC * PRIOR_ALPHA))
        lpb[...] = jnp.broadcast_to(lp, (KC, 128))
        set_means(mu)

    zero_sums()
    beta0 = beta_ref[0]

    def first_block(b):
        prep(b)
        cross(b, a0)
        soft(b, a0, beta0, 0)

        @pl.when(b % GRP == GRP - 1)
        def _():
            send_stats(b // GRP, 0)

    ld_x.wait()

    @pl.loop(0, NCH + 4)
    def _(it):
        @pl.when(it < NCH - 1)
        def _():
            x_copy(it).wait_recv()
            y_copy(it).start()

        @pl.when((it >= 3) & (it < NCH + 2))
        def _():
            y_copy(it - 3).wait_recv()
            d_copy(it - 3).start()

        @pl.when(it == NCH + 1)
        def _():
            x_copy(NCH - 1).wait_recv()
            x_copy(NCH).wait_recv()
            d_copy(NCH - 1).start()

        @pl.when((it < NCH) & (it // 8 != core) & (it % 2 == 0))
        def _():
            own_copy((it % 8) // 2).wait_recv()

        @pl.when(it < NCH)
        def _():
            first_block(it)

        @pl.when(it >= 4)
        def _():
            d_copy(it - 4).wait_recv()
            first_block(NBLK // 2 + it - 4)

        @pl.when((it >= 8) & (it < NCH) & (it % 4 == 0))
        def _():
            mstep((it - 8) // 4, 0)

        @pl.when((it >= 14) & (it < NCH) & (it % 4 == 2))
        def _():
            mstep(NGRP // 2 + (it - 14) // 4, 0)

    for g in (2, 3, 5, 6):
        mstep(g, 0)
    mstep(NGRP - 1, 0)
    finish_sweep()

    def all_sent(n, sem):
        ref = xb.at[pl.ds(0, n), :]
        remote(ref, ref, sem, own_r.at[0], sib).wait_send()

    all_sent(SHARD, own_s)
    all_sent((NCH + 1) * Z, xs)
    all_sent((NCH - 1) * Z, ys)
    all_sent(NCH * 2 * Z, ds)

    @pl.loop(1, SWEEPS)
    def _(t):
        par = t % 2
        beta = beta_ref[t]
        zero_sums()
        @pl.loop(0, NBLK // 8)
        def _(i):
            for k in range(8):
                b = 8 * i + k
                soft(b, jnp.dot(mu2[...], xt_ref[b], preferred_element_type=F32), beta, par)
            for g in range(8 // GRP):
                send_stats(i * (8 // GRP) + g, par)

        for g in range(NGRP):
            wait_stats(g, par)
            resp(g, par, (rb0, rb1)[g % 2])
            gather(g, (rb0, rb1)[g % 2])
        finish_sweep()

    def block(s, q, n):
        return mu_out.at[s, pl.ds(cbase + q * QC, n), :]

    def fx_copy(q):
        ref = block(side, q, QC)
        return remote(ref, ref, fxs, fxr.at[q], xpt)

    def relay(q):
        ref = block(1 - side, q, QC)
        return remote(ref, ref, frs, frr, sib)

    mu_out[side, pl.ds(cbase, KC), :] = mu_f[...]
    to_sib = remote(block(side, 0, KC), block(side, 0, KC), fds, fdr, sib)

    slot = side * 2 + core
    lpbuf[slot] = jnp.transpose(lpb[...])[0:1, :]
    lp_devs = (sib, xpt, xdg)

    def lp_copy(i):
        return remote(lpbuf.at[slot], lpbuf.at[slot], lps, lpr, lp_devs[i])


    halves = ([], [])
    for g in range(NCH):
        piece = lse_ref[:, pl.ds(pl.multiple_of(OWN + g * (4 * Z) + core * (2 * Z), 128), 128)]
        halves[0].append(piece[:, 0:Z])
        halves[1].append(piece[:, Z:2 * Z])
    lse_snd[...] = jnp.concatenate(halves[0] + halves[1], axis=1)
    lse_out[pl.ds(side, 1), :] = lse_ref[:, pl.ds(pl.multiple_of(core * SHARD, SHARD), SHARD)]
    lse_copy = remote(lse_snd, lse_rcv, ls_s, ls_r, xpt)
    lse_copy.start()
    for i in range(3):
        lp_copy(i).start()
    for q in range(NQ):
        fx_copy(q).start()
    to_sib.start()
    lse_copy.wait()
    lse_out[pl.ds(1 - side, 1), :] = lse_rcv[...]
    remote(lpbuf.at[pl.ds(0, 3)], lpbuf.at[pl.ds(0, 3)], lps, lpr, sib).wait()
    for s in range(2):
        for c in range(2):
            lp_out[s:s + 1, c * KC:(c + 1) * KC] = lpbuf[s * 2 + c]

    for q in range(NQ):
        fx_copy(q).wait_recv()
        relay(q).start()

    to_sib.wait()
    remote(block(1 - side, 0, KC), block(1 - side, 0, KC), frs, frr, sib).wait()
    remote(block(side, 0, KC), block(side, 0, KC), fxs, frr, xpt).wait_send()


def solution(mesh):
    def local_fit(x_local, mu_init, logpi_init, inv_temp):
        dma = pltpu.SemaphoreType.DMA
        vmem = pl.BlockSpec(memory_space=pltpu.VMEM)
        hbm = pl.BlockSpec(memory_space=pltpu.HBM)
        outs = [jax.ShapeDtypeStruct(mu_init.shape, F32),
                jax.ShapeDtypeStruct(logpi_init.shape, F32),
                jax.ShapeDtypeStruct((2, x_local.shape[0]), F32)]
        res = pl.pallas_call(
            body,
            out_shape=tuple(pltpu.VMEM(o.shape, o.dtype) for o in outs),
            in_specs=[hbm, hbm, vmem, pl.BlockSpec(memory_space=pltpu.SMEM)],
            out_specs=(vmem, vmem, vmem),
            scratch_shapes=[
                pltpu.VMEM((ROWS, HALF), BF16),
                pltpu.VMEM((NBLK, HALF, BLK), BF16),
                pltpu.VMEM((NBLK, KC, BLK), F32),
                pltpu.VMEM((KC, BLK), F32), pltpu.VMEM((KC, BLK), F32),
                pltpu.VMEM((KC, GRP * BLK), BF16),
                pltpu.VMEM((KC, GRP * BLK), BF16),
                pltpu.VMEM((KC, HALF), F32),
                pltpu.VMEM((KC, 128), F32),
                pltpu.VMEM((KC, HALF), F32),
                pltpu.VMEM((KC, HALF), BF16),
                pltpu.VMEM((KC, 128), F32),
                pltpu.VMEM((KC, 128), F32),
                pltpu.VMEM((NBLK, 1, BLK), F32),
                pltpu.VMEM((NBLK, 1, BLK), F32),
                pltpu.VMEM((1, ROWS), F32),
                pltpu.VMEM((2, NGRP, GRP, 1, BLK), F32),
                pltpu.VMEM((2, NGRP, 3, GRP, 1, BLK), F32),
                pltpu.VMEM((4, 1, KC), F32),
                pltpu.VMEM((1, SHARD), F32),
                pltpu.VMEM((1, SHARD), F32),
                dma((2,)),
                dma, dma((NCH + 1,)),
                dma, dma((NCH - 1,)),
                dma, dma((NCH,)),
                dma, dma((NOWN,)),
                dma((NGRP,)), dma((2, NGRP)),
                dma, dma,
                dma, dma,
                dma, dma((NQ,)),
                dma, dma,
                dma, dma,
            ],
            compiler_params=pltpu.CompilerParams(
                collective_id=0, has_side_effects=True,
                vmem_limit_bytes=56 * 1024 * 1024),
        )(x_local, mu_init, logpi_init, inv_temp)
        return tuple(res)

    return jax.shard_map(
        local_fit,
        mesh=mesh,
        in_specs=(P(("grp", "row"), None), P(None, ("grp", "comp"), None), P(None, ("grp", "comp")), P()),
        out_specs=(P(None, ("grp", "comp"), None), P(None, ("grp", "comp")), P(None, ("grp", "row"))),
        check_vma=False,
    )
```

```python
import jax
import jax.numpy as jnp
from jax import lax
from jax.experimental import pallas as pl
from jax.experimental.pallas import tpu as pltpu
from jax.sharding import PartitionSpec as P

EPS_COUNT = 1e-6
PRIOR_ALPHA = 1e-3

F32 = jnp.float32
BF16 = jnp.bfloat16
MESH = pl.DeviceIdType.MESH

SWEEPS = 3
HALF = 512
HH = HALF // 2
SHARD = 2048
ROWS = 8192
KC = 256
BLK = 256
NBLK = ROWS // BLK
GRP = 4
NGRP = NBLK // GRP
NCH = 16
Z = SHARD // 2 // NCH
PRE = 4
NOWN = 4
PIECE = SHARD // NOWN
OWN = 2 * SHARD
NQ = 4
QC = KC // NQ


def body(x_hbm, mu_hbm, lp_hbm, beta_hbm,
         mu_out, lp_out, lse_out,
         xb, xt_ref, p_ref, rb, xpre, lp_in, beta_ref, s_ref, nacc, inv_n, mu_f, mu2, sqmu, lpb, sqx, mx_ref, lse_ref,
         st_own, st_rem, lpbuf, lse_snd, lse_rcv,
         loc_sem, xs, xr, ys, yr, ds, dr, own_s, own_r,
         st_s, st_r, lps, lpr, ls_s, ls_r, fxs, fxr, fds, fdr, frs, frr):
    comp = lax.axis_index("comp")
    row = lax.axis_index("row")
    side = row // 2
    core = row % 2
    sib = {"row": side * 2 + (1 - core)}
    ypt = {"comp": 1 - comp}
    ydg = {"comp": 1 - comp, "row": side * 2 + (1 - core)}
    xpt = {"row": (1 - side) * 2 + core}
    xdg = {"row": (1 - side) * 2 + (1 - core)}
    peers = (sib, ypt, ydg)

    barrier = pltpu.get_barrier_semaphore()
    for dev in (xpt, sib, ypt, ydg, xdg):
        pl.semaphore_signal(barrier, inc=1, device_id=dev, device_id_type=MESH)

    def remote(src, dst, ssem, rsem, dev):
        return pltpu.make_async_remote_copy(
            src_ref=src, dst_ref=dst, send_sem=ssem, recv_sem=rsem,
            device_id=dev, device_id_type=MESH)

    fit_cols = pl.ds(pl.multiple_of(side * HALF, HALF), HALF)
    oth_cols = pl.ds(pl.multiple_of((1 - side) * HALF, HALF), HALF)
    cbase = pl.multiple_of(core * KC, KC)

    def own_rows(c):
        return xb.at[pl.ds(pl.multiple_of(c * SHARD, SHARD), SHARD), :]

    ld_x = pltpu.make_async_copy(x_hbm.at[:, fit_cols], own_rows(core), loc_sem.at[0])
    ld_mu = pltpu.make_async_copy(mu_hbm.at[side, pl.ds(cbase, KC), :], mu_f, loc_sem.at[1])
    ld_pre = pltpu.make_async_copy(
        x_hbm.at[pl.ds(pl.multiple_of(comp * (SHARD // 2), PRE * Z), PRE * Z), oth_cols],
        xpre, loc_sem.at[2])
    ld_lp = pltpu.make_async_copy(lp_hbm, lp_in, loc_sem.at[3])
    ld_beta = pltpu.make_async_copy(beta_hbm, beta_ref, loc_sem.at[4])
    ld_pre.start()
    ld_mu.start()
    ld_lp.start()
    ld_beta.start()
    ld_x.start()

    def place(g, c, half, n):
        return xb.at[pl.ds(pl.multiple_of(OWN + g * (4 * Z) + c * (2 * Z) + half * Z, Z), n), :]

    def x_copy(g):
        extra = g // NCH
        g0 = g - extra
        half = comp + extra * (1 - 2 * comp)
        src = x_hbm.at[pl.ds(pl.multiple_of(half * (SHARD // 2) + g0 * Z, Z), Z), oth_cols]
        return remote(src, place(g0, core, half, Z), xs, xr.at[g], xpt)

    def y_copy(g):
        ref = place(g, core, comp, Z)
        return remote(ref, ref, ys, yr.at[g], ypt)

    def d_copy(g):
        ref = place(g, core, 0, 2 * Z)
        return remote(ref, ref, ds, dr.at[g], sib)

    def own_copy(k):
        src = x_hbm.at[pl.ds(pl.multiple_of(k * PIECE, PIECE), PIECE), fit_cols]
        dst = xb.at[pl.ds(pl.multiple_of(core * SHARD + k * PIECE, PIECE), PIECE), :]
        return remote(src, dst, own_s, own_r.at[k], sib)

    pl.semaphore_wait(barrier, 5)
    ld_pre.wait()
    for g in range(PRE):
        remote(xpre.at[pl.ds(g * Z, Z), :], place(g, core, comp, Z), xs, xr.at[g], xpt).start()
    for k in range(NOWN):
        own_copy(k).start()

    @pl.loop(PRE, NCH + 1)
    def _(g):
        x_copy(g).start()

    def bc(row_vec):
        return jnp.transpose(jnp.broadcast_to(row_vec, (128, KC)))

    def set_means(h, mu):
        mu2[:, h * HH:(h + 1) * HH] = mu.astype(BF16) * jnp.asarray(-2.0, BF16)
        sq = jnp.broadcast_to(jnp.sum(mu * mu, axis=1, keepdims=True), (KC, 128))
        sqmu[...] = sq if h == 0 else sqmu[...] + sq

    ld_lp.wait()
    ld_beta.wait()
    lpb[...] = bc(lp_in[pl.ds(side, 1), pl.ds(cbase, KC)])
    ld_mu.wait()
    for h in range(2):
        set_means(h, mu_f[:, h * HH:(h + 1) * HH])

    def prep(b):
        xt = jnp.transpose(xb[pl.ds(pl.multiple_of(b * BLK, BLK), BLK), :])
        xt_ref[b] = xt
        xf = xt.astype(F32)
        sqx[b] = jnp.sum(xf * xf, axis=0, keepdims=True)

    def cross(b):
        return jnp.dot(mu2[...], xt_ref[b], preferred_element_type=F32)

    def soft(b, a2, beta, par):
        sq = sqx[b]
        grp = b // GRP
        j = b % GRP
        for h in range(BLK // 128):
            cols = slice(h * 128, (h + 1) * 128)
            t = (a2[:, cols] + sq[:, cols]) + sqmu[...]
            logit = lpb[...] - beta * t
            m = jnp.max(logit, axis=0, keepdims=True)
            e = jnp.exp(logit - m)
            r = jnp.sum(e, axis=0, keepdims=True)
            p_ref[b, :, cols] = e
            mx_ref[b, :, cols] = m
            st_own[par, grp, j, :, cols] = m + jnp.log(r)

    def st_copy(grp, par, i):
        return remote(st_own.at[par, grp], st_rem.at[par, grp, i],
                      st_s.at[grp], st_r.at[par, grp], peers[i])

    def send_stats(grp, par):
        for i in range(3):
            st_copy(grp, par, i).start()

    def wait_stats(grp, par):
        three = st_rem.at[par, grp]
        both = remote(three, three, st_s.at[grp], st_r.at[par, grp], sib)
        both.wait_recv()
        both.wait_send()

    def resp(grp, par):
        st = [st_own[par, grp]] + [st_rem[par, grp, i] for i in range(3)]
        top = jnp.maximum(jnp.maximum(st[0], st[1]), jnp.maximum(st[2], st[3]))
        es = [jnp.exp(v - top) for v in st]
        tot = (es[0] + es[1]) + (es[2] + es[3])
        lse = top + jnp.log(tot)
        first = pl.multiple_of(grp * GRP, GRP)
        scale = jnp.exp(mx_ref[pl.ds(first, GRP)] - top) / tot
        cnt = nacc[...]
        for j in range(GRP):
            lse_ref[:, pl.ds(pl.multiple_of((grp * GRP + j) * BLK, BLK), BLK)] = lse[j]
            rj = p_ref[grp * GRP + j] * scale[j]
            cnt = cnt + (rj[:, 0:128] + rj[:, 128:256])
            rb[grp, :, j * BLK:(j + 1) * BLK] = rj.astype(BF16)
        nacc[...] = cnt

    def gather(grp, h):
        rows = pl.ds(pl.multiple_of(grp * (GRP * BLK), GRP * BLK), GRP * BLK)
        s_ref[h] += jnp.dot(rb[grp], xb[rows, h * HH:(h + 1) * HH], preferred_element_type=F32)

    def mstep(grp, par):
        wait_stats(grp, par)
        resp(grp, par)
        gather(grp, 0)
        gather(grp, 1)

    def zero_sums():
        nacc[...] = jnp.zeros_like(nacc)
        s_ref[...] = jnp.zeros_like(s_ref)

    def finish_counts():
        n = jnp.sum(nacc[...], axis=1, keepdims=True)
        lp = jnp.log((n + PRIOR_ALPHA) / (ROWS + 4 * KC * PRIOR_ALPHA))
        lpb[...] = jnp.broadcast_to(lp, (KC, 128))
        inv_n[...] = jnp.broadcast_to(1.0 / (n + EPS_COUNT), (KC, 128))

    def finish_means(h):
        inv = inv_n[...]
        mu = s_ref[h] * jnp.concatenate([inv, inv], axis=1)
        mu_out[side, pl.ds(cbase, KC), h * HH:(h + 1) * HH] = mu
        set_means(h, mu)

    zero_sums()
    beta0 = beta_ref[0]

    def first_block(b):
        prep(b)
        soft(b, cross(b), beta0, 0)

        @pl.when(b % GRP == GRP - 1)
        def _():
            send_stats(b // GRP, 0)

    def own_block(n):
        @pl.when((n >= 8) & (n % 2 == 0))
        def _():
            own_copy((n - 8) // 2).wait_recv()

        first_block((core * 8 + n) % 16)

    ld_x.wait()

    @pl.loop(0, 4)
    def _(n):
        own_block(n)

    @pl.loop(0, NCH + 4)
    def _(it):
        @pl.when(it < NCH - 1)
        def _():
            x_copy(it).wait_recv()
            y_copy(it).start()

        @pl.when((it >= 3) & (it < NCH + 2))
        def _():
            y_copy(it - 3).wait_recv()
            d_copy(it - 3).start()

        @pl.when(it == NCH + 1)
        def _():
            x_copy(NCH - 1).wait_recv()
            x_copy(NCH).wait_recv()
            d_copy(NCH - 1).start()

        @pl.when(it < 4)
        def _():
            @pl.loop(0, 2)
            def _(k):
                own_block(4 + 2 * it + k)

        @pl.when((it >= 4) & (it < 8))
        def _():
            own_block(8 + it)

        @pl.when(it >= 4)
        def _():
            d_copy(it - 4).wait_recv()
            first_block(NBLK // 2 + it - 4)

        @pl.when((it >= 9) & (it < 15))
        def _():
            mstep(it - 9, 0)

    mstep(NGRP - 2, 0)
    mstep(NGRP - 1, 0)
    finish_counts()
    for h in range(2):
        finish_means(h)

    def all_sent(n, sem):
        ref = xb.at[pl.ds(0, n), :]
        remote(ref, ref, sem, own_r.at[0], sib).wait_send()

    all_sent(SHARD, own_s)
    all_sent((NCH + 1) * Z, xs)
    all_sent((NCH - 1) * Z, ys)
    all_sent(NCH * 2 * Z, ds)

    def block(s, q):
        return mu_out.at[s, pl.ds(cbase + (q % 2) * (KC // 2), KC // 2), pl.ds((q // 2) * HH, HH)]

    def whole(s):
        return mu_out.at[s, pl.ds(cbase, KC), :]

    def fx_copy(q):
        ref = block(side, q)
        return remote(ref, ref, fxs, fxr.at[q], xpt)

    def relay(q):
        ref = block(1 - side, q)
        return remote(ref, ref, frs, frr, sib)

    def send_half(h):
        for q in (2 * h, 2 * h + 1):
            fx_copy(q).start()
        ref = mu_out.at[side, pl.ds(cbase, KC), pl.ds(h * HH, HH)]
        remote(ref, ref, fds, fdr, sib).start()

    slot = side * 2 + core
    lp_devs = (sib, xpt, xdg)
    lse_copy = remote(lse_snd, lse_rcv, ls_s, ls_r, xpt)

    def send_small():
        lpbuf[slot] = jnp.transpose(lpb[...])[0:1, :]
        halves = ([], [])
        for g in range(NCH):
            piece = lse_ref[:, pl.ds(pl.multiple_of(OWN + g * (4 * Z) + core * (2 * Z), 128), 128)]
            halves[0].append(piece[:, 0:Z])
            halves[1].append(piece[:, Z:2 * Z])
        lse_snd[...] = jnp.concatenate(halves[0] + halves[1], axis=1)
        lse_out[pl.ds(side, 1), :] = lse_ref[:, pl.ds(pl.multiple_of(core * SHARD, SHARD), SHARD)]
        lse_copy.start()
        for i in range(3):
            remote(lpbuf.at[slot], lpbuf.at[slot], lps, lpr, lp_devs[i]).start()

    @pl.loop(1, SWEEPS)
    def _(t):
        par = t % 2
        beta = beta_ref[t]
        zero_sums()
        @pl.loop(0, NBLK // 8)
        def _(i):
            for k in range(8):
                b = 8 * i + k
                soft(b, cross(b), beta, par)
            for g in range(8 // GRP):
                send_stats(i * (8 // GRP) + g, par)

        for g in range(NGRP):
            wait_stats(g, par)
            resp(g, par)
            gather(g, 0)
        finish_counts()
        finish_means(0)

        @pl.when(t == SWEEPS - 1)
        def _():
            send_small()
            send_half(0)

        for g in range(NGRP):
            gather(g, 1)
        finish_means(1)

        @pl.when(t == SWEEPS - 1)
        def _():
            send_half(1)

    lse_copy.wait()
    lse_out[pl.ds(1 - side, 1), :] = lse_rcv[...]
    remote(lpbuf.at[pl.ds(0, 3)], lpbuf.at[pl.ds(0, 3)], lps, lpr, sib).wait()
    for s in range(2):
        for c in range(2):
            lp_out[s:s + 1, c * KC:(c + 1) * KC] = lpbuf[s * 2 + c]

    for q in range(NQ):
        fx_copy(q).wait_recv()
        relay(q).start()

    remote(whole(side), whole(side), fds, fdr, sib).wait()
    remote(whole(1 - side), whole(1 - side), frs, frr, sib).wait()
    remote(whole(side), whole(side), fxs, frr, xpt).wait_send()


def write_out(mu_v, lp_v, lse_v, mu_o, lp_o, lse_o, sem):
    pairs = ((mu_v, mu_o), (lp_v, lp_o), (lse_v, lse_o))
    copies = [pltpu.make_async_copy(src, dst, sem.at[i]) for i, (src, dst) in enumerate(pairs)]
    for c in copies:
        c.start()
    for c in copies:
        c.wait()


def solution(mesh):
    def local_fit(x_local, mu_init, logpi_init, inv_temp):
        dma = pltpu.SemaphoreType.DMA
        vmem = pl.BlockSpec(memory_space=pltpu.VMEM)
        hbm = pl.BlockSpec(memory_space=pltpu.HBM)
        outs = [jax.ShapeDtypeStruct(mu_init.shape, F32),
                jax.ShapeDtypeStruct(logpi_init.shape, F32),
                jax.ShapeDtypeStruct((2, x_local.shape[0]), F32)]
        res = pl.pallas_call(
            body,
            out_shape=tuple(pltpu.VMEM(o.shape, o.dtype) for o in outs),
            in_specs=[hbm] * 4,
            out_specs=(vmem, vmem, vmem),
            scratch_shapes=[
                pltpu.VMEM((ROWS, HALF), BF16),
                pltpu.VMEM((NBLK, HALF, BLK), BF16),
                pltpu.VMEM((NBLK, KC, BLK), F32),
                pltpu.VMEM((NGRP, KC, GRP * BLK), BF16),
                pltpu.VMEM((PRE * Z, HALF), BF16),
                pltpu.VMEM((2, 2 * KC), F32),
                pltpu.SMEM((SWEEPS,), F32),
                pltpu.VMEM((2, KC, HH), F32),
                pltpu.VMEM((KC, 128), F32),
                pltpu.VMEM((KC, 128), F32),
                pltpu.VMEM((KC, HALF), F32),
                pltpu.VMEM((KC, HALF), BF16),
                pltpu.VMEM((KC, 128), F32),
                pltpu.VMEM((KC, 128), F32),
                pltpu.VMEM((NBLK, 1, BLK), F32),
                pltpu.VMEM((NBLK, 1, BLK), F32),
                pltpu.VMEM((1, ROWS), F32),
                pltpu.VMEM((2, NGRP, GRP, 1, BLK), F32),
                pltpu.VMEM((2, NGRP, 3, GRP, 1, BLK), F32),
                pltpu.VMEM((4, 1, KC), F32),
                pltpu.VMEM((1, SHARD), F32),
                pltpu.VMEM((1, SHARD), F32),
                dma((5,)),
                dma, dma((NCH + 1,)),
                dma, dma((NCH - 1,)),
                dma, dma((NCH,)),
                dma, dma((NOWN,)),
                dma((NGRP,)), dma((2, NGRP)),
                dma, dma,
                dma, dma,
                dma, dma((NQ,)),
                dma, dma,
                dma, dma,
            ],
            compiler_params=pltpu.CompilerParams(
                collective_id=0, has_side_effects=True,
                vmem_limit_bytes=56 * 1024 * 1024),
        )(x_local, mu_init, logpi_init, inv_temp)
        return pl.pallas_call(
            write_out,
            out_shape=tuple(outs),
            in_specs=[vmem] * 3,
            out_specs=(hbm,) * 3,
            scratch_shapes=[dma((3,))],
        )(*[pltpu.with_memory_space_constraint(r, pltpu.VMEM) for r in res])

    return jax.shard_map(
        local_fit,
        mesh=mesh,
        in_specs=(P(("grp", "row"), None), P(None, ("grp", "comp"), None), P(None, ("grp", "comp")), P()),
        out_specs=(P(None, ("grp", "comp"), None), P(None, ("grp", "comp")), P(None, ("grp", "row"))),
        check_vma=False,
    )
```

```python
import jax
import jax.numpy as jnp
from jax import lax
from jax.experimental import pallas as pl
from jax.experimental.pallas import tpu as pltpu
from jax.sharding import PartitionSpec as P

EPS_COUNT = 1e-6
PRIOR_ALPHA = 1e-3

F32 = jnp.float32
BF16 = jnp.bfloat16
MESH = pl.DeviceIdType.MESH

SWEEPS = 3
HALF = 512
SHARD = 2048
ROWS = 8192
KC = 256
BLK = 256
NBLK = ROWS // BLK
GRP = 4
NGRP = NBLK // GRP
NCH = 16
Z = SHARD // 2 // NCH
PRE = 4
NOWN = 4
PIECE = SHARD // NOWN
OWN = 2 * SHARD
NQ = 4
QC = KC // NQ


def body(x_hbm, mu_hbm, lp_hbm, beta_hbm,
         mu_out, lp_out, lse_out,
         xb, xt_ref, p_ref, rb, xpre, lp_in, beta_ref, s_ref, nacc, mu_f, mu2, sqmu, lpb, sqx, mx_ref, lse_ref,
         st_own, st_rem, lpbuf, lse_snd, lse_rcv,
         loc_sem, xs, xr, ys, yr, ds, dr, own_s, own_r,
         st_s, st_r, lps, lpr, ls_s, ls_r, fxs, fxr, fds, fdr, frs, frr):
    comp = lax.axis_index("comp")
    row = lax.axis_index("row")
    side = row // 2
    core = row % 2
    sib = {"row": side * 2 + (1 - core)}
    ypt = {"comp": 1 - comp}
    ydg = {"comp": 1 - comp, "row": side * 2 + (1 - core)}
    xpt = {"row": (1 - side) * 2 + core}
    xdg = {"row": (1 - side) * 2 + (1 - core)}
    peers = (sib, ypt, ydg)

    barrier = pltpu.get_barrier_semaphore()
    for dev in (xpt, sib, ypt, ydg, xdg):
        pl.semaphore_signal(barrier, inc=1, device_id=dev, device_id_type=MESH)

    def remote(src, dst, ssem, rsem, dev):
        return pltpu.make_async_remote_copy(
            src_ref=src, dst_ref=dst, send_sem=ssem, recv_sem=rsem,
            device_id=dev, device_id_type=MESH)

    fit_cols = pl.ds(pl.multiple_of(side * HALF, HALF), HALF)
    oth_cols = pl.ds(pl.multiple_of((1 - side) * HALF, HALF), HALF)
    cbase = pl.multiple_of(core * KC, KC)

    def own_rows(c):
        return xb.at[pl.ds(pl.multiple_of(c * SHARD, SHARD), SHARD), :]

    ld_x = pltpu.make_async_copy(x_hbm.at[:, fit_cols], own_rows(core), loc_sem.at[0])
    ld_mu = pltpu.make_async_copy(mu_hbm.at[side, pl.ds(cbase, KC), :], mu_f, loc_sem.at[1])
    ld_pre = pltpu.make_async_copy(
        x_hbm.at[pl.ds(pl.multiple_of(comp * (SHARD // 2), PRE * Z), PRE * Z), oth_cols],
        xpre, loc_sem.at[2])
    ld_lp = pltpu.make_async_copy(lp_hbm, lp_in, loc_sem.at[3])
    ld_beta = pltpu.make_async_copy(beta_hbm, beta_ref, loc_sem.at[4])
    ld_pre.start()
    ld_mu.start()
    ld_lp.start()
    ld_beta.start()
    ld_x.start()

    def place(g, c, half, n):
        return xb.at[pl.ds(pl.multiple_of(OWN + g * (4 * Z) + c * (2 * Z) + half * Z, Z), n), :]

    def x_copy(g):
        extra = g // NCH
        g0 = g - extra
        half = comp + extra * (1 - 2 * comp)
        src = x_hbm.at[pl.ds(pl.multiple_of(half * (SHARD // 2) + g0 * Z, Z), Z), oth_cols]
        return remote(src, place(g0, core, half, Z), xs, xr.at[g], xpt)

    def y_copy(g):
        ref = place(g, core, comp, Z)
        return remote(ref, ref, ys, yr.at[g], ypt)

    def d_copy(g):
        ref = place(g, core, 0, 2 * Z)
        return remote(ref, ref, ds, dr.at[g], sib)

    def own_copy(k):
        src = x_hbm.at[pl.ds(pl.multiple_of(k * PIECE, PIECE), PIECE), fit_cols]
        dst = xb.at[pl.ds(pl.multiple_of(core * SHARD + k * PIECE, PIECE), PIECE), :]
        return remote(src, dst, own_s, own_r.at[k], sib)

    pl.semaphore_wait(barrier, 5)
    ld_pre.wait()
    for g in range(PRE):
        remote(xpre.at[pl.ds(g * Z, Z), :], place(g, core, comp, Z), xs, xr.at[g], xpt).start()
    for k in range(NOWN):
        own_copy(k).start()

    @pl.loop(PRE, NCH + 1)
    def _(g):
        x_copy(g).start()

    def bc(row_vec):
        return jnp.transpose(jnp.broadcast_to(row_vec, (128, KC)))

    def set_means(mu):
        mu2[...] = mu.astype(BF16) * jnp.asarray(-2.0, BF16)
        sqmu[...] = jnp.broadcast_to(jnp.sum(mu * mu, axis=1, keepdims=True), (KC, 128))

    ld_lp.wait()
    ld_beta.wait()
    lpb[...] = bc(lp_in[pl.ds(side, 1), pl.ds(cbase, KC)])
    ld_mu.wait()
    set_means(mu_f[...])

    def prep(b):
        xt = jnp.transpose(xb[pl.ds(pl.multiple_of(b * BLK, BLK), BLK), :])
        xt_ref[b // 2, :, pl.ds(pl.multiple_of(b % 2 * BLK, BLK), BLK)] = xt
        xf = xt.astype(F32)
        sqx[b] = jnp.sum(xf * xf, axis=0, keepdims=True)

    def cross(xt):
        return jnp.dot(mu2[...], xt, preferred_element_type=F32)

    def soft(b, a2, beta, par):
        sq = sqx[b]
        grp = b // GRP
        j = b % GRP
        for h in range(BLK // 128):
            cols = slice(h * 128, (h + 1) * 128)
            t = (a2[:, cols] + sq[:, cols]) + sqmu[...]
            logit = lpb[...] - beta * t
            m = jnp.max(logit, axis=0, keepdims=True)
            e = jnp.exp(logit - m)
            r = jnp.sum(e, axis=0, keepdims=True)
            p_ref[b, :, cols] = e
            mx_ref[b, :, cols] = m
            st_own[par, grp, j, :, cols] = m + jnp.log(r)

    def st_copy(grp, par, i):
        return remote(st_own.at[par, grp], st_rem.at[par, grp, i],
                      st_s.at[grp], st_r.at[par, grp], peers[i])

    def send_stats(grp, par):
        for i in range(3):
            st_copy(grp, par, i).start()

    def wait_stats(grp, par):
        three = st_rem.at[par, grp]
        both = remote(three, three, st_s.at[grp], st_r.at[par, grp], sib)
        both.wait_recv()
        both.wait_send()

    def resp(grp, par):
        st = [st_own[par, grp]] + [st_rem[par, grp, i] for i in range(3)]
        top = jnp.maximum(jnp.maximum(st[0], st[1]), jnp.maximum(st[2], st[3]))
        es = [jnp.exp(v - top) for v in st]
        tot = (es[0] + es[1]) + (es[2] + es[3])
        lse = top + jnp.log(tot)
        first = pl.multiple_of(grp * GRP, GRP)
        scale = jnp.exp(mx_ref[pl.ds(first, GRP)] - top) / tot
        cnt = nacc[...]
        for j in range(GRP):
            lse_ref[:, pl.ds(pl.multiple_of((grp * GRP + j) * BLK, BLK), BLK)] = lse[j]
            rj = p_ref[grp * GRP + j] * scale[j]
            cnt = cnt + (rj[:, 0:128] + rj[:, 128:256])
            rb[grp % 2, :, j * BLK:(j + 1) * BLK] = rj.astype(BF16)
        nacc[...] = cnt

    def gather(grp):
        rows = pl.ds(pl.multiple_of(grp * (GRP * BLK), GRP * BLK), GRP * BLK)
        s_ref[...] += jnp.dot(rb[grp % 2], xb[rows, :], preferred_element_type=F32)

    def mstep(grp, par):
        wait_stats(grp, par)
        resp(grp, par)
        gather(grp)

    def zero_sums():
        nacc[...] = jnp.zeros_like(nacc)
        s_ref[...] = jnp.zeros_like(s_ref)

    def finish_sweep():
        n = jnp.sum(nacc[...], axis=1, keepdims=True)
        lp = jnp.log((n + PRIOR_ALPHA) / (ROWS + 4 * KC * PRIOR_ALPHA))
        lpb[...] = jnp.broadcast_to(lp, (KC, 128))
        mu = s_ref[...] * (1.0 / (n + EPS_COUNT))
        mu_out[side, pl.ds(cbase, KC), :] = mu
        set_means(mu)

    zero_sums()
    beta0 = beta_ref[0]

    def first_block(b):
        prep(b)
        soft(b, cross(xt_ref[b // 2, :, pl.ds(pl.multiple_of(b % 2 * BLK, BLK), BLK)]), beta0, 0)

        @pl.when(b % GRP == GRP - 1)
        def _():
            send_stats(b // GRP, 0)

    def own_block(n):
        @pl.when((n >= 8) & (n % 2 == 0))
        def _():
            own_copy((n - 8) // 2).wait_recv()

        first_block((core * 8 + n) % 16)

    ld_x.wait()

    @pl.loop(0, 4)
    def _(n):
        own_block(n)

    @pl.loop(0, NCH + 4)
    def _(it):
        @pl.when(it < NCH - 1)
        def _():
            x_copy(it).wait_recv()
            y_copy(it).start()

        @pl.when((it >= 3) & (it < NCH + 2))
        def _():
            y_copy(it - 3).wait_recv()
            d_copy(it - 3).start()

        @pl.when(it == NCH + 1)
        def _():
            x_copy(NCH - 1).wait_recv()
            x_copy(NCH).wait_recv()
            d_copy(NCH - 1).start()

        @pl.when(it < 4)
        def _():
            @pl.loop(0, 2)
            def _(k):
                own_block(4 + 2 * it + k)

        @pl.when((it >= 4) & (it < 8))
        def _():
            own_block(8 + it)

        @pl.when(it >= 4)
        def _():
            d_copy(it - 4).wait_recv()
            first_block(NBLK // 2 + it - 4)

        @pl.when((it >= 9) & (it < 15))
        def _():
            mstep(it - 9, 0)

    mstep(NGRP - 2, 0)
    mstep(NGRP - 1, 0)
    finish_sweep()

    def all_sent(n, sem):
        ref = xb.at[pl.ds(0, n), :]
        remote(ref, ref, sem, own_r.at[0], sib).wait_send()

    all_sent(SHARD, own_s)
    all_sent((NCH + 1) * Z, xs)
    all_sent((NCH - 1) * Z, ys)
    all_sent(NCH * 2 * Z, ds)

    def block(s, q):
        return mu_out.at[s, pl.ds(cbase + q * QC, QC), :]

    def whole(s):
        return mu_out.at[s, pl.ds(cbase, KC), :]

    def fx_copy(q):
        ref = block(side, q)
        return remote(ref, ref, fxs, fxr.at[q], xpt)

    def relay(q):
        ref = block(1 - side, q)
        return remote(ref, ref, frs, frr, sib)

    slot = side * 2 + core
    lp_devs = (sib, xpt, xdg)
    lse_copy = remote(lse_snd, lse_rcv, ls_s, ls_r, xpt)

    def send_small():
        lpbuf[slot] = jnp.transpose(lpb[...])[0:1, :]
        halves = ([], [])
        for g in range(NCH):
            piece = lse_ref[:, pl.ds(pl.multiple_of(OWN + g * (4 * Z) + core * (2 * Z), 128), 128)]
            halves[0].append(piece[:, 0:Z])
            halves[1].append(piece[:, Z:2 * Z])
        lse_snd[...] = jnp.concatenate(halves[0] + halves[1], axis=1)
        lse_out[pl.ds(side, 1), :] = lse_ref[:, pl.ds(pl.multiple_of(core * SHARD, SHARD), SHARD)]
        lse_copy.start()
        for i in range(3):
            remote(lpbuf.at[slot], lpbuf.at[slot], lps, lpr, lp_devs[i]).start()

    @pl.loop(1, SWEEPS)
    def _(t):
        par = t % 2
        beta = beta_ref[t]
        zero_sums()
        @pl.loop(0, NBLK // 8)
        def _(i):
            for k in range(4):
                a2 = cross(xt_ref[4 * i + k])
                for h in range(2):
                    soft(8 * i + 2 * k + h, a2[:, h * BLK:(h + 1) * BLK], beta, par)
            for g in range(8 // GRP):
                send_stats(i * (8 // GRP) + g, par)

        for g in range(NGRP):
            mstep(g, par)
        finish_sweep()

    send_small()
    for q in range(NQ):
        fx_copy(q).start()
    to_sib = remote(whole(side), whole(side), fds, fdr, sib)
    to_sib.start()

    lse_copy.wait()
    lse_out[pl.ds(1 - side, 1), :] = lse_rcv[...]
    remote(lpbuf.at[pl.ds(0, 3)], lpbuf.at[pl.ds(0, 3)], lps, lpr, sib).wait()
    for s in range(2):
        for c in range(2):
            lp_out[s:s + 1, c * KC:(c + 1) * KC] = lpbuf[s * 2 + c]

    for q in range(NQ):
        fx_copy(q).wait_recv()
        relay(q).start()

    to_sib.wait()
    remote(whole(1 - side), whole(1 - side), frs, frr, sib).wait()
    remote(whole(side), whole(side), fxs, frr, xpt).wait_send()


def write_out(mu_v, lp_v, lse_v, mu_o, lp_o, lse_o, sem):
    pairs = ((mu_v, mu_o), (lp_v, lp_o), (lse_v, lse_o))
    copies = [pltpu.make_async_copy(src, dst, sem.at[i]) for i, (src, dst) in enumerate(pairs)]
    for c in copies:
        c.start()
    for c in copies:
        c.wait()


def solution(mesh):
    def local_fit(x_local, mu_init, logpi_init, inv_temp):
        dma = pltpu.SemaphoreType.DMA
        vmem = pl.BlockSpec(memory_space=pltpu.VMEM)
        hbm = pl.BlockSpec(memory_space=pltpu.HBM)
        outs = [jax.ShapeDtypeStruct(mu_init.shape, F32),
                jax.ShapeDtypeStruct(logpi_init.shape, F32),
                jax.ShapeDtypeStruct((2, x_local.shape[0]), F32)]
        res = pl.pallas_call(
            body,
            out_shape=tuple(pltpu.VMEM(o.shape, o.dtype) for o in outs),
            in_specs=[hbm] * 4,
            out_specs=(vmem, vmem, vmem),
            scratch_shapes=[
                pltpu.VMEM((ROWS, HALF), BF16),
                pltpu.VMEM((NBLK // 2, HALF, 2 * BLK), BF16),
                pltpu.VMEM((NBLK, KC, BLK), F32),
                pltpu.VMEM((2, KC, GRP * BLK), BF16),
                pltpu.VMEM((PRE * Z, HALF), BF16),
                pltpu.VMEM((2, 2 * KC), F32),
                pltpu.SMEM((SWEEPS,), F32),
                pltpu.VMEM((KC, HALF), F32),
                pltpu.VMEM((KC, 128), F32),
                pltpu.VMEM((KC, HALF), F32),
                pltpu.VMEM((KC, HALF), BF16),
                pltpu.VMEM((KC, 128), F32),
                pltpu.VMEM((KC, 128), F32),
                pltpu.VMEM((NBLK, 1, BLK), F32),
                pltpu.VMEM((NBLK, 1, BLK), F32),
                pltpu.VMEM((1, ROWS), F32),
                pltpu.VMEM((2, NGRP, GRP, 1, BLK), F32),
                pltpu.VMEM((2, NGRP, 3, GRP, 1, BLK), F32),
                pltpu.VMEM((4, 1, KC), F32),
                pltpu.VMEM((1, SHARD), F32),
                pltpu.VMEM((1, SHARD), F32),
                dma((5,)),
                dma, dma((NCH + 1,)),
                dma, dma((NCH - 1,)),
                dma, dma((NCH,)),
                dma, dma((NOWN,)),
                dma((NGRP,)), dma((2, NGRP)),
                dma, dma,
                dma, dma,
                dma, dma((NQ,)),
                dma, dma,
                dma, dma,
            ],
            compiler_params=pltpu.CompilerParams(
                collective_id=0, has_side_effects=True,
                vmem_limit_bytes=56 * 1024 * 1024),
        )(x_local, mu_init, logpi_init, inv_temp)
        return pl.pallas_call(
            write_out,
            out_shape=tuple(outs),
            in_specs=[vmem] * 3,
            out_specs=(hbm,) * 3,
            scratch_shapes=[dma((3,))],
        )(*[pltpu.with_memory_space_constraint(r, pltpu.VMEM) for r in res])

    return jax.shard_map(
        local_fit,
        mesh=mesh,
        in_specs=(P(("grp", "row"), None), P(None, ("grp", "comp"), None), P(None, ("grp", "comp")), P()),
        out_specs=(P(None, ("grp", "comp"), None), P(None, ("grp", "comp")), P(None, ("grp", "row"))),
        check_vma=False,
    )
```

```python
import jax
import jax.numpy as jnp
from jax import lax
from jax.experimental import pallas as pl
from jax.experimental.pallas import tpu as pltpu
from jax.sharding import PartitionSpec as P

EPS_COUNT = 1e-6
PRIOR_ALPHA = 1e-3

F32 = jnp.float32
BF16 = jnp.bfloat16
MESH = pl.DeviceIdType.MESH

SWEEPS = 3
HALF = 512
SHARD = 2048
ROWS = 8192
KC = 256
BLK = 256
NBLK = ROWS // BLK
GRP = 4
NGRP = NBLK // GRP
NCH = 16
Z = SHARD // 2 // NCH
PRE = 4
NOWN = 4
PIECE = SHARD // NOWN
OWN = 2 * SHARD
NQ = 4
QC = KC // NQ


def body(x_hbm, mu_hbm, lp_hbm, beta_hbm,
         mu_out, lp_out, lse_out,
         xb, xt_ref, p_ref, rb, xpre, lp_in, beta_ref, s_ref, nacc, mu_f, mu2, sqmu, lpb, sqx, mx_ref, lse_ref,
         st_own, st_rem, lpbuf, lse_snd, lse_rcv,
         loc_sem, xs, xr, ys, yr, ds, dr, own_s, own_r,
         st_s, st_r, lps, lpr, ls_s, ls_r, fxs, fxr, fds, fdr, frs, frr):
    comp = lax.axis_index("comp")
    row = lax.axis_index("row")
    side = row // 2
    core = row % 2
    sib = {"row": side * 2 + (1 - core)}
    ypt = {"comp": 1 - comp}
    ydg = {"comp": 1 - comp, "row": side * 2 + (1 - core)}
    xpt = {"row": (1 - side) * 2 + core}
    xdg = {"row": (1 - side) * 2 + (1 - core)}
    peers = (sib, ypt, ydg)

    barrier = pltpu.get_barrier_semaphore()
    for dev in (xpt, sib, ypt, ydg, xdg):
        pl.semaphore_signal(barrier, inc=1, device_id=dev, device_id_type=MESH)

    def remote(src, dst, ssem, rsem, dev):
        return pltpu.make_async_remote_copy(
            src_ref=src, dst_ref=dst, send_sem=ssem, recv_sem=rsem,
            device_id=dev, device_id_type=MESH)

    fit_cols = pl.ds(pl.multiple_of(side * HALF, HALF), HALF)
    oth_cols = pl.ds(pl.multiple_of((1 - side) * HALF, HALF), HALF)
    cbase = pl.multiple_of(core * KC, KC)

    def own_rows(c):
        return xb.at[pl.ds(pl.multiple_of(c * SHARD, SHARD), SHARD), :]

    ld_x = pltpu.make_async_copy(x_hbm.at[:, fit_cols], own_rows(core), loc_sem.at[0])
    ld_mu = pltpu.make_async_copy(mu_hbm.at[side, pl.ds(cbase, KC), :], mu_f, loc_sem.at[1])
    ld_pre = pltpu.make_async_copy(
        x_hbm.at[pl.ds(pl.multiple_of(comp * (SHARD // 2), PRE * Z), PRE * Z), oth_cols],
        xpre, loc_sem.at[2])
    ld_lp = pltpu.make_async_copy(lp_hbm, lp_in, loc_sem.at[3])
    ld_beta = pltpu.make_async_copy(beta_hbm, beta_ref, loc_sem.at[4])
    ld_pre.start()
    ld_mu.start()
    ld_lp.start()
    ld_beta.start()
    ld_x.start()

    def place(g, c, half, n):
        return xb.at[pl.ds(pl.multiple_of(OWN + g * (4 * Z) + c * (2 * Z) + half * Z, Z), n), :]

    def x_copy(g):
        extra = g // NCH
        g0 = g - extra
        half = comp + extra * (1 - 2 * comp)
        src = x_hbm.at[pl.ds(pl.multiple_of(half * (SHARD // 2) + g0 * Z, Z), Z), oth_cols]
        return remote(src, place(g0, core, half, Z), xs, xr.at[g], xpt)

    def y_copy(g):
        ref = place(g, core, comp, Z)
        return remote(ref, ref, ys, yr.at[g], ypt)

    def d_copy(g):
        ref = place(g, core, 0, 2 * Z)
        return remote(ref, ref, ds, dr.at[g], sib)

    def own_copy(k):
        src = x_hbm.at[pl.ds(pl.multiple_of(k * PIECE, PIECE), PIECE), fit_cols]
        dst = xb.at[pl.ds(pl.multiple_of(core * SHARD + k * PIECE, PIECE), PIECE), :]
        return remote(src, dst, own_s, own_r.at[k], sib)

    pl.semaphore_wait(barrier, 5)
    ld_pre.wait()
    for g in range(PRE):
        remote(xpre.at[pl.ds(g * Z, Z), :], place(g, core, comp, Z), xs, xr.at[g], xpt).start()
    for k in range(NOWN):
        own_copy(k).start()

    @pl.loop(PRE, NCH + 1)
    def _(g):
        x_copy(g).start()

    def bc(row_vec):
        return jnp.transpose(jnp.broadcast_to(row_vec, (128, KC)))

    def set_means(mu):
        mu2[...] = mu.astype(BF16) * jnp.asarray(-2.0, BF16)
        sqmu[...] = jnp.broadcast_to(jnp.sum(mu * mu, axis=1, keepdims=True), (KC, 128))

    ld_lp.wait()
    ld_beta.wait()
    lpb[...] = bc(lp_in[pl.ds(side, 1), pl.ds(cbase, KC)])
    ld_mu.wait()
    set_means(mu_f[...])

    def prep(b):
        xt = jnp.transpose(xb[pl.ds(pl.multiple_of(b * BLK, BLK), BLK), :])
        xt_ref[b // 2, :, pl.ds(pl.multiple_of(b % 2 * BLK, BLK), BLK)] = xt
        xf = xt.astype(F32)
        sqx[b] = jnp.sum(xf * xf, axis=0, keepdims=True)

    def cross(xt):
        return jnp.dot(mu2[...], xt, preferred_element_type=F32)

    def soft(b, a2, beta, par):
        sq = sqx[b]
        grp = b // GRP
        j = b % GRP
        for h in range(BLK // 128):
            cols = slice(h * 128, (h + 1) * 128)
            t = (a2[:, cols] + sq[:, cols]) + sqmu[...]
            logit = lpb[...] - beta * t
            m = jnp.max(logit, axis=0, keepdims=True)
            e = jnp.exp(logit - m)
            r = jnp.sum(e, axis=0, keepdims=True)
            p_ref[b, :, cols] = e
            mx_ref[b, :, cols] = m
            st_own[par, grp, j, :, cols] = m + jnp.log(r)

    def send_stats(grp, par, n):
        own = st_own.at[par, pl.ds(grp, n)]
        for i in range(3):
            remote(own, st_rem.at[par, i, pl.ds(grp, n)], st_s, st_r.at[par, grp], peers[i]).start()

    def wait_stats(grp, par, n):
        three = st_rem.at[par, :, pl.ds(grp, n)]
        remote(three, three, st_s, st_r.at[par, grp], sib).wait_recv()

    def stats_sent(par):
        remote(st_rem.at[par], st_rem.at[par], st_s, st_r.at[par, 0], sib).wait_send()

    def resp(grp, par):
        st = [st_own[par, grp]] + [st_rem[par, i, grp] for i in range(3)]
        top = jnp.maximum(jnp.maximum(st[0], st[1]), jnp.maximum(st[2], st[3]))
        es = [jnp.exp(v - top) for v in st]
        tot = (es[0] + es[1]) + (es[2] + es[3])
        lse = top + jnp.log(tot)
        first = pl.multiple_of(grp * GRP, GRP)
        scale = jnp.exp(mx_ref[pl.ds(first, GRP)] - top) / tot
        cnt = nacc[...]
        for j in range(GRP):
            lse_ref[:, pl.ds(pl.multiple_of((grp * GRP + j) * BLK, BLK), BLK)] = lse[j]
            rj = p_ref[grp * GRP + j] * scale[j]
            cnt = cnt + (rj[:, 0:128] + rj[:, 128:256])
            rb[grp % 2, :, j * BLK:(j + 1) * BLK] = rj.astype(BF16)
        nacc[...] = cnt

    def gather(grp):
        rows = pl.ds(pl.multiple_of(grp * (GRP * BLK), GRP * BLK), GRP * BLK)
        s_ref[...] += jnp.dot(rb[grp % 2], xb[rows, :], preferred_element_type=F32)

    def mstep(grp, par, n=1):
        if n:
            wait_stats(grp, par, n)
        resp(grp, par)
        gather(grp)

    def zero_sums():
        nacc[...] = jnp.zeros_like(nacc)
        s_ref[...] = jnp.zeros_like(s_ref)

    def finish_sweep():
        n = jnp.sum(nacc[...], axis=1, keepdims=True)
        lp = jnp.log((n + PRIOR_ALPHA) / (ROWS + 4 * KC * PRIOR_ALPHA))
        lpb[...] = jnp.broadcast_to(lp, (KC, 128))
        mu = s_ref[...] * (1.0 / (n + EPS_COUNT))
        mu_out[side, pl.ds(cbase, KC), :] = mu
        set_means(mu)

    zero_sums()
    beta0 = beta_ref[0]

    def first_block(b):
        prep(b)
        soft(b, cross(xt_ref[b // 2, :, pl.ds(pl.multiple_of(b % 2 * BLK, BLK), BLK)]), beta0, 0)

        @pl.when(b % GRP == GRP - 1)
        def _():
            send_stats(b // GRP, 0, 1)

    def own_block(n):
        @pl.when((n >= 8) & (n % 2 == 0))
        def _():
            own_copy((n - 8) // 2).wait_recv()

        first_block((core * 8 + n) % 16)

    ld_x.wait()

    @pl.loop(0, 4)
    def _(n):
        own_block(n)

    @pl.loop(0, NCH + 4)
    def _(it):
        @pl.when(it < NCH - 1)
        def _():
            x_copy(it).wait_recv()
            y_copy(it).start()

        @pl.when((it >= 3) & (it < NCH + 2))
        def _():
            y_copy(it - 3).wait_recv()
            d_copy(it - 3).start()

        @pl.when(it == NCH + 1)
        def _():
            x_copy(NCH - 1).wait_recv()
            x_copy(NCH).wait_recv()
            d_copy(NCH - 1).start()

        @pl.when(it < 4)
        def _():
            @pl.loop(0, 2)
            def _(k):
                own_block(4 + 2 * it + k)

        @pl.when((it >= 4) & (it < 8))
        def _():
            own_block(8 + it)

        @pl.when(it >= 4)
        def _():
            d_copy(it - 4).wait_recv()
            first_block(NBLK // 2 + it - 4)

        @pl.when((it >= 9) & (it < 15))
        def _():
            mstep(it - 9, 0)

    mstep(NGRP - 2, 0)
    mstep(NGRP - 1, 0)
    stats_sent(0)
    finish_sweep()

    def all_sent(n, sem):
        ref = xb.at[pl.ds(0, n), :]
        remote(ref, ref, sem, own_r.at[0], sib).wait_send()

    all_sent(SHARD, own_s)
    all_sent((NCH + 1) * Z, xs)
    all_sent((NCH - 1) * Z, ys)
    all_sent(NCH * 2 * Z, ds)

    def block(s, q):
        return mu_out.at[s, pl.ds(cbase + q * QC, QC), :]

    def whole(s):
        return mu_out.at[s, pl.ds(cbase, KC), :]

    def fx_copy(q):
        ref = block(side, q)
        return remote(ref, ref, fxs, fxr.at[q], xpt)

    def relay(q):
        ref = block(1 - side, q)
        return remote(ref, ref, frs, frr, sib)

    slot = side * 2 + core
    lp_devs = (sib, xpt, xdg)
    lse_copy = remote(lse_snd, lse_rcv, ls_s, ls_r, xpt)

    def send_small():
        lpbuf[slot] = jnp.transpose(lpb[...])[0:1, :]
        halves = ([], [])
        for g in range(NCH):
            piece = lse_ref[:, pl.ds(pl.multiple_of(OWN + g * (4 * Z) + core * (2 * Z), 128), 128)]
            halves[0].append(piece[:, 0:Z])
            halves[1].append(piece[:, Z:2 * Z])
        lse_snd[...] = jnp.concatenate(halves[0] + halves[1], axis=1)
        lse_out[pl.ds(side, 1), :] = lse_ref[:, pl.ds(pl.multiple_of(core * SHARD, SHARD), SHARD)]
        lse_copy.start()
        for i in range(3):
            remote(lpbuf.at[slot], lpbuf.at[slot], lps, lpr, lp_devs[i]).start()

    @pl.loop(1, SWEEPS)
    def _(t):
        par = t % 2
        beta = beta_ref[t]
        zero_sums()
        @pl.loop(0, NBLK // 8)
        def _(i):
            for k in range(4):
                a2 = cross(xt_ref[4 * i + k])
                for h in range(2):
                    soft(8 * i + 2 * k + h, a2[:, h * BLK:(h + 1) * BLK], beta, par)
            send_stats(2 * i, par, 2)

        for g in range(NGRP):
            mstep(g, par, 2 * (1 - g % 2))
        stats_sent(par)
        finish_sweep()

    send_small()
    for q in range(NQ):
        fx_copy(q).start()
    to_sib = remote(whole(side), whole(side), fds, fdr, sib)
    to_sib.start()

    lse_copy.wait()
    lse_out[pl.ds(1 - side, 1), :] = lse_rcv[...]
    remote(lpbuf.at[pl.ds(0, 3)], lpbuf.at[pl.ds(0, 3)], lps, lpr, sib).wait()
    for s in range(2):
        for c in range(2):
            lp_out[s:s + 1, c * KC:(c + 1) * KC] = lpbuf[s * 2 + c]

    for q in range(NQ):
        fx_copy(q).wait_recv()
        relay(q).start()

    to_sib.wait()
    remote(whole(1 - side), whole(1 - side), frs, frr, sib).wait()
    remote(whole(side), whole(side), fxs, frr, xpt).wait_send()


def write_out(mu_v, lp_v, lse_v, mu_o, lp_o, lse_o, sem):
    pairs = ((mu_v, mu_o), (lp_v, lp_o), (lse_v, lse_o))
    copies = [pltpu.make_async_copy(src, dst, sem.at[i]) for i, (src, dst) in enumerate(pairs)]
    for c in copies:
        c.start()
    for c in copies:
        c.wait()


def solution(mesh):
    def local_fit(x_local, mu_init, logpi_init, inv_temp):
        dma = pltpu.SemaphoreType.DMA
        vmem = pl.BlockSpec(memory_space=pltpu.VMEM)
        hbm = pl.BlockSpec(memory_space=pltpu.HBM)
        outs = [jax.ShapeDtypeStruct(mu_init.shape, F32),
                jax.ShapeDtypeStruct(logpi_init.shape, F32),
                jax.ShapeDtypeStruct((2, x_local.shape[0]), F32)]
        res = pl.pallas_call(
            body,
            out_shape=tuple(pltpu.VMEM(o.shape, o.dtype) for o in outs),
            in_specs=[hbm] * 4,
            out_specs=(vmem, vmem, vmem),
            scratch_shapes=[
                pltpu.VMEM((ROWS, HALF), BF16),
                pltpu.VMEM((NBLK // 2, HALF, 2 * BLK), BF16),
                pltpu.VMEM((NBLK, KC, BLK), F32),
                pltpu.VMEM((2, KC, GRP * BLK), BF16),
                pltpu.VMEM((PRE * Z, HALF), BF16),
                pltpu.VMEM((2, 2 * KC), F32),
                pltpu.SMEM((SWEEPS,), F32),
                pltpu.VMEM((KC, HALF), F32),
                pltpu.VMEM((KC, 128), F32),
                pltpu.VMEM((KC, HALF), F32),
                pltpu.VMEM((KC, HALF), BF16),
                pltpu.VMEM((KC, 128), F32),
                pltpu.VMEM((KC, 128), F32),
                pltpu.VMEM((NBLK, 1, BLK), F32),
                pltpu.VMEM((NBLK, 1, BLK), F32),
                pltpu.VMEM((1, ROWS), F32),
                pltpu.VMEM((2, NGRP, GRP, 1, BLK), F32),
                pltpu.VMEM((2, 3, NGRP, GRP, 1, BLK), F32),
                pltpu.VMEM((4, 1, KC), F32),
                pltpu.VMEM((1, SHARD), F32),
                pltpu.VMEM((1, SHARD), F32),
                dma((5,)),
                dma, dma((NCH + 1,)),
                dma, dma((NCH - 1,)),
                dma, dma((NCH,)),
                dma, dma((NOWN,)),
                dma, dma((2, NGRP)),
                dma, dma,
                dma, dma,
                dma, dma((NQ,)),
                dma, dma,
                dma, dma,
            ],
            compiler_params=pltpu.CompilerParams(
                collective_id=0, has_side_effects=True,
                vmem_limit_bytes=56 * 1024 * 1024),
        )(x_local, mu_init, logpi_init, inv_temp)
        return pl.pallas_call(
            write_out,
            out_shape=tuple(outs),
            in_specs=[vmem] * 3,
            out_specs=(hbm,) * 3,
            scratch_shapes=[dma((3,))],
        )(*[pltpu.with_memory_space_constraint(r, pltpu.VMEM) for r in res])

    return jax.shard_map(
        local_fit,
        mesh=mesh,
        in_specs=(P(("grp", "row"), None), P(None, ("grp", "comp"), None), P(None, ("grp", "comp")), P()),
        out_specs=(P(None, ("grp", "comp"), None), P(None, ("grp", "comp")), P(None, ("grp", "row"))),
        check_vma=False,
    )
```

```python
import jax
import jax.numpy as jnp
from jax import lax
from jax.experimental import pallas as pl
from jax.experimental.pallas import tpu as pltpu
from jax.sharding import PartitionSpec as P

EPS_COUNT = 1e-6
PRIOR_ALPHA = 1e-3

F32 = jnp.float32
BF16 = jnp.bfloat16
MESH = pl.DeviceIdType.MESH

SWEEPS = 3
HALF = 512
SHARD = 2048
ROWS = 8192
KC = 256
BLK = 256
NBLK = ROWS // BLK
GRP = 4
NGRP = NBLK // GRP
NCH = 16
Z = SHARD // 2 // NCH
PRE = 4
NOWN = 4
PIECE = SHARD // NOWN
OWN = 2 * SHARD
NQ = 4
QC = KC // NQ


def body(x_hbm, mu_hbm, lp_hbm, beta_hbm,
         mu_out, lp_out, lse_out,
         xb, xt_ref, p_ref, rb, xpre, lp_in, beta_ref, s_ref, nacc, mu_f, mu2, sqmu, lpb, sqx, mx_ref, lse_ref,
         st_own, st_rem, lpbuf, lse_snd, lse_rcv,
         loc_sem, xs, xr, ys, yr, ds, dr, own_s, own_r,
         st_s, st_r, lps, lpr, ls_s, ls_r, fxs, fxr, fds, fdr, frs, frr):
    comp = lax.axis_index("comp")
    row = lax.axis_index("row")
    side = row // 2
    core = row % 2
    sib = {"row": side * 2 + (1 - core)}
    ypt = {"comp": 1 - comp}
    ydg = {"comp": 1 - comp, "row": side * 2 + (1 - core)}
    xpt = {"row": (1 - side) * 2 + core}
    xdg = {"row": (1 - side) * 2 + (1 - core)}
    peers = (sib, ypt, ydg)

    barrier = pltpu.get_barrier_semaphore()
    for dev in (xpt, sib, ypt, ydg, xdg):
        pl.semaphore_signal(barrier, inc=1, device_id=dev, device_id_type=MESH)

    def remote(src, dst, ssem, rsem, dev):
        return pltpu.make_async_remote_copy(
            src_ref=src, dst_ref=dst, send_sem=ssem, recv_sem=rsem,
            device_id=dev, device_id_type=MESH)

    fit_cols = pl.ds(pl.multiple_of(side * HALF, HALF), HALF)
    oth_cols = pl.ds(pl.multiple_of((1 - side) * HALF, HALF), HALF)
    cbase = pl.multiple_of(core * KC, KC)

    def own_rows(c):
        return xb.at[pl.ds(pl.multiple_of(c * SHARD, SHARD), SHARD), :]

    ld_x = pltpu.make_async_copy(x_hbm.at[:, fit_cols], own_rows(core), loc_sem.at[0])
    ld_mu = pltpu.make_async_copy(mu_hbm.at[side, pl.ds(cbase, KC), :], mu_f, loc_sem.at[1])
    ld_pre = pltpu.make_async_copy(
        x_hbm.at[pl.ds(pl.multiple_of(comp * (SHARD // 2), PRE * Z), PRE * Z), oth_cols],
        xpre, loc_sem.at[2])
    ld_lp = pltpu.make_async_copy(lp_hbm, lp_in, loc_sem.at[3])
    ld_beta = pltpu.make_async_copy(beta_hbm, beta_ref, loc_sem.at[4])
    ld_pre.start()
    ld_mu.start()
    ld_lp.start()
    ld_beta.start()
    ld_x.start()

    def place(g, c, half, n):
        return xb.at[pl.ds(pl.multiple_of(OWN + g * (4 * Z) + c * (2 * Z) + half * Z, Z), n), :]

    def x_copy(g):
        extra = g // NCH
        g0 = g - extra
        half = comp + extra * (1 - 2 * comp)
        src = x_hbm.at[pl.ds(pl.multiple_of(half * (SHARD // 2) + g0 * Z, Z), Z), oth_cols]
        return remote(src, place(g0, core, half, Z), xs, xr.at[g], xpt)

    def y_copy(g):
        ref = place(g, core, comp, Z)
        return remote(ref, ref, ys, yr.at[g], ypt)

    def d_copy(g):
        ref = place(g, core, 0, 2 * Z)
        return remote(ref, ref, ds, dr.at[g], sib)

    def own_copy(k):
        src = x_hbm.at[pl.ds(pl.multiple_of(k * PIECE, PIECE), PIECE), fit_cols]
        dst = xb.at[pl.ds(pl.multiple_of(core * SHARD + k * PIECE, PIECE), PIECE), :]
        return remote(src, dst, own_s, own_r.at[k], sib)

    pl.semaphore_wait(barrier, 5)
    ld_pre.wait()
    for g in range(PRE):
        remote(xpre.at[pl.ds(g * Z, Z), :], place(g, core, comp, Z), xs, xr.at[g], xpt).start()
    for k in range(NOWN):
        own_copy(k).start()

    @pl.loop(PRE, NCH + 1)
    def _(g):
        x_copy(g).start()

    def bc(row_vec):
        return jnp.transpose(jnp.broadcast_to(row_vec, (128, KC)))

    def set_means(mu):
        mu2[...] = mu.astype(BF16) * jnp.asarray(-2.0, BF16)
        sqmu[...] = jnp.broadcast_to(jnp.sum(mu * mu, axis=1, keepdims=True), (KC, 128))

    ld_lp.wait()
    ld_beta.wait()
    lpb[...] = bc(lp_in[pl.ds(side, 1), pl.ds(cbase, KC)])
    ld_mu.wait()
    set_means(mu_f[...])

    def prep(b):
        xt = jnp.transpose(xb[pl.ds(pl.multiple_of(b * BLK, BLK), BLK), :])
        xt_ref[b // 2, :, pl.ds(pl.multiple_of(b % 2 * BLK, BLK), BLK)] = xt
        xf = xt.astype(F32)
        sqx[b] = jnp.sum(xf * xf, axis=0, keepdims=True)

    def cross(xt):
        return jnp.dot(mu2[...], xt, preferred_element_type=F32)

    def soft(b, a2, beta, par):
        sq = sqx[b]
        grp = b // GRP
        j = b % GRP
        for h in range(BLK // 128):
            cols = slice(h * 128, (h + 1) * 128)
            t = (a2[:, cols] + sq[:, cols]) + sqmu[...]
            logit = lpb[...] - beta * t
            m = jnp.max(logit, axis=0, keepdims=True)
            e = jnp.exp(logit - m)
            r = jnp.sum(e, axis=0, keepdims=True)
            p_ref[b, :, cols] = e
            mx_ref[b, :, cols] = m
            st_own[par, grp, j, :, cols] = m + jnp.log(r)

    def send_stats(grp, par, n):
        own = st_own.at[par, pl.ds(grp, n)]
        for i in range(3):
            remote(own, st_rem.at[par, i, pl.ds(grp, n)], st_s, st_r.at[par, grp], peers[i]).start()

    def wait_stats(grp, par, n):
        three = st_rem.at[par, :, pl.ds(grp, n)]
        remote(three, three, st_s, st_r.at[par, grp], sib).wait_recv()

    def stats_sent(par):
        remote(st_rem.at[par], st_rem.at[par], st_s, st_r.at[par, 0], sib).wait_send()

    def resp(grp, par):
        st = [st_own[par, grp]] + [st_rem[par, i, grp] for i in range(3)]
        top = jnp.maximum(jnp.maximum(st[0], st[1]), jnp.maximum(st[2], st[3]))
        es = [jnp.exp(v - top) for v in st]
        tot = (es[0] + es[1]) + (es[2] + es[3])
        lse = top + jnp.log(tot)
        first = pl.multiple_of(grp * GRP, GRP)
        scale = jnp.exp(mx_ref[pl.ds(first, GRP)] - top) / tot
        cnt = nacc[...]
        for j in range(GRP):
            lse_ref[:, pl.ds(pl.multiple_of((grp * GRP + j) * BLK, BLK), BLK)] = lse[j]
            rj = p_ref[grp * GRP + j] * scale[j]
            cnt = cnt + (rj[:, 0:128] + rj[:, 128:256])
            rb[grp % 2, :, j * BLK:(j + 1) * BLK] = rj.astype(BF16)
        nacc[...] = cnt

    def gather(grp):
        rows = pl.ds(pl.multiple_of(grp * (GRP * BLK), GRP * BLK), GRP * BLK)
        s_ref[...] += jnp.dot(rb[grp % 2], xb[rows, :], preferred_element_type=F32)

    def mstep(grp, par, n=1):
        if n:
            wait_stats(grp, par, n)
        resp(grp, par)
        gather(grp)

    def zero_sums():
        nacc[...] = jnp.zeros_like(nacc)
        s_ref[...] = jnp.zeros_like(s_ref)

    def finish_sweep():
        n = jnp.sum(nacc[...], axis=1, keepdims=True)
        lp = jnp.log((n + PRIOR_ALPHA) / (ROWS + 4 * KC * PRIOR_ALPHA))
        lpb[...] = jnp.broadcast_to(lp, (KC, 128))
        mu = s_ref[...] * (1.0 / (n + EPS_COUNT))
        mu_out[side, pl.ds(cbase, KC), :] = mu

    zero_sums()
    beta0 = beta_ref[0]

    def first_block(b):
        prep(b)
        soft(b, cross(xt_ref[b // 2, :, pl.ds(pl.multiple_of(b % 2 * BLK, BLK), BLK)]), beta0, 0)

    def own_block(n):
        @pl.when((n >= 8) & (n % 2 == 0))
        def _():
            own_copy((n - 8) // 2).wait_recv()

        first_block((core * 8 + n) % 16)

    ld_x.wait()

    @pl.loop(0, 4)
    def _(n):
        own_block(n)

    @pl.loop(0, NCH + 4)
    def _(it):
        @pl.when(it < NCH - 1)
        def _():
            x_copy(it).wait_recv()
            y_copy(it).start()

        @pl.when((it >= 3) & (it < NCH + 2))
        def _():
            y_copy(it - 3).wait_recv()
            d_copy(it - 3).start()

        @pl.when(it == NCH + 1)
        def _():
            x_copy(NCH - 1).wait_recv()
            x_copy(NCH).wait_recv()
            d_copy(NCH - 1).start()

        @pl.when(it < 4)
        def _():
            @pl.loop(0, 2)
            def _(k):
                own_block(4 + 2 * it + k)

        @pl.when((it >= 4) & (it < 8))
        def _():
            own_block(8 + it)

        @pl.when(it >= 4)
        def _():
            d_copy(it - 4).wait_recv()
            first_block(NBLK // 2 + it - 4)

        @pl.when(it == NCH - 2)
        def _():
            send_stats(0, 0, 4)
            send_stats(4, 0, 2)

        @pl.when(it == NCH - 1)
        def _():
            send_stats(6, 0, 1)

    send_stats(7, 0, 1)
    for g in range(NGRP):
        mstep(g, 0, {0: 4, 4: 2, 6: 1, 7: 1}.get(g, 0))
    stats_sent(0)
    finish_sweep()
    set_means(mu_out[side, pl.ds(cbase, KC), :])

    def all_sent(n, sem):
        ref = xb.at[pl.ds(0, n), :]
        remote(ref, ref, sem, own_r.at[0], sib).wait_send()

    all_sent(SHARD, own_s)
    all_sent((NCH + 1) * Z, xs)
    all_sent((NCH - 1) * Z, ys)
    all_sent(NCH * 2 * Z, ds)

    def block(s, q):
        return mu_out.at[s, pl.ds(cbase + q * QC, QC), :]

    def whole(s):
        return mu_out.at[s, pl.ds(cbase, KC), :]

    def fx_copy(q):
        ref = block(side, q)
        return remote(ref, ref, fxs, fxr.at[q], xpt)

    def relay(q):
        ref = block(1 - side, q)
        return remote(ref, ref, frs, frr, sib)

    slot = side * 2 + core
    lp_devs = (sib, xpt, xdg)
    lse_copy = remote(lse_snd, lse_rcv, ls_s, ls_r, xpt)

    def send_small():
        lpbuf[slot] = jnp.transpose(lpb[...])[0:1, :]
        halves = ([], [])
        for g in range(NCH):
            piece = lse_ref[:, pl.ds(pl.multiple_of(OWN + g * (4 * Z) + core * (2 * Z), 128), 128)]
            halves[0].append(piece[:, 0:Z])
            halves[1].append(piece[:, Z:2 * Z])
        lse_snd[...] = jnp.concatenate(halves[0] + halves[1], axis=1)
        lse_out[pl.ds(side, 1), :] = lse_ref[:, pl.ds(pl.multiple_of(core * SHARD, SHARD), SHARD)]
        lse_copy.start()
        for i in range(3):
            remote(lpbuf.at[slot], lpbuf.at[slot], lps, lpr, lp_devs[i]).start()

    @pl.loop(1, SWEEPS)
    def _(t):
        par = t % 2
        beta = beta_ref[t]
        zero_sums()
        @pl.loop(0, NBLK // 8)
        def _(i):
            for k in range(4):
                a2 = cross(xt_ref[4 * i + k])
                for h in range(2):
                    soft(8 * i + 2 * k + h, a2[:, h * BLK:(h + 1) * BLK], beta, par)
            send_stats(2 * i, par, 2)

        for g in range(NGRP):
            mstep(g, par, 2 * (1 - g % 2))
        finish_sweep()

        @pl.when(t < SWEEPS - 1)
        def _():
            set_means(mu_out[side, pl.ds(cbase, KC), :])

        stats_sent(par)

    fx_copy(0).start()
    send_small()
    for q in range(1, NQ):
        fx_copy(q).start()
    to_sib = remote(whole(side), whole(side), fds, fdr, sib)
    to_sib.start()

    lse_copy.wait()
    lse_out[pl.ds(1 - side, 1), :] = lse_rcv[...]
    remote(lpbuf.at[pl.ds(0, 3)], lpbuf.at[pl.ds(0, 3)], lps, lpr, sib).wait()
    for s in range(2):
        for c in range(2):
            lp_out[s:s + 1, c * KC:(c + 1) * KC] = lpbuf[s * 2 + c]

    for q in range(NQ):
        fx_copy(q).wait_recv()
        relay(q).start()

    to_sib.wait()
    remote(whole(1 - side), whole(1 - side), frs, frr, sib).wait()
    remote(whole(side), whole(side), fxs, frr, xpt).wait_send()


def write_out(mu_v, lp_v, lse_v, mu_o, lp_o, lse_o, sem):
    pairs = [(lp_v, lp_o), (lse_v, lse_o)]
    for s in range(2):
        for k in range(2):
            part = pl.ds(k * KC, KC)
            pairs.append((mu_v.at[s, part, :], mu_o.at[s, part, :]))
    copies = [pltpu.make_async_copy(src, dst, sem.at[i]) for i, (src, dst) in enumerate(pairs)]
    for c in copies:
        c.start()
    for c in copies:
        c.wait()


def solution(mesh):
    def local_fit(x_local, mu_init, logpi_init, inv_temp):
        dma = pltpu.SemaphoreType.DMA
        vmem = pl.BlockSpec(memory_space=pltpu.VMEM)
        hbm = pl.BlockSpec(memory_space=pltpu.HBM)
        outs = [jax.ShapeDtypeStruct(mu_init.shape, F32),
                jax.ShapeDtypeStruct(logpi_init.shape, F32),
                jax.ShapeDtypeStruct((2, x_local.shape[0]), F32)]
        res = pl.pallas_call(
            body,
            out_shape=tuple(pltpu.VMEM(o.shape, o.dtype) for o in outs),
            in_specs=[hbm] * 4,
            out_specs=(vmem, vmem, vmem),
            scratch_shapes=[
                pltpu.VMEM((ROWS, HALF), BF16),
                pltpu.VMEM((NBLK // 2, HALF, 2 * BLK), BF16),
                pltpu.VMEM((NBLK, KC, BLK), F32),
                pltpu.VMEM((2, KC, GRP * BLK), BF16),
                pltpu.VMEM((PRE * Z, HALF), BF16),
                pltpu.VMEM((2, 2 * KC), F32),
                pltpu.SMEM((SWEEPS,), F32),
                pltpu.VMEM((KC, HALF), F32),
                pltpu.VMEM((KC, 128), F32),
                pltpu.VMEM((KC, HALF), F32),
                pltpu.VMEM((KC, HALF), BF16),
                pltpu.VMEM((KC, 128), F32),
                pltpu.VMEM((KC, 128), F32),
                pltpu.VMEM((NBLK, 1, BLK), F32),
                pltpu.VMEM((NBLK, 1, BLK), F32),
                pltpu.VMEM((1, ROWS), F32),
                pltpu.VMEM((2, NGRP, GRP, 1, BLK), F32),
                pltpu.VMEM((2, 3, NGRP, GRP, 1, BLK), F32),
                pltpu.VMEM((4, 1, KC), F32),
                pltpu.VMEM((1, SHARD), F32),
                pltpu.VMEM((1, SHARD), F32),
                dma((5,)),
                dma, dma((NCH + 1,)),
                dma, dma((NCH - 1,)),
                dma, dma((NCH,)),
                dma, dma((NOWN,)),
                dma, dma((2, NGRP)),
                dma, dma,
                dma, dma,
                dma, dma((NQ,)),
                dma, dma,
                dma, dma,
            ],
            compiler_params=pltpu.CompilerParams(
                collective_id=0, has_side_effects=True,
                vmem_limit_bytes=56 * 1024 * 1024),
        )(x_local, mu_init, logpi_init, inv_temp)
        return pl.pallas_call(
            write_out,
            out_shape=tuple(outs),
            in_specs=[vmem] * 3,
            out_specs=(hbm,) * 3,
            scratch_shapes=[dma((6,))],
        )(*[pltpu.with_memory_space_constraint(r, pltpu.VMEM) for r in res])

    return jax.shard_map(
        local_fit,
        mesh=mesh,
        in_specs=(P(("grp", "row"), None), P(None, ("grp", "comp"), None), P(None, ("grp", "comp")), P()),
        out_specs=(P(None, ("grp", "comp"), None), P(None, ("grp", "comp")), P(None, ("grp", "row"))),
        check_vma=False,
    )
```

```python
import jax
import jax.numpy as jnp
from jax import lax
from jax.experimental import pallas as pl
from jax.experimental.pallas import tpu as pltpu
from jax.sharding import PartitionSpec as P

EPS_COUNT = 1e-6
PRIOR_ALPHA = 1e-3

F32 = jnp.float32
BF16 = jnp.bfloat16
MESH = pl.DeviceIdType.MESH

SWEEPS = 3
HALF = 512
SHARD = 2048
ROWS = 8192
KC = 256
BLK = 256
NBLK = ROWS // BLK
GRP = 4
NGRP = NBLK // GRP
NCH = 16
Z = SHARD // 2 // NCH
PRE = 4
NOWN = 4
PIECE = SHARD // NOWN
OWN = 2 * SHARD
NQ = 4
QC = KC // NQ


def body(x_hbm, mu_hbm, lp_hbm, beta_hbm,
         mu_out, lp_out, lse_out,
         xb, xt_ref, p_ref, rb, xpre, lp_in, beta_ref, s_ref, nacc, mu_f, mu2, sqmu, lpb, sqx, mx_ref, lse_ref,
         st_own, st_rem, lpbuf, lse_snd, lse_rcv,
         loc_sem, xs, xr, ys, yr, ds, dr, own_s, own_r,
         st_s, st_r, lps, lpr, ls_s, ls_r, fxs, fxr, fds, fdr, frs, frr):
    comp = lax.axis_index("comp")
    row = lax.axis_index("row")
    side = row // 2
    core = row % 2
    sib = {"row": side * 2 + (1 - core)}
    ypt = {"comp": 1 - comp}
    ydg = {"comp": 1 - comp, "row": side * 2 + (1 - core)}
    xpt = {"row": (1 - side) * 2 + core}
    xdg = {"row": (1 - side) * 2 + (1 - core)}
    peers = (sib, ypt, ydg)

    barrier = pltpu.get_barrier_semaphore()
    for dev in (xpt, sib, ypt, ydg, xdg):
        pl.semaphore_signal(barrier, inc=1, device_id=dev, device_id_type=MESH)

    def remote(src, dst, ssem, rsem, dev):
        return pltpu.make_async_remote_copy(
            src_ref=src, dst_ref=dst, send_sem=ssem, recv_sem=rsem,
            device_id=dev, device_id_type=MESH)

    fit_cols = pl.ds(pl.multiple_of(side * HALF, HALF), HALF)
    oth_cols = pl.ds(pl.multiple_of((1 - side) * HALF, HALF), HALF)
    cbase = pl.multiple_of(core * KC, KC)

    def own_rows(c):
        return xb.at[pl.ds(pl.multiple_of(c * SHARD, SHARD), SHARD), :]

    ld_x = pltpu.make_async_copy(x_hbm.at[:, fit_cols], own_rows(core), loc_sem.at[0])
    ld_mu = pltpu.make_async_copy(mu_hbm.at[side, pl.ds(cbase, KC), :], mu_f, loc_sem.at[1])
    ld_pre = pltpu.make_async_copy(
        x_hbm.at[pl.ds(pl.multiple_of(comp * (SHARD // 2), PRE * Z), PRE * Z), oth_cols],
        xpre, loc_sem.at[2])
    ld_lp = pltpu.make_async_copy(lp_hbm, lp_in, loc_sem.at[3])
    ld_beta = pltpu.make_async_copy(beta_hbm, beta_ref, loc_sem.at[4])
    ld_pre.start()
    ld_mu.start()
    ld_lp.start()
    ld_beta.start()
    ld_x.start()

    def place(g, c, half, n):
        return xb.at[pl.ds(pl.multiple_of(OWN + g * (4 * Z) + c * (2 * Z) + half * Z, Z), n), :]

    def x_copy(g):
        extra = g // NCH
        g0 = g - extra
        half = comp + extra * (1 - 2 * comp)
        src = x_hbm.at[pl.ds(pl.multiple_of(half * (SHARD // 2) + g0 * Z, Z), Z), oth_cols]
        return remote(src, place(g0, core, half, Z), xs, xr.at[g], xpt)

    def y_copy(g):
        ref = place(g, core, comp, Z)
        return remote(ref, ref, ys, yr.at[g], ypt)

    def d_copy(g):
        ref = place(g, core, 0, 2 * Z)
        return remote(ref, ref, ds, dr.at[g], sib)

    def own_copy(k):
        src = x_hbm.at[pl.ds(pl.multiple_of(k * PIECE, PIECE), PIECE), fit_cols]
        dst = xb.at[pl.ds(pl.multiple_of(core * SHARD + k * PIECE, PIECE), PIECE), :]
        return remote(src, dst, own_s, own_r.at[k], sib)

    pl.semaphore_wait(barrier, 5)
    ld_pre.wait()
    for g in range(PRE):
        remote(xpre.at[pl.ds(g * Z, Z), :], place(g, core, comp, Z), xs, xr.at[g], xpt).start()
    for k in range(NOWN):
        own_copy(k).start()

    @pl.loop(PRE, NCH + 1)
    def _(g):
        x_copy(g).start()

    def bc(row_vec):
        return jnp.transpose(jnp.broadcast_to(row_vec, (128, KC)))

    def set_means(mu):
        mu2[...] = mu.astype(BF16) * jnp.asarray(-2.0, BF16)
        sqmu[...] = jnp.broadcast_to(jnp.sum(mu * mu, axis=1, keepdims=True), (KC, 128))

    ld_lp.wait()
    ld_beta.wait()
    lpb[...] = bc(lp_in[pl.ds(side, 1), pl.ds(cbase, KC)])
    ld_mu.wait()
    set_means(mu_f[...])

    def prep(b):
        xt = jnp.transpose(xb[pl.ds(pl.multiple_of(b * BLK, BLK), BLK), :])
        xt_ref[b // 2, :, pl.ds(pl.multiple_of(b % 2 * BLK, BLK), BLK)] = xt
        xf = xt.astype(F32)
        sqx[b] = jnp.sum(xf * xf, axis=0, keepdims=True)

    def cross(xt):
        return jnp.dot(mu2[...], xt, preferred_element_type=F32)

    def soft(b, a2, beta, par):
        sq = sqx[b]
        grp = b // GRP
        j = b % GRP
        for h in range(BLK // 128):
            cols = slice(h * 128, (h + 1) * 128)
            t = (a2[:, cols] + sq[:, cols]) + sqmu[...]
            logit = lpb[...] - beta * t
            m = jnp.max(logit, axis=0, keepdims=True)
            e = jnp.exp(logit - m)
            r = jnp.sum(e, axis=0, keepdims=True)
            p_ref[b, :, cols] = e
            mx_ref[b, :, cols] = m
            st_own[par, grp, j, :, cols] = m + jnp.log(r)

    def send_stats(grp, par, n):
        own = st_own.at[par, pl.ds(grp, n)]
        for i in range(3):
            remote(own, st_rem.at[par, i, pl.ds(grp, n)], st_s, st_r.at[par, grp], peers[i]).start()

    def wait_stats(grp, par, n):
        three = st_rem.at[par, :, pl.ds(grp, n)]
        remote(three, three, st_s, st_r.at[par, grp], sib).wait_recv()

    def stats_sent(par):
        remote(st_rem.at[par], st_rem.at[par], st_s, st_r.at[par, 0], sib).wait_send()

    def resp(grp, par):
        st = [st_own[par, grp]] + [st_rem[par, i, grp] for i in range(3)]
        top = jnp.maximum(jnp.maximum(st[0], st[1]), jnp.maximum(st[2], st[3]))
        es = [jnp.exp(v - top) for v in st]
        tot = (es[0] + es[1]) + (es[2] + es[3])
        lse = top + jnp.log(tot)
        first = pl.multiple_of(grp * GRP, GRP)
        scale = jnp.exp(mx_ref[pl.ds(first, GRP)] - top) / tot
        cnt = nacc[...]
        for j in range(GRP):
            lse_ref[:, pl.ds(pl.multiple_of((grp * GRP + j) * BLK, BLK), BLK)] = lse[j]
            rj = p_ref[grp * GRP + j] * scale[j]
            cnt = cnt + (rj[:, 0:128] + rj[:, 128:256])
            rb[grp % 2, :, j * BLK:(j + 1) * BLK] = rj.astype(BF16)
        nacc[...] = cnt

    def gather(grp):
        rows = pl.ds(pl.multiple_of(grp * (GRP * BLK), GRP * BLK), GRP * BLK)
        s_ref[...] += jnp.dot(rb[grp % 2], xb[rows, :], preferred_element_type=F32)

    def mstep(grp, par, n=1):
        if n:
            wait_stats(grp, par, n)
        resp(grp, par)
        gather(grp)

    def zero_sums():
        nacc[...] = jnp.zeros_like(nacc)
        s_ref[...] = jnp.zeros_like(s_ref)

    def finish_sweep():
        n = jnp.sum(nacc[...], axis=1, keepdims=True)
        lp = jnp.log((n + PRIOR_ALPHA) / (ROWS + 4 * KC * PRIOR_ALPHA))
        lpb[...] = jnp.broadcast_to(lp, (KC, 128))
        mu = s_ref[...] * (1.0 / (n + EPS_COUNT))
        mu_out[side, pl.ds(cbase, KC), :] = mu

    zero_sums()
    beta0 = beta_ref[0]

    def first_block(b):
        prep(b)
        soft(b, cross(xt_ref[b // 2, :, pl.ds(pl.multiple_of(b % 2 * BLK, BLK), BLK)]), beta0, 0)

    def own_block(n):
        @pl.when((n >= 8) & (n % 2 == 0))
        def _():
            own_copy((n - 8) // 2).wait_recv()

        first_block((core * 8 + n) % 16)

    ld_x.wait()

    @pl.loop(0, 4)
    def _(n):
        own_block(n)

    @pl.loop(0, NCH + 4)
    def _(it):
        @pl.when(it < NCH - 1)
        def _():
            x_copy(it).wait_recv()
            y_copy(it).start()

        @pl.when(it == NCH + 1)
        def _():
            x_copy(NCH - 1).wait_recv()
            x_copy(NCH).wait_recv()
            d_copy(NCH - 1).start()

        @pl.when((it >= 3) & (it < NCH + 2))
        def _():
            y_copy(it - 3).wait_recv()
            d_copy(it - 3).start()

        @pl.when(it < 4)
        def _():
            @pl.loop(0, 2)
            def _(k):
                own_block(4 + 2 * it + k)

        @pl.when((it >= 4) & (it < 8))
        def _():
            own_block(8 + it)

        @pl.when(it >= 4)
        def _():
            g = it - 4 + (it // (NCH + 2)) * (1 - 2 * (it % 2))
            d_copy(g).wait_recv()
            first_block(NBLK // 2 + g)

        @pl.when(it == NCH - 2)
        def _():
            send_stats(0, 0, 4)
            send_stats(4, 0, 2)

        @pl.when(it == NCH - 1)
        def _():
            send_stats(6, 0, 1)

    send_stats(7, 0, 1)
    for g in range(NGRP):
        mstep(g, 0, {0: 4, 4: 2, 6: 1, 7: 1}.get(g, 0))
    stats_sent(0)
    finish_sweep()
    set_means(mu_out[side, pl.ds(cbase, KC), :])

    def all_sent(n, sem):
        ref = xb.at[pl.ds(0, n), :]
        remote(ref, ref, sem, own_r.at[0], sib).wait_send()

    all_sent(SHARD, own_s)
    all_sent((NCH + 1) * Z, xs)
    all_sent((NCH - 1) * Z, ys)
    all_sent(NCH * 2 * Z, ds)

    def block(s, q):
        return mu_out.at[s, pl.ds(cbase + q * QC, QC), :]

    def whole(s):
        return mu_out.at[s, pl.ds(cbase, KC), :]

    def fx_copy(q):
        ref = block(side, q)
        return remote(ref, ref, fxs, fxr.at[q], xpt)

    def relay(q):
        ref = block(1 - side, q)
        return remote(ref, ref, frs, frr, sib)

    slot = side * 2 + core
    lp_devs = (sib, xpt, xdg)
    lse_copy = remote(lse_snd, lse_rcv, ls_s, ls_r, xpt)

    def send_small():
        lpbuf[slot] = jnp.transpose(lpb[...])[0:1, :]
        halves = ([], [])
        for g in range(NCH):
            piece = lse_ref[:, pl.ds(pl.multiple_of(OWN + g * (4 * Z) + core * (2 * Z), 128), 128)]
            halves[0].append(piece[:, 0:Z])
            halves[1].append(piece[:, Z:2 * Z])
        lse_snd[...] = jnp.concatenate(halves[0] + halves[1], axis=1)
        lse_out[pl.ds(side, 1), :] = lse_ref[:, pl.ds(pl.multiple_of(core * SHARD, SHARD), SHARD)]
        lse_copy.start()
        for i in range(3):
            remote(lpbuf.at[slot], lpbuf.at[slot], lps, lpr, lp_devs[i]).start()

    @pl.loop(1, SWEEPS)
    def _(t):
        par = t % 2
        beta = beta_ref[t]
        zero_sums()
        @pl.loop(0, NBLK // 8)
        def _(i):
            for k in range(4):
                a2 = cross(xt_ref[4 * i + k])
                for h in range(2):
                    soft(8 * i + 2 * k + h, a2[:, h * BLK:(h + 1) * BLK], beta, par)
            send_stats(2 * i, par, 2)

        for g in range(NGRP):
            mstep(g, par, 2 * (1 - g % 2))
        finish_sweep()

        @pl.when(t < SWEEPS - 1)
        def _():
            set_means(mu_out[side, pl.ds(cbase, KC), :])

        stats_sent(par)

    fx_copy(0).start()
    send_small()
    for q in range(1, NQ):
        fx_copy(q).start()
    to_sib = remote(whole(side), whole(side), fds, fdr, sib)
    to_sib.start()

    lse_copy.wait()
    lse_out[pl.ds(1 - side, 1), :] = lse_rcv[...]
    remote(lpbuf.at[pl.ds(0, 3)], lpbuf.at[pl.ds(0, 3)], lps, lpr, sib).wait()
    for s in range(2):
        for c in range(2):
            lp_out[s:s + 1, c * KC:(c + 1) * KC] = lpbuf[s * 2 + c]

    for q in range(NQ):
        fx_copy(q).wait_recv()
        relay(q).start()

    to_sib.wait()
    remote(whole(1 - side), whole(1 - side), frs, frr, sib).wait()
    remote(whole(side), whole(side), fxs, frr, xpt).wait_send()


def write_out(mu_v, lp_v, lse_v, mu_o, lp_o, lse_o, sem):
    pairs = [(lp_v, lp_o), (lse_v, lse_o)]
    for s in range(2):
        for k in range(2):
            part = pl.ds(k * KC, KC)
            pairs.append((mu_v.at[s, part, :], mu_o.at[s, part, :]))
    copies = [pltpu.make_async_copy(src, dst, sem.at[i]) for i, (src, dst) in enumerate(pairs)]
    for c in copies:
        c.start()
    for c in copies:
        c.wait()


def solution(mesh):
    def local_fit(x_local, mu_init, logpi_init, inv_temp):
        dma = pltpu.SemaphoreType.DMA
        vmem = pl.BlockSpec(memory_space=pltpu.VMEM)
        hbm = pl.BlockSpec(memory_space=pltpu.HBM)
        outs = [jax.ShapeDtypeStruct(mu_init.shape, F32),
                jax.ShapeDtypeStruct(logpi_init.shape, F32),
                jax.ShapeDtypeStruct((2, x_local.shape[0]), F32)]
        res = pl.pallas_call(
            body,
            out_shape=tuple(pltpu.VMEM(o.shape, o.dtype) for o in outs),
            in_specs=[hbm] * 4,
            out_specs=(vmem, vmem, vmem),
            scratch_shapes=[
                pltpu.VMEM((ROWS, HALF), BF16),
                pltpu.VMEM((NBLK // 2, HALF, 2 * BLK), BF16),
                pltpu.VMEM((NBLK, KC, BLK), F32),
                pltpu.VMEM((2, KC, GRP * BLK), BF16),
                pltpu.VMEM((PRE * Z, HALF), BF16),
                pltpu.VMEM((2, 2 * KC), F32),
                pltpu.SMEM((SWEEPS,), F32),
                pltpu.VMEM((KC, HALF), F32),
                pltpu.VMEM((KC, 128), F32),
                pltpu.VMEM((KC, HALF), F32),
                pltpu.VMEM((KC, HALF), BF16),
                pltpu.VMEM((KC, 128), F32),
                pltpu.VMEM((KC, 128), F32),
                pltpu.VMEM((NBLK, 1, BLK), F32),
                pltpu.VMEM((NBLK, 1, BLK), F32),
                pltpu.VMEM((1, ROWS), F32),
                pltpu.VMEM((2, NGRP, GRP, 1, BLK), F32),
                pltpu.VMEM((2, 3, NGRP, GRP, 1, BLK), F32),
                pltpu.VMEM((4, 1, KC), F32),
                pltpu.VMEM((1, SHARD), F32),
                pltpu.VMEM((1, SHARD), F32),
                dma((5,)),
                dma, dma((NCH + 1,)),
                dma, dma((NCH - 1,)),
                dma, dma((NCH,)),
                dma, dma((NOWN,)),
                dma, dma((2, NGRP)),
                dma, dma,
                dma, dma,
                dma, dma((NQ,)),
                dma, dma,
                dma, dma,
            ],
            compiler_params=pltpu.CompilerParams(
                collective_id=0, has_side_effects=True,
                vmem_limit_bytes=56 * 1024 * 1024),
        )(x_local, mu_init, logpi_init, inv_temp)
        return pl.pallas_call(
            write_out,
            out_shape=tuple(outs),
            in_specs=[vmem] * 3,
            out_specs=(hbm,) * 3,
            scratch_shapes=[dma((6,))],
        )(*[pltpu.with_memory_space_constraint(r, pltpu.VMEM) for r in res])

    return jax.shard_map(
        local_fit,
        mesh=mesh,
        in_specs=(P(("grp", "row"), None), P(None, ("grp", "comp"), None), P(None, ("grp", "comp")), P()),
        out_specs=(P(None, ("grp", "comp"), None), P(None, ("grp", "comp")), P(None, ("grp", "row"))),
        check_vma=False,
    )
```

```python
import jax
import jax.numpy as jnp
from jax import lax
from jax.experimental import pallas as pl
from jax.experimental.pallas import tpu as pltpu
from jax.sharding import PartitionSpec as P

EPS_COUNT = 1e-6
PRIOR_ALPHA = 1e-3

F32 = jnp.float32
BF16 = jnp.bfloat16
MESH = pl.DeviceIdType.MESH

SWEEPS = 3
HALF = 512
SHARD = 2048
ROWS = 8192
KC = 256
BLK = 256
NBLK = ROWS // BLK
GRP = 4
NGRP = NBLK // GRP
NCH = 16
Z = SHARD // 2 // NCH
PRE = 4
NOWN = 4
PIECE = SHARD // NOWN
OWN = 2 * SHARD
NQ = 4
QC = KC // NQ


def body(x_hbm, mu_hbm, lp_hbm, beta_hbm,
         mu_out, lp_out, lse_out,
         xb, xt_ref, p_ref, rb, xpre, lp_in, beta_ref, s_ref, nacc, mu_f, mu2, sqmu, lpb, sqx, mx_ref, lse_ref,
         st_own, st_rem, lpbuf, lse_snd, lse_rcv,
         loc_sem, xs, xr, ys, yr, ds, dr, own_s, own_r,
         st_s, st_r, lps, lpr, ls_s, ls_r, fxs, fxr, fds, fdr, frs, frr):
    comp = lax.axis_index("comp")
    row = lax.axis_index("row")
    side = row // 2
    core = row % 2
    sib = {"row": side * 2 + (1 - core)}
    ypt = {"comp": 1 - comp}
    ydg = {"comp": 1 - comp, "row": side * 2 + (1 - core)}
    xpt = {"row": (1 - side) * 2 + core}
    xdg = {"row": (1 - side) * 2 + (1 - core)}
    peers = (sib, ypt, ydg)

    barrier = pltpu.get_barrier_semaphore()
    for dev in (xpt, sib, ypt, ydg, xdg):
        pl.semaphore_signal(barrier, inc=1, device_id=dev, device_id_type=MESH)

    def remote(src, dst, ssem, rsem, dev):
        return pltpu.make_async_remote_copy(
            src_ref=src, dst_ref=dst, send_sem=ssem, recv_sem=rsem,
            device_id=dev, device_id_type=MESH)

    fit_cols = pl.ds(pl.multiple_of(side * HALF, HALF), HALF)
    oth_cols = pl.ds(pl.multiple_of((1 - side) * HALF, HALF), HALF)
    cbase = pl.multiple_of(core * KC, KC)

    def own_rows(c):
        return xb.at[pl.ds(pl.multiple_of(c * SHARD, SHARD), SHARD), :]

    ld_x = pltpu.make_async_copy(x_hbm.at[:, fit_cols], own_rows(core), loc_sem.at[0])
    ld_mu = pltpu.make_async_copy(mu_hbm.at[side, pl.ds(cbase, KC), :], mu_f, loc_sem.at[1])
    ld_pre = pltpu.make_async_copy(
        x_hbm.at[pl.ds(pl.multiple_of(comp * (SHARD // 2), PRE * Z), PRE * Z), oth_cols],
        xpre, loc_sem.at[2])
    ld_lp = pltpu.make_async_copy(lp_hbm, lp_in, loc_sem.at[3])
    ld_beta = pltpu.make_async_copy(beta_hbm, beta_ref, loc_sem.at[4])
    ld_pre.start()
    ld_mu.start()
    ld_lp.start()
    ld_beta.start()
    ld_x.start()

    def place(g, c, half, n):
        return xb.at[pl.ds(pl.multiple_of(OWN + g * (4 * Z) + c * (2 * Z) + half * Z, Z), n), :]

    def x_copy(g):
        extra = g // NCH
        g0 = g - extra
        half = comp + extra * (1 - 2 * comp)
        src = x_hbm.at[pl.ds(pl.multiple_of(half * (SHARD // 2) + g0 * Z, Z), Z), oth_cols]
        return remote(src, place(g0, core, half, Z), xs, xr.at[g], xpt)

    def y_copy(g):
        ref = place(g, core, comp, Z)
        return remote(ref, ref, ys, yr.at[g], ypt)

    def d_copy(g):
        ref = place(g, core, 0, 2 * Z)
        return remote(ref, ref, ds, dr.at[g], sib)

    def own_copy(k):
        src = x_hbm.at[pl.ds(pl.multiple_of(k * PIECE, PIECE), PIECE), fit_cols]
        dst = xb.at[pl.ds(pl.multiple_of(core * SHARD + k * PIECE, PIECE), PIECE), :]
        return remote(src, dst, own_s, own_r.at[k], sib)

    pl.semaphore_wait(barrier, 5)
    ld_pre.wait()
    for g in range(PRE):
        remote(xpre.at[pl.ds(g * Z, Z), :], place(g, core, comp, Z), xs, xr.at[g], xpt).start()
    for k in range(NOWN):
        own_copy(k).start()

    @pl.loop(PRE, NCH + 1)
    def _(g):
        x_copy(g).start()

    def bc(row_vec):
        return jnp.transpose(jnp.broadcast_to(row_vec, (128, KC)))

    def set_means(mu):
        mu2[...] = mu.astype(BF16) * jnp.asarray(-2.0, BF16)
        sqmu[...] = jnp.broadcast_to(jnp.sum(mu * mu, axis=1, keepdims=True), (KC, 128))

    ld_lp.wait()
    ld_beta.wait()
    lpb[...] = bc(lp_in[pl.ds(side, 1), pl.ds(cbase, KC)])
    ld_mu.wait()
    set_means(mu_f[...])

    def prep(b):
        xt = jnp.transpose(xb[pl.ds(pl.multiple_of(b * BLK, BLK), BLK), :])
        xt_ref[b // 2, :, pl.ds(pl.multiple_of(b % 2 * BLK, BLK), BLK)] = xt
        xf = xt.astype(F32)
        sqx[b] = jnp.sum(xf * xf, axis=0, keepdims=True)

    def cross(xt):
        return jnp.dot(mu2[...], xt, preferred_element_type=F32)

    def soft(b, a2, beta, par):
        sq = sqx[b]
        grp = b // GRP
        j = b % GRP
        for h in range(BLK // 128):
            cols = slice(h * 128, (h + 1) * 128)
            t = (a2[:, cols] + sq[:, cols]) + sqmu[...]
            logit = lpb[...] - beta * t
            m = jnp.max(logit, axis=0, keepdims=True)
            e = jnp.exp(logit - m)
            r = jnp.sum(e, axis=0, keepdims=True)
            p_ref[b, :, cols] = e
            mx_ref[b, :, cols] = m
            st_own[par, grp, j, :, cols] = m + jnp.log(r)

    def soft_pair(b, a2, beta, par):
        sq = jnp.concatenate([sqx[b], sqx[b + 1]], axis=1)
        m = None
        for c in range(0, KC, 8):
            rows = slice(c, c + 8)
            t = (a2[rows] + sq) + jnp.concatenate([sqmu[rows]] * 4, axis=1)
            logit = jnp.concatenate([lpb[rows]] * 4, axis=1) - beta * t
            p_ref[b, rows, :] = logit[:, 0:BLK]
            p_ref[b + 1, rows, :] = logit[:, BLK:2 * BLK]
            m = logit if m is None else jnp.maximum(m, logit)
        m = jnp.max(m, axis=0, keepdims=True)
        for k in range(2):
            mk = m[:, k * BLK:(k + 1) * BLK]
            mx_ref[b + k] = mk
            r = None
            for c in range(0, KC, 8):
                rows = slice(c, c + 8)
                e = jnp.exp(p_ref[b + k, rows, :] - mk)
                p_ref[b + k, rows, :] = e
                r = e if r is None else r + e
            lse = mk + jnp.log(jnp.sum(r, axis=0, keepdims=True))
            st_own[par, (b + k) // GRP, (b + k) % GRP] = lse

    def send_stats(grp, par, n):
        own = st_own.at[par, pl.ds(grp, n)]
        for i in range(3):
            remote(own, st_rem.at[par, i, pl.ds(grp, n)], st_s, st_r.at[par, grp], peers[i]).start()

    def wait_stats(grp, par, n):
        three = st_rem.at[par, :, pl.ds(grp, n)]
        remote(three, three, st_s, st_r.at[par, grp], sib).wait_recv()

    def stats_sent(par):
        remote(st_rem.at[par], st_rem.at[par], st_s, st_r.at[par, 0], sib).wait_send()

    def resp(grp, par):
        st = [st_own[par, grp]] + [st_rem[par, i, grp] for i in range(3)]
        top = jnp.maximum(jnp.maximum(st[0], st[1]), jnp.maximum(st[2], st[3]))
        es = [jnp.exp(v - top) for v in st]
        tot = (es[0] + es[1]) + (es[2] + es[3])
        lse = top + jnp.log(tot)
        first = pl.multiple_of(grp * GRP, GRP)
        scale = jnp.exp(mx_ref[pl.ds(first, GRP)] - top) / tot
        cnt = nacc[...]
        for j in range(GRP):
            lse_ref[:, pl.ds(pl.multiple_of((grp * GRP + j) * BLK, BLK), BLK)] = lse[j]
            rj = p_ref[grp * GRP + j] * scale[j]
            cnt = cnt + (rj[:, 0:128] + rj[:, 128:256])
            rb[grp % 2, :, j * BLK:(j + 1) * BLK] = rj.astype(BF16)
        nacc[...] = cnt

    def gather(grp):
        rows = pl.ds(pl.multiple_of(grp * (GRP * BLK), GRP * BLK), GRP * BLK)
        s_ref[...] += jnp.dot(rb[grp % 2], xb[rows, :], preferred_element_type=F32)

    def mstep(grp, par, n=1):
        if n:
            wait_stats(grp, par, n)
        resp(grp, par)
        gather(grp)

    def zero_sums():
        nacc[...] = jnp.zeros_like(nacc)
        s_ref[...] = jnp.zeros_like(s_ref)

    def finish_sweep():
        n = jnp.sum(nacc[...], axis=1, keepdims=True)
        lp = jnp.log((n + PRIOR_ALPHA) / (ROWS + 4 * KC * PRIOR_ALPHA))
        lpb[...] = jnp.broadcast_to(lp, (KC, 128))
        mu = s_ref[...] * (1.0 / (n + EPS_COUNT))
        mu_out[side, pl.ds(cbase, KC), :] = mu

    zero_sums()
    beta0 = beta_ref[0]

    def first_block(b):
        prep(b)
        soft(b, cross(xt_ref[b // 2, :, pl.ds(pl.multiple_of(b % 2 * BLK, BLK), BLK)]), beta0, 0)

    def own_block(n):
        @pl.when((n >= 8) & (n % 2 == 0))
        def _():
            own_copy((n - 8) // 2).wait_recv()

        first_block((core * 8 + n) % 16)

    ld_x.wait()

    @pl.loop(0, 4)
    def _(n):
        own_block(n)

    @pl.loop(0, NCH + 4)
    def _(it):
        @pl.when(it < NCH - 1)
        def _():
            x_copy(it).wait_recv()
            y_copy(it).start()

        @pl.when(it == NCH + 1)
        def _():
            x_copy(NCH - 1).wait_recv()
            x_copy(NCH).wait_recv()
            d_copy(NCH - 1).start()

        @pl.when((it >= 3) & (it < NCH + 2))
        def _():
            y_copy(it - 3).wait_recv()
            d_copy(it - 3).start()

        @pl.when(it < 4)
        def _():
            @pl.loop(0, 2)
            def _(k):
                own_block(4 + 2 * it + k)

        @pl.when((it >= 4) & (it < 8))
        def _():
            own_block(8 + it)

        @pl.when(it >= 4)
        def _():
            g = it - 4 + (it // (NCH + 2)) * (1 - 2 * (it % 2))
            d_copy(g).wait_recv()
            first_block(NBLK // 2 + g)

        @pl.when(it == NCH - 2)
        def _():
            send_stats(0, 0, 4)
            send_stats(4, 0, 2)

        @pl.when(it == NCH - 1)
        def _():
            send_stats(6, 0, 1)

    send_stats(7, 0, 1)
    for g in range(NGRP):
        mstep(g, 0, {0: 4, 4: 2, 6: 1, 7: 1}.get(g, 0))
    stats_sent(0)
    finish_sweep()
    set_means(mu_out[side, pl.ds(cbase, KC), :])

    def all_sent(n, sem):
        ref = xb.at[pl.ds(0, n), :]
        remote(ref, ref, sem, own_r.at[0], sib).wait_send()

    all_sent(SHARD, own_s)
    all_sent((NCH + 1) * Z, xs)
    all_sent((NCH - 1) * Z, ys)
    all_sent(NCH * 2 * Z, ds)

    def block(s, q):
        return mu_out.at[s, pl.ds(cbase + q * QC, QC), :]

    def whole(s):
        return mu_out.at[s, pl.ds(cbase, KC), :]

    def fx_copy(q):
        ref = block(side, q)
        return remote(ref, ref, fxs, fxr.at[q], xpt)

    def relay(q):
        ref = block(1 - side, q)
        return remote(ref, ref, frs, frr, sib)

    slot = side * 2 + core
    lp_devs = (sib, xpt, xdg)
    lse_copy = remote(lse_snd, lse_rcv, ls_s, ls_r, xpt)

    def send_small():
        lpbuf[slot] = jnp.transpose(lpb[...])[0:1, :]
        halves = ([], [])
        for g in range(NCH):
            piece = lse_ref[:, pl.ds(pl.multiple_of(OWN + g * (4 * Z) + core * (2 * Z), 128), 128)]
            halves[0].append(piece[:, 0:Z])
            halves[1].append(piece[:, Z:2 * Z])
        lse_snd[...] = jnp.concatenate(halves[0] + halves[1], axis=1)
        lse_out[pl.ds(side, 1), :] = lse_ref[:, pl.ds(pl.multiple_of(core * SHARD, SHARD), SHARD)]
        lse_copy.start()
        for i in range(3):
            remote(lpbuf.at[slot], lpbuf.at[slot], lps, lpr, lp_devs[i]).start()

    @pl.loop(1, SWEEPS)
    def _(t):
        par = t % 2
        beta = beta_ref[t]
        zero_sums()
        @pl.loop(0, NBLK // 8)
        def _(i):
            for k in range(4):
                a2 = cross(xt_ref[4 * i + k])
                soft_pair(8 * i + 2 * k, a2, beta, par)
            send_stats(2 * i, par, 2)

        for g in range(NGRP):
            mstep(g, par, 2 * (1 - g % 2))
        finish_sweep()

        @pl.when(t < SWEEPS - 1)
        def _():
            set_means(mu_out[side, pl.ds(cbase, KC), :])

        stats_sent(par)

    fx_copy(0).start()
    send_small()
    for q in range(1, NQ):
        fx_copy(q).start()
    to_sib = remote(whole(side), whole(side), fds, fdr, sib)
    to_sib.start()

    lse_copy.wait()
    lse_out[pl.ds(1 - side, 1), :] = lse_rcv[...]
    remote(lpbuf.at[pl.ds(0, 3)], lpbuf.at[pl.ds(0, 3)], lps, lpr, sib).wait()
    for s in range(2):
        for c in range(2):
            lp_out[s:s + 1, c * KC:(c + 1) * KC] = lpbuf[s * 2 + c]

    for q in range(NQ):
        fx_copy(q).wait_recv()
        relay(q).start()

    to_sib.wait()
    remote(whole(1 - side), whole(1 - side), frs, frr, sib).wait()
    remote(whole(side), whole(side), fxs, frr, xpt).wait_send()


def write_out(mu_v, lp_v, lse_v, mu_o, lp_o, lse_o, sem):
    pairs = [(lp_v, lp_o), (lse_v, lse_o)]
    for s in range(2):
        for k in range(2):
            part = pl.ds(k * KC, KC)
            pairs.append((mu_v.at[s, part, :], mu_o.at[s, part, :]))
    copies = [pltpu.make_async_copy(src, dst, sem.at[i]) for i, (src, dst) in enumerate(pairs)]
    for c in copies:
        c.start()
    for c in copies:
        c.wait()


def solution(mesh):
    def local_fit(x_local, mu_init, logpi_init, inv_temp):
        dma = pltpu.SemaphoreType.DMA
        vmem = pl.BlockSpec(memory_space=pltpu.VMEM)
        hbm = pl.BlockSpec(memory_space=pltpu.HBM)
        outs = [jax.ShapeDtypeStruct(mu_init.shape, F32),
                jax.ShapeDtypeStruct(logpi_init.shape, F32),
                jax.ShapeDtypeStruct((2, x_local.shape[0]), F32)]
        res = pl.pallas_call(
            body,
            out_shape=tuple(pltpu.VMEM(o.shape, o.dtype) for o in outs),
            in_specs=[hbm] * 4,
            out_specs=(vmem, vmem, vmem),
            scratch_shapes=[
                pltpu.VMEM((ROWS, HALF), BF16),
                pltpu.VMEM((NBLK // 2, HALF, 2 * BLK), BF16),
                pltpu.VMEM((NBLK, KC, BLK), F32),
                pltpu.VMEM((2, KC, GRP * BLK), BF16),
                pltpu.VMEM((PRE * Z, HALF), BF16),
                pltpu.VMEM((2, 2 * KC), F32),
                pltpu.SMEM((SWEEPS,), F32),
                pltpu.VMEM((KC, HALF), F32),
                pltpu.VMEM((KC, 128), F32),
                pltpu.VMEM((KC, HALF), F32),
                pltpu.VMEM((KC, HALF), BF16),
                pltpu.VMEM((KC, 128), F32),
                pltpu.VMEM((KC, 128), F32),
                pltpu.VMEM((NBLK, 1, BLK), F32),
                pltpu.VMEM((NBLK, 1, BLK), F32),
                pltpu.VMEM((1, ROWS), F32),
                pltpu.VMEM((2, NGRP, GRP, 1, BLK), F32),
                pltpu.VMEM((2, 3, NGRP, GRP, 1, BLK), F32),
                pltpu.VMEM((4, 1, KC), F32),
                pltpu.VMEM((1, SHARD), F32),
                pltpu.VMEM((1, SHARD), F32),
                dma((5,)),
                dma, dma((NCH + 1,)),
                dma, dma((NCH - 1,)),
                dma, dma((NCH,)),
                dma, dma((NOWN,)),
                dma, dma((2, NGRP)),
                dma, dma,
                dma, dma,
                dma, dma((NQ,)),
                dma, dma,
                dma, dma,
            ],
            compiler_params=pltpu.CompilerParams(
                collective_id=0, has_side_effects=True,
                vmem_limit_bytes=56 * 1024 * 1024),
        )(x_local, mu_init, logpi_init, inv_temp)
        return pl.pallas_call(
            write_out,
            out_shape=tuple(outs),
            in_specs=[vmem] * 3,
            out_specs=(hbm,) * 3,
            scratch_shapes=[dma((6,))],
        )(*[pltpu.with_memory_space_constraint(r, pltpu.VMEM) for r in res])

    return jax.shard_map(
        local_fit,
        mesh=mesh,
        in_specs=(P(("grp", "row"), None), P(None, ("grp", "comp"), None), P(None, ("grp", "comp")), P()),
        out_specs=(P(None, ("grp", "comp"), None), P(None, ("grp", "comp")), P(None, ("grp", "row"))),
        check_vma=False,
    )
```

```python
import jax
import jax.numpy as jnp
from jax import lax
from jax.experimental import pallas as pl
from jax.experimental.pallas import tpu as pltpu
from jax.sharding import PartitionSpec as P

EPS_COUNT = 1e-6
PRIOR_ALPHA = 1e-3

F32 = jnp.float32
BF16 = jnp.bfloat16
MESH = pl.DeviceIdType.MESH

SWEEPS = 3
HALF = 512
SHARD = 2048
ROWS = 8192
KC = 256
BLK = 256
NBLK = ROWS // BLK
GRP = 4
NGRP = NBLK // GRP
NCH = 16
Z = SHARD // 2 // NCH
PRE = 4
NOWN = 4
PIECE = SHARD // NOWN
OWN = 2 * SHARD
NQ = 4
QC = KC // NQ


def body(x_hbm, mu_hbm, lp_hbm, beta_hbm,
         mu_out, lp_out, lse_out,
         xb, xt_ref, p_ref, rb, xpre, lp_in, beta_ref, s_ref, nacc, mu_f, mu2, sqmu, lpb, sqx, mx_ref, lse_ref,
         st_own, st_rem, lpbuf, lse_snd, lse_rcv,
         loc_sem, xs, xr, ys, yr, ds, dr, own_s, own_r,
         st_s, st_r, lps, lpr, ls_s, ls_r, fxs, fxr, fds, fdr, frs, frr):
    comp = lax.axis_index("comp")
    row = lax.axis_index("row")
    side = row // 2
    core = row % 2
    sib = {"row": side * 2 + (1 - core)}
    ypt = {"comp": 1 - comp}
    ydg = {"comp": 1 - comp, "row": side * 2 + (1 - core)}
    xpt = {"row": (1 - side) * 2 + core}
    xdg = {"row": (1 - side) * 2 + (1 - core)}
    peers = (sib, ypt, ydg)

    barrier = pltpu.get_barrier_semaphore()
    for dev in (xpt, sib, ypt, ydg, xdg):
        pl.semaphore_signal(barrier, inc=1, device_id=dev, device_id_type=MESH)

    def remote(src, dst, ssem, rsem, dev):
        return pltpu.make_async_remote_copy(
            src_ref=src, dst_ref=dst, send_sem=ssem, recv_sem=rsem,
            device_id=dev, device_id_type=MESH)

    fit_cols = pl.ds(pl.multiple_of(side * HALF, HALF), HALF)
    oth_cols = pl.ds(pl.multiple_of((1 - side) * HALF, HALF), HALF)
    cbase = pl.multiple_of(core * KC, KC)

    def own_rows(c):
        return xb.at[pl.ds(pl.multiple_of(c * SHARD, SHARD), SHARD), :]

    ld_x = pltpu.make_async_copy(x_hbm.at[:, fit_cols], own_rows(core), loc_sem.at[0])
    ld_mu = pltpu.make_async_copy(mu_hbm.at[side, pl.ds(cbase, KC), :], mu_f, loc_sem.at[1])
    ld_pre = pltpu.make_async_copy(
        x_hbm.at[pl.ds(pl.multiple_of(comp * (SHARD // 2), PRE * Z), PRE * Z), oth_cols],
        xpre, loc_sem.at[2])
    ld_lp = pltpu.make_async_copy(lp_hbm, lp_in, loc_sem.at[3])
    ld_beta = pltpu.make_async_copy(beta_hbm, beta_ref, loc_sem.at[4])
    ld_pre.start()
    ld_mu.start()
    ld_lp.start()
    ld_beta.start()
    ld_x.start()

    def place(g, c, half, n):
        return xb.at[pl.ds(pl.multiple_of(OWN + g * (4 * Z) + c * (2 * Z) + half * Z, Z), n), :]

    def x_copy(g):
        extra = g // NCH
        g0 = g - extra
        half = comp + extra * (1 - 2 * comp)
        src = x_hbm.at[pl.ds(pl.multiple_of(half * (SHARD // 2) + g0 * Z, Z), Z), oth_cols]
        return remote(src, place(g0, core, half, Z), xs, xr.at[g], xpt)

    def y_copy(g):
        ref = place(g, core, comp, Z)
        return remote(ref, ref, ys, yr.at[g], ypt)

    def d_copy(g):
        ref = place(g, core, 0, 2 * Z)
        return remote(ref, ref, ds, dr.at[g], sib)

    def own_copy(k):
        src = x_hbm.at[pl.ds(pl.multiple_of(k * PIECE, PIECE), PIECE), fit_cols]
        dst = xb.at[pl.ds(pl.multiple_of(core * SHARD + k * PIECE, PIECE), PIECE), :]
        return remote(src, dst, own_s, own_r.at[k], sib)

    pl.semaphore_wait(barrier, 5)
    ld_pre.wait()
    for g in range(PRE):
        remote(xpre.at[pl.ds(g * Z, Z), :], place(g, core, comp, Z), xs, xr.at[g], xpt).start()
    for k in range(NOWN):
        own_copy(k).start()

    @pl.loop(PRE, NCH + 1)
    def _(g):
        x_copy(g).start()

    def bc(row_vec):
        return jnp.transpose(jnp.broadcast_to(row_vec, (128, KC)))

    def set_means(mu):
        mu2[...] = mu.astype(BF16) * jnp.asarray(-2.0, BF16)
        sqmu[...] = jnp.broadcast_to(jnp.sum(mu * mu, axis=1, keepdims=True), (KC, 128))

    ld_lp.wait()
    ld_beta.wait()
    lpb[...] = bc(lp_in[pl.ds(side, 1), pl.ds(cbase, KC)])
    ld_mu.wait()
    set_means(mu_f[...])

    def prep(b, c):
        rows = pl.ds(pl.multiple_of(b * BLK + c * 128, 128), 128)
        xt = jnp.transpose(xb[rows, :])
        xt_ref[b // 2, :, pl.ds(pl.multiple_of(b % 2 * BLK + c * 128, 128), 128)] = xt
        xf = xt.astype(F32)
        sqx[b, :, pl.ds(pl.multiple_of(c * 128, 128), 128)] = jnp.sum(xf * xf, axis=0, keepdims=True)

    def cross(xt):
        return jnp.dot(mu2[...], xt, preferred_element_type=F32)

    def soft(b, a2, beta, par):
        sq = sqx[b]
        grp = b // GRP
        j = b % GRP
        for h in range(BLK // 128):
            cols = slice(h * 128, (h + 1) * 128)
            t = (a2[:, cols] + sq[:, cols]) + sqmu[...]
            logit = lpb[...] - beta * t
            m = jnp.max(logit, axis=0, keepdims=True)
            e = jnp.exp(logit - m)
            r = jnp.sum(e, axis=0, keepdims=True)
            p_ref[b, :, cols] = e
            mx_ref[b, :, cols] = m
            st_own[par, grp, j, :, cols] = m + jnp.log(r)

    def send_stats(grp, par, n):
        own = st_own.at[par, pl.ds(grp, n)]
        for i in range(3):
            remote(own, st_rem.at[par, i, pl.ds(grp, n)], st_s, st_r.at[par, grp], peers[i]).start()

    def wait_stats(grp, par, n):
        three = st_rem.at[par, :, pl.ds(grp, n)]
        remote(three, three, st_s, st_r.at[par, grp], sib).wait_recv()

    def stats_sent(par):
        remote(st_rem.at[par], st_rem.at[par], st_s, st_r.at[par, 0], sib).wait_send()

    def resp(grp, par):
        st = [st_own[par, grp]] + [st_rem[par, i, grp] for i in range(3)]
        top = jnp.maximum(jnp.maximum(st[0], st[1]), jnp.maximum(st[2], st[3]))
        es = [jnp.exp(v - top) for v in st]
        tot = (es[0] + es[1]) + (es[2] + es[3])
        lse = top + jnp.log(tot)
        first = pl.multiple_of(grp * GRP, GRP)
        scale = jnp.exp(mx_ref[pl.ds(first, GRP)] - top) / tot
        cnt = nacc[...]
        for j in range(GRP):
            lse_ref[:, pl.ds(pl.multiple_of((grp * GRP + j) * BLK, BLK), BLK)] = lse[j]
            rj = p_ref[grp * GRP + j] * scale[j]
            cnt = cnt + (rj[:, 0:128] + rj[:, 128:256])
            rb[grp % 2, :, j * BLK:(j + 1) * BLK] = rj.astype(BF16)
        nacc[...] = cnt

    def gather(grp):
        rows = pl.ds(pl.multiple_of(grp * (GRP * BLK), GRP * BLK), GRP * BLK)
        s_ref[...] += jnp.dot(rb[grp % 2], xb[rows, :], preferred_element_type=F32)

    def mstep(grp, par, n=1):
        if n:
            wait_stats(grp, par, n)
        resp(grp, par)
        gather(grp)

    def zero_sums():
        nacc[...] = jnp.zeros_like(nacc)
        s_ref[...] = jnp.zeros_like(s_ref)

    def finish_sweep():
        n = jnp.sum(nacc[...], axis=1, keepdims=True)
        lp = jnp.log((n + PRIOR_ALPHA) / (ROWS + 4 * KC * PRIOR_ALPHA))
        lpb[...] = jnp.broadcast_to(lp, (KC, 128))
        mu = s_ref[...] * (1.0 / (n + EPS_COUNT))
        mu_out[side, pl.ds(cbase, KC), :] = mu

    zero_sums()
    beta0 = beta_ref[0]

    def first_block(b):
        soft(b, cross(xt_ref[b // 2, :, pl.ds(pl.multiple_of(b % 2 * BLK, BLK), BLK)]), beta0, 0)

    def own_block(n):
        @pl.when((n >= 8) & (n % 2 == 0))
        def _():
            own_copy((n - 8) // 2).wait_recv()

        b = (core * 8 + n) % 16
        prep(b, 0)
        prep(b, 1)
        first_block(b)

    ld_x.wait()

    @pl.loop(0, 4)
    def _(n):
        own_block(n)

    @pl.loop(0, NCH + 4)
    def _(it):
        @pl.when(it < NCH - 1)
        def _():
            x_copy(it).wait_recv()
            y_copy(it).start()

        @pl.when(it == NCH + 1)
        def _():
            x_copy(NCH - 1).wait_recv()
            x_copy(NCH).wait_recv()
            d_copy(NCH - 1).start()
            prep(NBLK - 1, core)

        @pl.when((it >= 3) & (it < NCH + 2))
        def _():
            y_copy(it - 3).wait_recv()
            d_copy(it - 3).start()
            prep(NBLK // 2 + it - 3, core)

        @pl.when(it < 4)
        def _():
            @pl.loop(0, 2)
            def _(k):
                own_block(4 + 2 * it + k)

        @pl.when((it >= 4) & (it < 8))
        def _():
            own_block(8 + it)

        @pl.when(it >= 4)
        def _():
            g = it - 4 + (it // (NCH + 2)) * (1 - 2 * (it % 2))
            d_copy(g).wait_recv()
            prep(NBLK // 2 + g, 1 - core)
            first_block(NBLK // 2 + g)

        @pl.when(it == NCH - 2)
        def _():
            send_stats(0, 0, 4)
            send_stats(4, 0, 2)

        @pl.when(it == NCH - 1)
        def _():
            send_stats(6, 0, 1)

    send_stats(7, 0, 1)
    for g in range(NGRP):
        mstep(g, 0, {0: 4, 4: 2, 6: 1, 7: 1}.get(g, 0))
    stats_sent(0)
    finish_sweep()
    set_means(mu_out[side, pl.ds(cbase, KC), :])

    def all_sent(n, sem):
        ref = xb.at[pl.ds(0, n), :]
        remote(ref, ref, sem, own_r.at[0], sib).wait_send()

    all_sent(SHARD, own_s)
    all_sent((NCH + 1) * Z, xs)
    all_sent((NCH - 1) * Z, ys)
    all_sent(NCH * 2 * Z, ds)

    def block(s, q):
        return mu_out.at[s, pl.ds(cbase + q * QC, QC), :]

    def whole(s):
        return mu_out.at[s, pl.ds(cbase, KC), :]

    def fx_copy(q):
        ref = block(side, q)
        return remote(ref, ref, fxs, fxr.at[q], xpt)

    def relay(q):
        ref = block(1 - side, q)
        return remote(ref, ref, frs, frr, sib)

    slot = side * 2 + core
    lp_devs = (sib, xpt, xdg)
    lse_copy = remote(lse_snd, lse_rcv, ls_s, ls_r, xpt)

    def send_small():
        lpbuf[slot] = jnp.transpose(lpb[...])[0:1, :]
        halves = ([], [])
        for g in range(NCH):
            piece = lse_ref[:, pl.ds(pl.multiple_of(OWN + g * (4 * Z) + core * (2 * Z), 128), 128)]
            halves[0].append(piece[:, 0:Z])
            halves[1].append(piece[:, Z:2 * Z])
        lse_snd[...] = jnp.concatenate(halves[0] + halves[1], axis=1)
        lse_out[pl.ds(side, 1), :] = lse_ref[:, pl.ds(pl.multiple_of(core * SHARD, SHARD), SHARD)]
        lse_copy.start()
        for i in range(3):
            remote(lpbuf.at[slot], lpbuf.at[slot], lps, lpr, lp_devs[i]).start()

    @pl.loop(1, SWEEPS)
    def _(t):
        par = t % 2
        beta = beta_ref[t]
        zero_sums()
        def epairs(first, n):
            for k in range(n):
                a2 = cross(xt_ref[first + k])
                for h in range(2):
                    soft(2 * (first + k) + h, a2[:, h * BLK:(h + 1) * BLK], beta, par)

        @pl.loop(0, NBLK // 8 - 1)
        def _(i):
            epairs(4 * i, 4)
            send_stats(2 * i, par, 2)

        for g in (NGRP - 2, NGRP - 1):
            epairs(2 * g, 2)
            send_stats(g, par, 1)

        for g in range(NGRP):
            mstep(g, par, 1 if g >= NGRP - 2 else 2 * (1 - g % 2))
        finish_sweep()

        @pl.when(t < SWEEPS - 1)
        def _():
            set_means(mu_out[side, pl.ds(cbase, KC), :])

        stats_sent(par)

    fx_copy(0).start()
    send_small()
    for q in range(1, NQ):
        fx_copy(q).start()
    to_sib = remote(whole(side), whole(side), fds, fdr, sib)
    to_sib.start()

    lse_copy.wait()
    lse_out[pl.ds(1 - side, 1), :] = lse_rcv[...]
    remote(lpbuf.at[pl.ds(0, 3)], lpbuf.at[pl.ds(0, 3)], lps, lpr, sib).wait()
    for s in range(2):
        for c in range(2):
            lp_out[s:s + 1, c * KC:(c + 1) * KC] = lpbuf[s * 2 + c]

    for q in range(NQ):
        fx_copy(q).wait_recv()
        relay(q).start()

    to_sib.wait()
    remote(whole(1 - side), whole(1 - side), frs, frr, sib).wait()
    remote(whole(side), whole(side), fxs, frr, xpt).wait_send()


def write_out(mu_v, lp_v, lse_v, mu_o, lp_o, lse_o, sem):
    pairs = [(lp_v, lp_o), (lse_v, lse_o)]
    for s in range(2):
        for k in range(2):
            part = pl.ds(k * KC, KC)
            pairs.append((mu_v.at[s, part, :], mu_o.at[s, part, :]))
    copies = [pltpu.make_async_copy(src, dst, sem.at[i]) for i, (src, dst) in enumerate(pairs)]
    for c in copies:
        c.start()
    for c in copies:
        c.wait()


def solution(mesh):
    def local_fit(x_local, mu_init, logpi_init, inv_temp):
        dma = pltpu.SemaphoreType.DMA
        vmem = pl.BlockSpec(memory_space=pltpu.VMEM)
        hbm = pl.BlockSpec(memory_space=pltpu.HBM)
        outs = [jax.ShapeDtypeStruct(mu_init.shape, F32),
                jax.ShapeDtypeStruct(logpi_init.shape, F32),
                jax.ShapeDtypeStruct((2, x_local.shape[0]), F32)]
        res = pl.pallas_call(
            body,
            out_shape=tuple(pltpu.VMEM(o.shape, o.dtype) for o in outs),
            in_specs=[hbm] * 4,
            out_specs=(vmem, vmem, vmem),
            scratch_shapes=[
                pltpu.VMEM((ROWS, HALF), BF16),
                pltpu.VMEM((NBLK // 2, HALF, 2 * BLK), BF16),
                pltpu.VMEM((NBLK, KC, BLK), F32),
                pltpu.VMEM((2, KC, GRP * BLK), BF16),
                pltpu.VMEM((PRE * Z, HALF), BF16),
                pltpu.VMEM((2, 2 * KC), F32),
                pltpu.SMEM((SWEEPS,), F32),
                pltpu.VMEM((KC, HALF), F32),
                pltpu.VMEM((KC, 128), F32),
                pltpu.VMEM((KC, HALF), F32),
                pltpu.VMEM((KC, HALF), BF16),
                pltpu.VMEM((KC, 128), F32),
                pltpu.VMEM((KC, 128), F32),
                pltpu.VMEM((NBLK, 1, BLK), F32),
                pltpu.VMEM((NBLK, 1, BLK), F32),
                pltpu.VMEM((1, ROWS), F32),
                pltpu.VMEM((2, NGRP, GRP, 1, BLK), F32),
                pltpu.VMEM((2, 3, NGRP, GRP, 1, BLK), F32),
                pltpu.VMEM((4, 1, KC), F32),
                pltpu.VMEM((1, SHARD), F32),
                pltpu.VMEM((1, SHARD), F32),
                dma((5,)),
                dma, dma((NCH + 1,)),
                dma, dma((NCH - 1,)),
                dma, dma((NCH,)),
                dma, dma((NOWN,)),
                dma, dma((2, NGRP)),
                dma, dma,
                dma, dma,
                dma, dma((NQ,)),
                dma, dma,
                dma, dma,
            ],
            compiler_params=pltpu.CompilerParams(
                collective_id=0, has_side_effects=True,
                vmem_limit_bytes=56 * 1024 * 1024),
        )(x_local, mu_init, logpi_init, inv_temp)
        return pl.pallas_call(
            write_out,
            out_shape=tuple(outs),
            in_specs=[vmem] * 3,
            out_specs=(hbm,) * 3,
            scratch_shapes=[dma((6,))],
        )(*[pltpu.with_memory_space_constraint(r, pltpu.VMEM) for r in res])

    return jax.shard_map(
        local_fit,
        mesh=mesh,
        in_specs=(P(("grp", "row"), None), P(None, ("grp", "comp"), None), P(None, ("grp", "comp")), P()),
        out_specs=(P(None, ("grp", "comp"), None), P(None, ("grp", "comp")), P(None, ("grp", "row"))),
        check_vma=False,
    )
```

```python
import jax
import jax.numpy as jnp
from jax import lax
from jax.experimental import pallas as pl
from jax.experimental.pallas import tpu as pltpu
from jax.sharding import PartitionSpec as P

EPS_COUNT = 1e-6
PRIOR_ALPHA = 1e-3

F32 = jnp.float32
BF16 = jnp.bfloat16
MESH = pl.DeviceIdType.MESH

SWEEPS = 3
HALF = 512
SHARD = 2048
ROWS = 8192
KC = 256
BLK = 256
NBLK = ROWS // BLK
GRP = 4
NGRP = NBLK // GRP
NCH = 16
Z = SHARD // 2 // NCH
PRE = 4
NOWN = 4
PIECE = SHARD // NOWN
OWN = 2 * SHARD
NQ = 4
QC = KC // NQ


def body(x_hbm, mu_hbm, lp_hbm, beta_hbm,
         mu_out, lp_out, lse_out,
         xb, xt_ref, p_ref, rb, xpre, lp_in, beta_ref, s_ref, nacc, mu_f, mu2, sqmu, lpb, sqx, mx_ref, lse_ref,
         st_own, st_rem, lpbuf, lse_snd, lse_rcv,
         loc_sem, xs, xr, ys, yr, ds, dr, own_s, own_r,
         st_s, st_r, lps, lpr, ls_s, ls_r, fxs, fxr, fds, fdr, frs, frr):
    comp = lax.axis_index("comp")
    row = lax.axis_index("row")
    side = row // 2
    core = row % 2
    sib = {"row": side * 2 + (1 - core)}
    ypt = {"comp": 1 - comp}
    ydg = {"comp": 1 - comp, "row": side * 2 + (1 - core)}
    xpt = {"row": (1 - side) * 2 + core}
    xdg = {"row": (1 - side) * 2 + (1 - core)}
    peers = (sib, ypt, ydg)

    barrier = pltpu.get_barrier_semaphore()
    for dev in (xpt, sib, ypt, ydg, xdg):
        pl.semaphore_signal(barrier, inc=1, device_id=dev, device_id_type=MESH)

    def remote(src, dst, ssem, rsem, dev):
        return pltpu.make_async_remote_copy(
            src_ref=src, dst_ref=dst, send_sem=ssem, recv_sem=rsem,
            device_id=dev, device_id_type=MESH)

    fit_cols = pl.ds(pl.multiple_of(side * HALF, HALF), HALF)
    oth_cols = pl.ds(pl.multiple_of((1 - side) * HALF, HALF), HALF)
    cbase = pl.multiple_of(core * KC, KC)

    def own_rows(c):
        return xb.at[pl.ds(pl.multiple_of(c * SHARD, SHARD), SHARD), :]

    ld_x = pltpu.make_async_copy(x_hbm.at[:, fit_cols], own_rows(core), loc_sem.at[0])
    ld_mu = pltpu.make_async_copy(mu_hbm.at[side, pl.ds(cbase, KC), :], mu_f, loc_sem.at[1])
    ld_pre = pltpu.make_async_copy(
        x_hbm.at[pl.ds(pl.multiple_of(comp * (SHARD // 2), PRE * Z), PRE * Z), oth_cols],
        xpre, loc_sem.at[2])
    ld_lp = pltpu.make_async_copy(lp_hbm, lp_in, loc_sem.at[3])
    ld_beta = pltpu.make_async_copy(beta_hbm, beta_ref, loc_sem.at[4])
    ld_pre.start()
    ld_mu.start()
    ld_lp.start()
    ld_beta.start()
    ld_x.start()

    def place(g, c, half, n):
        return xb.at[pl.ds(pl.multiple_of(OWN + g * (4 * Z) + c * (2 * Z) + half * Z, Z), n), :]

    def x_copy(g):
        extra = g // NCH
        g0 = g - extra
        half = comp + extra * (1 - 2 * comp)
        src = x_hbm.at[pl.ds(pl.multiple_of(half * (SHARD // 2) + g0 * Z, Z), Z), oth_cols]
        return remote(src, place(g0, core, half, Z), xs, xr.at[g], xpt)

    def y_copy(g):
        ref = place(g, core, comp, Z)
        return remote(ref, ref, ys, yr.at[g], ypt)

    def d_copy(g):
        ref = place(g, core, 0, 2 * Z)
        return remote(ref, ref, ds, dr.at[g], sib)

    def own_copy(k):
        src = x_hbm.at[pl.ds(pl.multiple_of(k * PIECE, PIECE), PIECE), fit_cols]
        dst = xb.at[pl.ds(pl.multiple_of(core * SHARD + k * PIECE, PIECE), PIECE), :]
        return remote(src, dst, own_s, own_r.at[k], sib)

    pl.semaphore_wait(barrier, 5)
    ld_pre.wait()
    for g in range(PRE):
        remote(xpre.at[pl.ds(g * Z, Z), :], place(g, core, comp, Z), xs, xr.at[g], xpt).start()
    for k in range(NOWN):
        own_copy(k).start()

    @pl.loop(PRE, NCH + 1)
    def _(g):
        x_copy(g).start()

    def bc(row_vec):
        return jnp.transpose(jnp.broadcast_to(row_vec, (128, KC)))

    def set_means(mu):
        mu2[...] = mu.astype(BF16) * jnp.asarray(-2.0, BF16)
        sqmu[...] = jnp.broadcast_to(jnp.sum(mu * mu, axis=1, keepdims=True), (KC, 128))

    ld_lp.wait()
    ld_beta.wait()
    lpb[...] = bc(lp_in[pl.ds(side, 1), pl.ds(cbase, KC)])
    ld_mu.wait()
    set_means(mu_f[...])

    def prep(b, c):
        rows = pl.ds(pl.multiple_of(b * BLK + c * 128, 128), 128)
        xt = jnp.transpose(xb[rows, :])
        xt_ref[b // 2, :, pl.ds(pl.multiple_of(b % 2 * BLK + c * 128, 128), 128)] = xt
        xf = xt.astype(F32)
        sqx[b, :, pl.ds(pl.multiple_of(c * 128, 128), 128)] = jnp.sum(xf * xf, axis=0, keepdims=True)

    def cross(xt):
        return jnp.dot(mu2[...], xt, preferred_element_type=F32)

    def soft(b, a2, beta, par):
        sq = sqx[b]
        grp = b // GRP
        j = b % GRP
        for h in range(BLK // 128):
            cols = slice(h * 128, (h + 1) * 128)
            t = (a2[:, cols] + sq[:, cols]) + sqmu[...]
            logit = lpb[...] - beta * t
            m = jnp.max(logit, axis=0, keepdims=True)
            e = jnp.exp(logit - m)
            r = jnp.sum(e, axis=0, keepdims=True)
            p_ref[b, :, cols] = e
            mx_ref[b, :, cols] = m
            st_own[par, grp, j, :, cols] = m + jnp.log(r)

    def send_stats(grp, par, n):
        own = st_own.at[par, pl.ds(grp, n)]
        for i in range(3):
            remote(own, st_rem.at[par, i, pl.ds(grp, n)], st_s, st_r.at[par, grp], peers[i]).start()

    def wait_stats(grp, par, n):
        three = st_rem.at[par, :, pl.ds(grp, n)]
        remote(three, three, st_s, st_r.at[par, grp], sib).wait_recv()

    def stats_sent(par):
        remote(st_rem.at[par], st_rem.at[par], st_s, st_r.at[par, 0], sib).wait_send()

    def resp(grp, par):
        st = [st_own[par, grp]] + [st_rem[par, i, grp] for i in range(3)]
        top = jnp.maximum(jnp.maximum(st[0], st[1]), jnp.maximum(st[2], st[3]))
        es = [jnp.exp(v - top) for v in st]
        tot = (es[0] + es[1]) + (es[2] + es[3])
        lse = top + jnp.log(tot)
        first = pl.multiple_of(grp * GRP, GRP)
        scale = jnp.exp(mx_ref[pl.ds(first, GRP)] - top) / tot
        cnt = nacc[...]
        for j in range(GRP):
            lse_ref[:, pl.ds(pl.multiple_of((grp * GRP + j) * BLK, BLK), BLK)] = lse[j]
            rj = p_ref[grp * GRP + j] * scale[j]
            cnt = cnt + (rj[:, 0:128] + rj[:, 128:256])
            rb[grp % 2, :, j * BLK:(j + 1) * BLK] = rj.astype(BF16)
        nacc[...] = cnt

    def gather(grp):
        rows = pl.ds(pl.multiple_of(grp * (GRP * BLK), GRP * BLK), GRP * BLK)
        s_ref[...] += jnp.dot(rb[grp % 2], xb[rows, :], preferred_element_type=F32)

    def mstep(grp, par, n=1):
        if n:
            wait_stats(grp, par, n)
        resp(grp, par)
        gather(grp)

    def zero_sums():
        nacc[...] = jnp.zeros_like(nacc)
        s_ref[...] = jnp.zeros_like(s_ref)

    def finish_sweep():
        n = jnp.sum(nacc[...], axis=1, keepdims=True)
        lp = jnp.log((n + PRIOR_ALPHA) / (ROWS + 4 * KC * PRIOR_ALPHA))
        lpb[...] = jnp.broadcast_to(lp, (KC, 128))
        mu = s_ref[...] * (1.0 / (n + EPS_COUNT))
        mu_out[side, pl.ds(cbase, KC), :] = mu

    zero_sums()
    beta0 = beta_ref[0]

    def first_block(b):
        soft(b, cross(xt_ref[b // 2, :, pl.ds(pl.multiple_of(b % 2 * BLK, BLK), BLK)]), beta0, 0)

    def own_block(n):
        @pl.when((n >= 8) & (n % 2 == 0))
        def _():
            own_copy((n - 8) // 2).wait_recv()

        b = (core * 8 + n) % 16
        prep(b, 0)
        prep(b, 1)
        first_block(b)

    ld_x.wait()

    @pl.loop(0, 4)
    def _(n):
        own_block(n)

    @pl.loop(0, NCH + 2)
    def _(it):
        @pl.when(it < NCH - 1)
        def _():
            x_copy(it).wait_recv()
            y_copy(it).start()

        @pl.when(it == NCH + 1)
        def _():
            x_copy(NCH - 1).wait_recv()
            x_copy(NCH).wait_recv()
            d_copy(NCH - 1).start()
            prep(NBLK - 1, core)

        @pl.when((it >= 3) & (it < NCH + 2))
        def _():
            y_copy(it - 3).wait_recv()
            d_copy(it - 3).start()
            prep(NBLK // 2 + it - 3, core)

        @pl.when(it < 4)
        def _():
            @pl.loop(0, 2)
            def _(k):
                own_block(4 + 2 * it + k)

        @pl.when((it >= 4) & (it < 8))
        def _():
            own_block(8 + it)

        @pl.when(it >= 4)
        def _():
            d_copy(it - 4).wait_recv()
            prep(NBLK // 2 + it - 4, 1 - core)
            first_block(NBLK // 2 + it - 4)

        @pl.when(it == NCH - 2)
        def _():
            send_stats(0, 0, 4)
            send_stats(4, 0, 2)

        @pl.when(it == NCH - 1)
        def _():
            send_stats(6, 0, 1)

    for g in (NCH - 1, NCH - 2):
        d_copy(g).wait_recv()
        prep(NBLK // 2 + g, 1 - core)
    a2 = cross(xt_ref[NBLK // 2 - 1])
    for h in range(2):
        soft(NBLK - 2 + h, a2[:, h * BLK:(h + 1) * BLK], beta0, 0)
    send_stats(7, 0, 1)
    for g in range(NGRP):
        mstep(g, 0, {0: 4, 4: 2, 6: 1, 7: 1}.get(g, 0))
    stats_sent(0)
    finish_sweep()
    set_means(mu_out[side, pl.ds(cbase, KC), :])

    def all_sent(n, sem):
        ref = xb.at[pl.ds(0, n), :]
        remote(ref, ref, sem, own_r.at[0], sib).wait_send()

    all_sent(SHARD, own_s)
    all_sent((NCH + 1) * Z, xs)
    all_sent((NCH - 1) * Z, ys)
    all_sent(NCH * 2 * Z, ds)

    def block(s, q):
        return mu_out.at[s, pl.ds(cbase + q * QC, QC), :]

    def whole(s):
        return mu_out.at[s, pl.ds(cbase, KC), :]

    def fx_copy(q):
        ref = block(side, q)
        return remote(ref, ref, fxs, fxr.at[q], xpt)

    def relay(q):
        ref = block(1 - side, q)
        return remote(ref, ref, frs, frr, sib)

    slot = side * 2 + core
    lp_devs = (sib, xpt, xdg)
    lse_copy = remote(lse_snd, lse_rcv, ls_s, ls_r, xpt)

    def send_small():
        lpbuf[slot] = jnp.transpose(lpb[...])[0:1, :]
        halves = ([], [])
        for g in range(NCH):
            piece = lse_ref[:, pl.ds(pl.multiple_of(OWN + g * (4 * Z) + core * (2 * Z), 128), 128)]
            halves[0].append(piece[:, 0:Z])
            halves[1].append(piece[:, Z:2 * Z])
        lse_snd[...] = jnp.concatenate(halves[0] + halves[1], axis=1)
        lse_out[pl.ds(side, 1), :] = lse_ref[:, pl.ds(pl.multiple_of(core * SHARD, SHARD), SHARD)]
        lse_copy.start()
        for i in range(3):
            remote(lpbuf.at[slot], lpbuf.at[slot], lps, lpr, lp_devs[i]).start()

    @pl.loop(1, SWEEPS)
    def _(t):
        par = t % 2
        beta = beta_ref[t]
        zero_sums()
        def epairs(first, n):
            for k in range(n):
                a2 = cross(xt_ref[first + k])
                for h in range(2):
                    soft(2 * (first + k) + h, a2[:, h * BLK:(h + 1) * BLK], beta, par)

        @pl.loop(0, NBLK // 8 - 1)
        def _(i):
            epairs(4 * i, 4)
            send_stats(2 * i, par, 2)

        for g in (NGRP - 2, NGRP - 1):
            epairs(2 * g, 2)
            send_stats(g, par, 1)

        for g in range(NGRP):
            mstep(g, par, 1 if g >= NGRP - 2 else 2 * (1 - g % 2))
        finish_sweep()

        @pl.when(t < SWEEPS - 1)
        def _():
            set_means(mu_out[side, pl.ds(cbase, KC), :])

        stats_sent(par)

    fx_copy(0).start()
    send_small()
    for q in range(1, NQ):
        fx_copy(q).start()
    to_sib = remote(whole(side), whole(side), fds, fdr, sib)
    to_sib.start()

    lse_copy.wait()
    lse_out[pl.ds(1 - side, 1), :] = lse_rcv[...]
    remote(lpbuf.at[pl.ds(0, 3)], lpbuf.at[pl.ds(0, 3)], lps, lpr, sib).wait()
    for s in range(2):
        for c in range(2):
            lp_out[s:s + 1, c * KC:(c + 1) * KC] = lpbuf[s * 2 + c]

    for q in range(NQ):
        fx_copy(q).wait_recv()
        relay(q).start()

    to_sib.wait()
    remote(whole(1 - side), whole(1 - side), frs, frr, sib).wait()
    remote(whole(side), whole(side), fxs, frr, xpt).wait_send()


def write_out(mu_v, lp_v, lse_v, mu_o, lp_o, lse_o, sem):
    pairs = [(lp_v, lp_o), (lse_v, lse_o)]
    for s in range(2):
        for k in range(2):
            part = pl.ds(k * KC, KC)
            pairs.append((mu_v.at[s, part, :], mu_o.at[s, part, :]))
    copies = [pltpu.make_async_copy(src, dst, sem.at[i]) for i, (src, dst) in enumerate(pairs)]
    for c in copies:
        c.start()
    for c in copies:
        c.wait()


def solution(mesh):
    def local_fit(x_local, mu_init, logpi_init, inv_temp):
        dma = pltpu.SemaphoreType.DMA
        vmem = pl.BlockSpec(memory_space=pltpu.VMEM)
        hbm = pl.BlockSpec(memory_space=pltpu.HBM)
        outs = [jax.ShapeDtypeStruct(mu_init.shape, F32),
                jax.ShapeDtypeStruct(logpi_init.shape, F32),
                jax.ShapeDtypeStruct((2, x_local.shape[0]), F32)]
        res = pl.pallas_call(
            body,
            out_shape=tuple(pltpu.VMEM(o.shape, o.dtype) for o in outs),
            in_specs=[hbm] * 4,
            out_specs=(vmem, vmem, vmem),
            scratch_shapes=[
                pltpu.VMEM((ROWS, HALF), BF16),
                pltpu.VMEM((NBLK // 2, HALF, 2 * BLK), BF16),
                pltpu.VMEM((NBLK, KC, BLK), F32),
                pltpu.VMEM((2, KC, GRP * BLK), BF16),
                pltpu.VMEM((PRE * Z, HALF), BF16),
                pltpu.VMEM((2, 2 * KC), F32),
                pltpu.SMEM((SWEEPS,), F32),
                pltpu.VMEM((KC, HALF), F32),
                pltpu.VMEM((KC, 128), F32),
                pltpu.VMEM((KC, HALF), F32),
                pltpu.VMEM((KC, HALF), BF16),
                pltpu.VMEM((KC, 128), F32),
                pltpu.VMEM((KC, 128), F32),
                pltpu.VMEM((NBLK, 1, BLK), F32),
                pltpu.VMEM((NBLK, 1, BLK), F32),
                pltpu.VMEM((1, ROWS), F32),
                pltpu.VMEM((2, NGRP, GRP, 1, BLK), F32),
                pltpu.VMEM((2, 3, NGRP, GRP, 1, BLK), F32),
                pltpu.VMEM((4, 1, KC), F32),
                pltpu.VMEM((1, SHARD), F32),
                pltpu.VMEM((1, SHARD), F32),
                dma((5,)),
                dma, dma((NCH + 1,)),
                dma, dma((NCH - 1,)),
                dma, dma((NCH,)),
                dma, dma((NOWN,)),
                dma, dma((2, NGRP)),
                dma, dma,
                dma, dma,
                dma, dma((NQ,)),
                dma, dma,
                dma, dma,
            ],
            compiler_params=pltpu.CompilerParams(
                collective_id=0, has_side_effects=True,
                vmem_limit_bytes=56 * 1024 * 1024),
        )(x_local, mu_init, logpi_init, inv_temp)
        return pl.pallas_call(
            write_out,
            out_shape=tuple(outs),
            in_specs=[vmem] * 3,
            out_specs=(hbm,) * 3,
            scratch_shapes=[dma((6,))],
        )(*[pltpu.with_memory_space_constraint(r, pltpu.VMEM) for r in res])

    return jax.shard_map(
        local_fit,
        mesh=mesh,
        in_specs=(P(("grp", "row"), None), P(None, ("grp", "comp"), None), P(None, ("grp", "comp")), P()),
        out_specs=(P(None, ("grp", "comp"), None), P(None, ("grp", "comp")), P(None, ("grp", "row"))),
        check_vma=False,
    )
```

```python
import jax
import jax.numpy as jnp
from jax import lax
from jax.experimental import pallas as pl
from jax.experimental.pallas import tpu as pltpu
from jax.sharding import PartitionSpec as P

EPS_COUNT = 1e-6
PRIOR_ALPHA = 1e-3

F32 = jnp.float32
BF16 = jnp.bfloat16
MESH = pl.DeviceIdType.MESH

SWEEPS = 3
HALF = 512
SHARD = 2048
ROWS = 8192
KC = 256
BLK = 256
NBLK = ROWS // BLK
GRP = 4
NGRP = NBLK // GRP
NCH = 16
Z = SHARD // 2 // NCH
PRE = 4
NOWN = 4
PIECE = SHARD // NOWN
OWN = 2 * SHARD
NQ = 5
QUARTERS = ((0, 64), (64, 64), (128, 64), (192, 48), (240, 16))


def body(x_hbm, mu_hbm, lp_hbm, beta_hbm,
         mu_out, lp_out, lse_out,
         xb, xt_ref, p_ref, rb, xpre, lp_in, beta_ref, s_ref, nacc, mu_f, mu2, sqmu, lpb, sqx, mx_ref, lse_ref,
         st_own, st_rem, lpbuf, lse_snd, lse_rcv,
         loc_sem, xs, xr, ys, yr, ds, dr, own_s, own_r,
         st_s, st_r, lps, lpr, ls_s, ls_r, fxs, fxr, fds, fdr, frs, frr):
    comp = lax.axis_index("comp")
    row = lax.axis_index("row")
    side = row // 2
    core = row % 2
    sib = {"row": side * 2 + (1 - core)}
    ypt = {"comp": 1 - comp}
    ydg = {"comp": 1 - comp, "row": side * 2 + (1 - core)}
    xpt = {"row": (1 - side) * 2 + core}
    xdg = {"row": (1 - side) * 2 + (1 - core)}
    peers = (sib, ypt, ydg)

    barrier = pltpu.get_barrier_semaphore()
    for dev in (xpt, sib, ypt, ydg, xdg):
        pl.semaphore_signal(barrier, inc=1, device_id=dev, device_id_type=MESH)

    def remote(src, dst, ssem, rsem, dev):
        return pltpu.make_async_remote_copy(
            src_ref=src, dst_ref=dst, send_sem=ssem, recv_sem=rsem,
            device_id=dev, device_id_type=MESH)

    fit_cols = pl.ds(pl.multiple_of(side * HALF, HALF), HALF)
    oth_cols = pl.ds(pl.multiple_of((1 - side) * HALF, HALF), HALF)
    cbase = pl.multiple_of(core * KC, KC)

    def own_rows(c):
        return xb.at[pl.ds(pl.multiple_of(c * SHARD, SHARD), SHARD), :]

    ld_x = pltpu.make_async_copy(x_hbm.at[:, fit_cols], own_rows(core), loc_sem.at[0])
    ld_mu = pltpu.make_async_copy(mu_hbm.at[side, pl.ds(cbase, KC), :], mu_f, loc_sem.at[1])
    ld_pre = pltpu.make_async_copy(
        x_hbm.at[pl.ds(pl.multiple_of(comp * (SHARD // 2), PRE * Z), PRE * Z), oth_cols],
        xpre, loc_sem.at[2])
    ld_lp = pltpu.make_async_copy(lp_hbm, lp_in, loc_sem.at[3])
    ld_beta = pltpu.make_async_copy(beta_hbm, beta_ref, loc_sem.at[4])
    ld_pre.start()
    ld_mu.start()
    ld_lp.start()
    ld_beta.start()
    ld_x.start()

    def place(g, c, half, n):
        return xb.at[pl.ds(pl.multiple_of(OWN + g * (4 * Z) + c * (2 * Z) + half * Z, Z), n), :]

    def x_copy(g):
        extra = g // NCH
        g0 = g - extra
        half = comp + extra * (1 - 2 * comp)
        src = x_hbm.at[pl.ds(pl.multiple_of(half * (SHARD // 2) + g0 * Z, Z), Z), oth_cols]
        return remote(src, place(g0, core, half, Z), xs, xr.at[g], xpt)

    def y_copy(g):
        ref = place(g, core, comp, Z)
        return remote(ref, ref, ys, yr.at[g], ypt)

    def d_copy(g):
        ref = place(g, core, 0, 2 * Z)
        return remote(ref, ref, ds, dr.at[g], sib)

    def own_copy(k):
        src = x_hbm.at[pl.ds(pl.multiple_of(k * PIECE, PIECE), PIECE), fit_cols]
        dst = xb.at[pl.ds(pl.multiple_of(core * SHARD + k * PIECE, PIECE), PIECE), :]
        return remote(src, dst, own_s, own_r.at[k], sib)

    pl.semaphore_wait(barrier, 5)
    ld_pre.wait()
    for g in range(PRE):
        remote(xpre.at[pl.ds(g * Z, Z), :], place(g, core, comp, Z), xs, xr.at[g], xpt).start()
    for k in range(NOWN):
        own_copy(k).start()

    @pl.loop(PRE, NCH + 1)
    def _(g):
        x_copy(g).start()

    def bc(row_vec):
        return jnp.transpose(jnp.broadcast_to(row_vec, (128, KC)))

    def set_means(mu):
        mu2[...] = mu.astype(BF16) * jnp.asarray(-2.0, BF16)
        sqmu[...] = jnp.broadcast_to(jnp.sum(mu * mu, axis=1, keepdims=True), (KC, 128))

    ld_lp.wait()
    ld_beta.wait()
    lpb[...] = bc(lp_in[pl.ds(side, 1), pl.ds(cbase, KC)])
    ld_mu.wait()
    set_means(mu_f[...])

    def prep(b, c):
        rows = pl.ds(pl.multiple_of(b * BLK + c * 128, 128), 128)
        xt = jnp.transpose(xb[rows, :])
        xt_ref[b // 2, :, pl.ds(pl.multiple_of(b % 2 * BLK + c * 128, 128), 128)] = xt
        xf = xt.astype(F32)
        sqx[b, :, pl.ds(pl.multiple_of(c * 128, 128), 128)] = jnp.sum(xf * xf, axis=0, keepdims=True)

    def cross(xt):
        return jnp.dot(mu2[...], xt, preferred_element_type=F32)

    def soft(b, a2, beta, par):
        sq = sqx[b]
        grp = b // GRP
        j = b % GRP
        for h in range(BLK // 128):
            cols = slice(h * 128, (h + 1) * 128)
            t = (a2[:, cols] + sq[:, cols]) + sqmu[...]
            logit = lpb[...] - beta * t
            m = jnp.max(logit, axis=0, keepdims=True)
            e = jnp.exp(logit - m)
            r = jnp.sum(e, axis=0, keepdims=True)
            p_ref[b, :, cols] = e
            mx_ref[b, :, cols] = m
            st_own[par, grp, j, :, cols] = m + jnp.log(r)

    def send_stats(grp, par, n):
        own = st_own.at[par, pl.ds(grp, n)]
        for i in range(3):
            remote(own, st_rem.at[par, i, pl.ds(grp, n)], st_s, st_r.at[par, grp], peers[i]).start()

    def wait_stats(grp, par, n):
        three = st_rem.at[par, :, pl.ds(grp, n)]
        remote(three, three, st_s, st_r.at[par, grp], sib).wait_recv()

    def stats_sent(par):
        remote(st_rem.at[par], st_rem.at[par], st_s, st_r.at[par, 0], sib).wait_send()

    def resp(grp, par):
        st = [st_own[par, grp]] + [st_rem[par, i, grp] for i in range(3)]
        top = jnp.maximum(jnp.maximum(st[0], st[1]), jnp.maximum(st[2], st[3]))
        es = [jnp.exp(v - top) for v in st]
        tot = (es[0] + es[1]) + (es[2] + es[3])
        lse = top + jnp.log(tot)
        first = pl.multiple_of(grp * GRP, GRP)
        scale = jnp.exp(mx_ref[pl.ds(first, GRP)] - top) / tot
        cnt = nacc[...]
        for j in range(GRP):
            lse_ref[:, pl.ds(pl.multiple_of((grp * GRP + j) * BLK, BLK), BLK)] = lse[j]
            rj = p_ref[grp * GRP + j] * scale[j]
            cnt = cnt + (rj[:, 0:128] + rj[:, 128:256])
            rb[grp % 2, :, j * BLK:(j + 1) * BLK] = rj.astype(BF16)
        nacc[...] = cnt

    def gather(grp):
        rows = pl.ds(pl.multiple_of(grp * (GRP * BLK), GRP * BLK), GRP * BLK)
        s_ref[...] += jnp.dot(rb[grp % 2], xb[rows, :], preferred_element_type=F32)

    def mstep(grp, par, n=1):
        if n:
            wait_stats(grp, par, n)
        resp(grp, par)
        gather(grp)

    def zero_sums():
        nacc[...] = jnp.zeros_like(nacc)
        s_ref[...] = jnp.zeros_like(s_ref)

    def finish_sweep():
        n = jnp.sum(nacc[...], axis=1, keepdims=True)
        lp = jnp.log((n + PRIOR_ALPHA) / (ROWS + 4 * KC * PRIOR_ALPHA))
        lpb[...] = jnp.broadcast_to(lp, (KC, 128))
        mu = s_ref[...] * (1.0 / (n + EPS_COUNT))
        mu_out[side, pl.ds(cbase, KC), :] = mu

    zero_sums()
    beta0 = beta_ref[0]

    def first_block(b):
        soft(b, cross(xt_ref[b // 2, :, pl.ds(pl.multiple_of(b % 2 * BLK, BLK), BLK)]), beta0, 0)

    def own_block(n):
        @pl.when((n >= 8) & (n % 2 == 0))
        def _():
            own_copy((n - 8) // 2).wait_recv()

        b = (core * 8 + n) % 16
        prep(b, 0)
        prep(b, 1)
        first_block(b)

    ld_x.wait()

    @pl.loop(0, 4)
    def _(n):
        own_block(n)

    @pl.loop(0, NCH + 2)
    def _(it):
        @pl.when(it < NCH - 1)
        def _():
            x_copy(it).wait_recv()
            y_copy(it).start()

        @pl.when(it == NCH + 1)
        def _():
            x_copy(NCH - 1).wait_recv()
            x_copy(NCH).wait_recv()
            d_copy(NCH - 1).start()
            prep(NBLK - 1, core)

        @pl.when((it >= 3) & (it < NCH + 2))
        def _():
            y_copy(it - 3).wait_recv()
            d_copy(it - 3).start()
            prep(NBLK // 2 + it - 3, core)

        @pl.when(it < 4)
        def _():
            @pl.loop(0, 2)
            def _(k):
                own_block(4 + 2 * it + k)

        @pl.when((it >= 4) & (it < 8))
        def _():
            own_block(8 + it)

        @pl.when(it >= 4)
        def _():
            d_copy(it - 4).wait_recv()
            prep(NBLK // 2 + it - 4, 1 - core)
            first_block(NBLK // 2 + it - 4)

        @pl.when(it == NCH - 2)
        def _():
            send_stats(0, 0, 4)
            send_stats(4, 0, 2)

        @pl.when(it == NCH - 1)
        def _():
            send_stats(6, 0, 1)

    for g in (NCH - 1, NCH - 2):
        d_copy(g).wait_recv()
        prep(NBLK // 2 + g, 1 - core)
    a2 = cross(xt_ref[NBLK // 2 - 1])
    for h in range(2):
        soft(NBLK - 2 + h, a2[:, h * BLK:(h + 1) * BLK], beta0, 0)
    send_stats(7, 0, 1)
    for g in range(NGRP):
        mstep(g, 0, {0: 4, 4: 2, 6: 1, 7: 1}.get(g, 0))
    stats_sent(0)
    finish_sweep()
    set_means(mu_out[side, pl.ds(cbase, KC), :])

    def all_sent(n, sem):
        ref = xb.at[pl.ds(0, n), :]
        remote(ref, ref, sem, own_r.at[0], sib).wait_send()

    all_sent(SHARD, own_s)
    all_sent((NCH + 1) * Z, xs)
    all_sent((NCH - 1) * Z, ys)
    all_sent(NCH * 2 * Z, ds)

    def block(s, q):
        return mu_out.at[s, pl.ds(cbase + QUARTERS[q][0], QUARTERS[q][1]), :]

    def whole(s):
        return mu_out.at[s, pl.ds(cbase, KC), :]

    def fx_copy(q):
        ref = block(side, q)
        return remote(ref, ref, fxs, fxr.at[q], xpt)

    def relay(q):
        ref = block(1 - side, q)
        return remote(ref, ref, frs, frr, sib)

    slot = side * 2 + core
    lp_devs = (sib, xpt, xdg)
    lse_copy = remote(lse_snd, lse_rcv, ls_s, ls_r, xpt)

    def send_small():
        lpbuf[slot] = jnp.transpose(lpb[...])[0:1, :]
        halves = ([], [])
        for g in range(NCH):
            piece = lse_ref[:, pl.ds(pl.multiple_of(OWN + g * (4 * Z) + core * (2 * Z), 128), 128)]
            halves[0].append(piece[:, 0:Z])
            halves[1].append(piece[:, Z:2 * Z])
        lse_snd[...] = jnp.concatenate(halves[0] + halves[1], axis=1)
        lse_out[pl.ds(side, 1), :] = lse_ref[:, pl.ds(pl.multiple_of(core * SHARD, SHARD), SHARD)]
        lse_copy.start()
        for i in range(3):
            remote(lpbuf.at[slot], lpbuf.at[slot], lps, lpr, lp_devs[i]).start()

    @pl.loop(1, SWEEPS)
    def _(t):
        par = t % 2
        beta = beta_ref[t]
        zero_sums()
        def epairs(first, n):
            for k in range(n):
                a2 = cross(xt_ref[first + k])
                for h in range(2):
                    soft(2 * (first + k) + h, a2[:, h * BLK:(h + 1) * BLK], beta, par)

        @pl.loop(0, NBLK // 8 - 1)
        def _(i):
            epairs(4 * i, 4)
            send_stats(2 * i, par, 2)

        for g in (NGRP - 2, NGRP - 1):
            epairs(2 * g, 2)
            send_stats(g, par, 1)

        for g in range(NGRP):
            mstep(g, par, 1 if g >= NGRP - 2 else 2 * (1 - g % 2))
        finish_sweep()

        @pl.when(t < SWEEPS - 1)
        def _():
            set_means(mu_out[side, pl.ds(cbase, KC), :])

        stats_sent(par)

    fx_copy(0).start()
    send_small()
    for q in range(1, NQ):
        fx_copy(q).start()
    to_sib = remote(whole(side), whole(side), fds, fdr, sib)
    to_sib.start()

    lse_copy.wait()
    lse_out[pl.ds(1 - side, 1), :] = lse_rcv[...]
    remote(lpbuf.at[pl.ds(0, 3)], lpbuf.at[pl.ds(0, 3)], lps, lpr, sib).wait()
    for s in range(2):
        for c in range(2):
            lp_out[s:s + 1, c * KC:(c + 1) * KC] = lpbuf[s * 2 + c]

    for q in range(NQ):
        fx_copy(q).wait_recv()
        relay(q).start()

    to_sib.wait()
    remote(whole(1 - side), whole(1 - side), frs, frr, sib).wait()
    remote(whole(side), whole(side), fxs, frr, xpt).wait_send()


def write_out(mu_v, lp_v, lse_v, mu_o, lp_o, lse_o, sem):
    pairs = [(lp_v, lp_o), (lse_v, lse_o)]
    for s in range(2):
        for k in range(2):
            part = pl.ds(k * KC, KC)
            pairs.append((mu_v.at[s, part, :], mu_o.at[s, part, :]))
    copies = [pltpu.make_async_copy(src, dst, sem.at[i]) for i, (src, dst) in enumerate(pairs)]
    for c in copies:
        c.start()
    for c in copies:
        c.wait()


def solution(mesh):
    def local_fit(x_local, mu_init, logpi_init, inv_temp):
        dma = pltpu.SemaphoreType.DMA
        vmem = pl.BlockSpec(memory_space=pltpu.VMEM)
        hbm = pl.BlockSpec(memory_space=pltpu.HBM)
        outs = [jax.ShapeDtypeStruct(mu_init.shape, F32),
                jax.ShapeDtypeStruct(logpi_init.shape, F32),
                jax.ShapeDtypeStruct((2, x_local.shape[0]), F32)]
        res = pl.pallas_call(
            body,
            out_shape=tuple(pltpu.VMEM(o.shape, o.dtype) for o in outs),
            in_specs=[hbm] * 4,
            out_specs=(vmem, vmem, vmem),
            scratch_shapes=[
                pltpu.VMEM((ROWS, HALF), BF16),
                pltpu.VMEM((NBLK // 2, HALF, 2 * BLK), BF16),
                pltpu.VMEM((NBLK, KC, BLK), F32),
                pltpu.VMEM((2, KC, GRP * BLK), BF16),
                pltpu.VMEM((PRE * Z, HALF), BF16),
                pltpu.VMEM((2, 2 * KC), F32),
                pltpu.SMEM((SWEEPS,), F32),
                pltpu.VMEM((KC, HALF), F32),
                pltpu.VMEM((KC, 128), F32),
                pltpu.VMEM((KC, HALF), F32),
                pltpu.VMEM((KC, HALF), BF16),
                pltpu.VMEM((KC, 128), F32),
                pltpu.VMEM((KC, 128), F32),
                pltpu.VMEM((NBLK, 1, BLK), F32),
                pltpu.VMEM((NBLK, 1, BLK), F32),
                pltpu.VMEM((1, ROWS), F32),
                pltpu.VMEM((2, NGRP, GRP, 1, BLK), F32),
                pltpu.VMEM((2, 3, NGRP, GRP, 1, BLK), F32),
                pltpu.VMEM((4, 1, KC), F32),
                pltpu.VMEM((1, SHARD), F32),
                pltpu.VMEM((1, SHARD), F32),
                dma((5,)),
                dma, dma((NCH + 1,)),
                dma, dma((NCH - 1,)),
                dma, dma((NCH,)),
                dma, dma((NOWN,)),
                dma, dma((2, NGRP)),
                dma, dma,
                dma, dma,
                dma, dma((NQ,)),
                dma, dma,
                dma, dma,
            ],
            compiler_params=pltpu.CompilerParams(
                collective_id=0, has_side_effects=True,
                vmem_limit_bytes=56 * 1024 * 1024),
        )(x_local, mu_init, logpi_init, inv_temp)
        return pl.pallas_call(
            write_out,
            out_shape=tuple(outs),
            in_specs=[vmem] * 3,
            out_specs=(hbm,) * 3,
            scratch_shapes=[dma((6,))],
        )(*[pltpu.with_memory_space_constraint(r, pltpu.VMEM) for r in res])

    return jax.shard_map(
        local_fit,
        mesh=mesh,
        in_specs=(P(("grp", "row"), None), P(None, ("grp", "comp"), None), P(None, ("grp", "comp")), P()),
        out_specs=(P(None, ("grp", "comp"), None), P(None, ("grp", "comp")), P(None, ("grp", "row"))),
        check_vma=False,
    )
```

```python
import jax
import jax.numpy as jnp
from jax import lax
from jax.experimental import pallas as pl
from jax.experimental.pallas import tpu as pltpu
from jax.sharding import PartitionSpec as P

EPS_COUNT = 1e-6
PRIOR_ALPHA = 1e-3

F32 = jnp.float32
BF16 = jnp.bfloat16
MESH = pl.DeviceIdType.MESH

SWEEPS = 3
HALF = 512
SHARD = 2048
ROWS = 8192
KC = 256
BLK = 256
NBLK = ROWS // BLK
GRP = 4
NGRP = NBLK // GRP
NCH = 16
Z = SHARD // 2 // NCH
PRE = 4
NOWN = 4
PIECE = SHARD // NOWN
OWN = 2 * SHARD
NQ = 5
QUARTERS = ((0, 64), (64, 64), (128, 64), (192, 48), (240, 16))


def body(x_hbm, mu_hbm, lp_hbm, beta_hbm,
         mu_out, lp_out, lse_out,
         xb, xt_ref, p_ref, rb, xpre, lp_in, beta_ref, s_ref, nacc, mu_f, mu2, sqmu, lpb, sqx, mx_ref, lse_ref,
         st_own, st_rem, lpbuf, lse_snd, lse_rcv,
         loc_sem, xs, xr, ys, yr, ds, dr, own_s, own_r,
         st_s, st_r, lps, lpr, ls_s, ls_r, fxs, fxr):
    comp = lax.axis_index("comp")
    row = lax.axis_index("row")
    side = row // 2
    core = row % 2
    sib = {"row": side * 2 + (1 - core)}
    ypt = {"comp": 1 - comp}
    ydg = {"comp": 1 - comp, "row": side * 2 + (1 - core)}
    xpt = {"row": (1 - side) * 2 + core}
    xdg = {"row": (1 - side) * 2 + (1 - core)}
    peers = (sib, ypt, ydg)

    barrier = pltpu.get_barrier_semaphore()
    for dev in (xpt, sib, ypt, ydg, xdg):
        pl.semaphore_signal(barrier, inc=1, device_id=dev, device_id_type=MESH)

    def remote(src, dst, ssem, rsem, dev):
        return pltpu.make_async_remote_copy(
            src_ref=src, dst_ref=dst, send_sem=ssem, recv_sem=rsem,
            device_id=dev, device_id_type=MESH)

    fit_cols = pl.ds(pl.multiple_of(side * HALF, HALF), HALF)
    oth_cols = pl.ds(pl.multiple_of((1 - side) * HALF, HALF), HALF)
    cbase = pl.multiple_of(core * KC, KC)

    def own_rows(c):
        return xb.at[pl.ds(pl.multiple_of(c * SHARD, SHARD), SHARD), :]

    ld_x = pltpu.make_async_copy(x_hbm.at[:, fit_cols], own_rows(core), loc_sem.at[0])
    ld_mu = pltpu.make_async_copy(mu_hbm.at[side, pl.ds(cbase, KC), :], mu_f, loc_sem.at[1])
    ld_pre = pltpu.make_async_copy(
        x_hbm.at[pl.ds(pl.multiple_of(comp * (SHARD // 2), PRE * Z), PRE * Z), oth_cols],
        xpre, loc_sem.at[2])
    ld_lp = pltpu.make_async_copy(lp_hbm, lp_in, loc_sem.at[3])
    ld_beta = pltpu.make_async_copy(beta_hbm, beta_ref, loc_sem.at[4])
    ld_pre.start()
    ld_mu.start()
    ld_lp.start()
    ld_beta.start()
    ld_x.start()

    def place(g, c, half, n):
        return xb.at[pl.ds(pl.multiple_of(OWN + g * (4 * Z) + c * (2 * Z) + half * Z, Z), n), :]

    def x_copy(g):
        extra = g // NCH
        g0 = g - extra
        half = comp + extra * (1 - 2 * comp)
        src = x_hbm.at[pl.ds(pl.multiple_of(half * (SHARD // 2) + g0 * Z, Z), Z), oth_cols]
        return remote(src, place(g0, core, half, Z), xs, xr.at[g], xpt)

    def y_copy(g):
        ref = place(g, core, comp, Z)
        return remote(ref, ref, ys, yr.at[g], ypt)

    def d_copy(g):
        ref = place(g, core, 0, 2 * Z)
        return remote(ref, ref, ds, dr.at[g], sib)

    def own_copy(k):
        src = x_hbm.at[pl.ds(pl.multiple_of(k * PIECE, PIECE), PIECE), fit_cols]
        dst = xb.at[pl.ds(pl.multiple_of(core * SHARD + k * PIECE, PIECE), PIECE), :]
        return remote(src, dst, own_s, own_r.at[k], sib)

    pl.semaphore_wait(barrier, 5)
    ld_pre.wait()
    for g in range(PRE):
        remote(xpre.at[pl.ds(g * Z, Z), :], place(g, core, comp, Z), xs, xr.at[g], xpt).start()
    for k in range(NOWN):
        own_copy(k).start()

    @pl.loop(PRE, NCH + 1)
    def _(g):
        x_copy(g).start()

    def bc(row_vec):
        return jnp.transpose(jnp.broadcast_to(row_vec, (128, KC)))

    def set_means(mu):
        mu2[...] = mu.astype(BF16) * jnp.asarray(-2.0, BF16)
        sqmu[...] = jnp.broadcast_to(jnp.sum(mu * mu, axis=1, keepdims=True), (KC, 128))

    ld_lp.wait()
    ld_beta.wait()
    lpb[...] = bc(lp_in[pl.ds(side, 1), pl.ds(cbase, KC)])
    ld_mu.wait()
    set_means(mu_f[...])

    def prep(b, c):
        rows = pl.ds(pl.multiple_of(b * BLK + c * 128, 128), 128)
        xt = jnp.transpose(xb[rows, :])
        xt_ref[b // 2, :, pl.ds(pl.multiple_of(b % 2 * BLK + c * 128, 128), 128)] = xt
        xf = xt.astype(F32)
        sqx[b, :, pl.ds(pl.multiple_of(c * 128, 128), 128)] = jnp.sum(xf * xf, axis=0, keepdims=True)

    def cross(xt):
        return jnp.dot(mu2[...], xt, preferred_element_type=F32)

    def soft(b, a2, beta, par):
        sq = sqx[b]
        grp = b // GRP
        j = b % GRP
        for h in range(BLK // 128):
            cols = slice(h * 128, (h + 1) * 128)
            t = (a2[:, cols] + sq[:, cols]) + sqmu[...]
            logit = lpb[...] - beta * t
            m = jnp.max(logit, axis=0, keepdims=True)
            e = jnp.exp(logit - m)
            r = jnp.sum(e, axis=0, keepdims=True)
            p_ref[b, :, cols] = e
            mx_ref[b, :, cols] = m
            st_own[par, grp, j, :, cols] = m + jnp.log(r)

    def send_stats(grp, par, n):
        own = st_own.at[par, pl.ds(grp, n)]
        for i in range(3):
            remote(own, st_rem.at[par, i, pl.ds(grp, n)], st_s, st_r.at[par, grp], peers[i]).start()

    def wait_stats(grp, par, n):
        three = st_rem.at[par, :, pl.ds(grp, n)]
        remote(three, three, st_s, st_r.at[par, grp], sib).wait_recv()

    def stats_sent(par):
        remote(st_rem.at[par], st_rem.at[par], st_s, st_r.at[par, 0], sib).wait_send()

    def resp(grp, par):
        st = [st_own[par, grp]] + [st_rem[par, i, grp] for i in range(3)]
        top = jnp.maximum(jnp.maximum(st[0], st[1]), jnp.maximum(st[2], st[3]))
        es = [jnp.exp(v - top) for v in st]
        tot = (es[0] + es[1]) + (es[2] + es[3])
        lse = top + jnp.log(tot)
        first = pl.multiple_of(grp * GRP, GRP)
        scale = jnp.exp(mx_ref[pl.ds(first, GRP)] - top) / tot
        cnt = nacc[...]
        for j in range(GRP):
            lse_ref[:, pl.ds(pl.multiple_of((grp * GRP + j) * BLK, BLK), BLK)] = lse[j]
            rj = p_ref[grp * GRP + j] * scale[j]
            cnt = cnt + (rj[:, 0:128] + rj[:, 128:256])
            rb[grp % 2, :, j * BLK:(j + 1) * BLK] = rj.astype(BF16)
        nacc[...] = cnt

    def gather(grp):
        rows = pl.ds(pl.multiple_of(grp * (GRP * BLK), GRP * BLK), GRP * BLK)
        s_ref[...] += jnp.dot(rb[grp % 2], xb[rows, :], preferred_element_type=F32)

    def mstep(grp, par, n=1):
        if n:
            wait_stats(grp, par, n)
        resp(grp, par)
        gather(grp)

    def zero_sums():
        nacc[...] = jnp.zeros_like(nacc)
        s_ref[...] = jnp.zeros_like(s_ref)

    def finish_sweep():
        n = jnp.sum(nacc[...], axis=1, keepdims=True)
        lp = jnp.log((n + PRIOR_ALPHA) / (ROWS + 4 * KC * PRIOR_ALPHA))
        lpb[...] = jnp.broadcast_to(lp, (KC, 128))
        mu = s_ref[...] * (1.0 / (n + EPS_COUNT))
        mu_out[side, pl.ds(cbase, KC), :] = mu

    zero_sums()
    beta0 = beta_ref[0]

    def first_block(b):
        soft(b, cross(xt_ref[b // 2, :, pl.ds(pl.multiple_of(b % 2 * BLK, BLK), BLK)]), beta0, 0)

    def own_block(n):
        @pl.when((n >= 8) & (n % 2 == 0))
        def _():
            own_copy((n - 8) // 2).wait_recv()

        b = (core * 8 + n) % 16
        prep(b, 0)
        prep(b, 1)
        first_block(b)

    ld_x.wait()

    @pl.loop(0, 4)
    def _(n):
        own_block(n)

    @pl.loop(0, NCH + 2)
    def _(it):
        @pl.when(it < NCH - 1)
        def _():
            x_copy(it).wait_recv()
            y_copy(it).start()

        @pl.when(it == NCH + 1)
        def _():
            x_copy(NCH - 1).wait_recv()
            x_copy(NCH).wait_recv()
            d_copy(NCH - 1).start()
            prep(NBLK - 1, core)

        @pl.when((it >= 3) & (it < NCH + 2))
        def _():
            y_copy(it - 3).wait_recv()
            d_copy(it - 3).start()
            prep(NBLK // 2 + it - 3, core)

        @pl.when(it < 4)
        def _():
            @pl.loop(0, 2)
            def _(k):
                own_block(4 + 2 * it + k)

        @pl.when((it >= 4) & (it < 8))
        def _():
            own_block(8 + it)

        @pl.when(it >= 4)
        def _():
            d_copy(it - 4).wait_recv()
            prep(NBLK // 2 + it - 4, 1 - core)
            first_block(NBLK // 2 + it - 4)

        @pl.when(it == NCH - 2)
        def _():
            send_stats(0, 0, 4)
            send_stats(4, 0, 2)

        @pl.when(it == NCH - 1)
        def _():
            send_stats(6, 0, 1)

    for g in (NCH - 1, NCH - 2):
        d_copy(g).wait_recv()
        prep(NBLK // 2 + g, 1 - core)
    a2 = cross(xt_ref[NBLK // 2 - 1])
    for h in range(2):
        soft(NBLK - 2 + h, a2[:, h * BLK:(h + 1) * BLK], beta0, 0)
    send_stats(7, 0, 1)
    for g in range(NGRP):
        mstep(g, 0, {0: 4, 4: 2, 6: 1, 7: 1}.get(g, 0))
    stats_sent(0)
    finish_sweep()
    set_means(mu_out[side, pl.ds(cbase, KC), :])

    def all_sent(n, sem):
        ref = xb.at[pl.ds(0, n), :]
        remote(ref, ref, sem, own_r.at[0], sib).wait_send()

    all_sent(SHARD, own_s)
    all_sent((NCH + 1) * Z, xs)
    all_sent((NCH - 1) * Z, ys)
    all_sent(NCH * 2 * Z, ds)

    def block(s, q):
        return mu_out.at[s, pl.ds(cbase + QUARTERS[q][0], QUARTERS[q][1]), :]

    def whole(s):
        return mu_out.at[s, pl.ds(cbase, KC), :]

    def fx_copy(q):
        ref = block(side, q)
        return remote(ref, ref, fxs, fxr.at[q], xpt)

    def relay(q):
        ref = block(1 - side, q)
        return remote(ref, ref, ds, dr.at[0], sib)

    slot = side * 2 + core
    lp_devs = (sib, xpt, xdg)
    lse_copy = remote(lse_snd, lse_rcv, ls_s, ls_r, xpt)

    def send_small():
        lpbuf[slot] = jnp.transpose(lpb[...])[0:1, :]
        halves = ([], [])
        for g in range(NCH):
            piece = lse_ref[:, pl.ds(pl.multiple_of(OWN + g * (4 * Z) + core * (2 * Z), 128), 128)]
            halves[0].append(piece[:, 0:Z])
            halves[1].append(piece[:, Z:2 * Z])
        lse_snd[...] = jnp.concatenate(halves[0] + halves[1], axis=1)
        lse_out[pl.ds(side, 1), :] = lse_ref[:, pl.ds(pl.multiple_of(core * SHARD, SHARD), SHARD)]
        lse_copy.start()
        for i in range(3):
            remote(lpbuf.at[slot], lpbuf.at[slot], lps, lpr, lp_devs[i]).start()

    @pl.loop(1, SWEEPS)
    def _(t):
        par = t % 2
        beta = beta_ref[t]
        zero_sums()
        def epairs(first, n):
            for k in range(n):
                a2 = cross(xt_ref[first + k])
                for h in range(2):
                    soft(2 * (first + k) + h, a2[:, h * BLK:(h + 1) * BLK], beta, par)

        @pl.loop(0, NBLK // 8 - 1)
        def _(i):
            epairs(4 * i, 4)
            send_stats(2 * i, par, 2)

        for g in (NGRP - 2, NGRP - 1):
            epairs(2 * g, 2)
            send_stats(g, par, 1)

        for g in range(NGRP):
            mstep(g, par, 1 if g >= NGRP - 2 else 2 * (1 - g % 2))
        finish_sweep()

        @pl.when(t < SWEEPS - 1)
        def _():
            set_means(mu_out[side, pl.ds(cbase, KC), :])

        stats_sent(par)

    fx_copy(0).start()
    send_small()
    for q in range(1, NQ):
        fx_copy(q).start()
    to_sib = remote(whole(side), whole(side), own_s, own_r.at[0], sib)
    to_sib.start()

    lse_copy.wait()
    lse_out[pl.ds(1 - side, 1), :] = lse_rcv[...]
    remote(lpbuf.at[pl.ds(0, 3)], lpbuf.at[pl.ds(0, 3)], lps, lpr, sib).wait()
    for s in range(2):
        for c in range(2):
            lp_out[s:s + 1, c * KC:(c + 1) * KC] = lpbuf[s * 2 + c]

    for q in range(NQ):
        fx_copy(q).wait_recv()
        relay(q).start()

    to_sib.wait()
    remote(whole(1 - side), whole(1 - side), ds, dr.at[0], sib).wait()
    remote(whole(side), whole(side), fxs, dr.at[0], xpt).wait_send()


def write_out(mu_v, lp_v, lse_v, mu_o, lp_o, lse_o, sem):
    pairs = [(lp_v, lp_o), (lse_v, lse_o)]
    for s in range(2):
        for k in range(2):
            part = pl.ds(k * KC, KC)
            pairs.append((mu_v.at[s, part, :], mu_o.at[s, part, :]))
    copies = [pltpu.make_async_copy(src, dst, sem.at[i]) for i, (src, dst) in enumerate(pairs)]
    for c in copies:
        c.start()
    for c in copies:
        c.wait()


def solution(mesh):
    def local_fit(x_local, mu_init, logpi_init, inv_temp):
        dma = pltpu.SemaphoreType.DMA
        vmem = pl.BlockSpec(memory_space=pltpu.VMEM)
        hbm = pl.BlockSpec(memory_space=pltpu.HBM)
        outs = [jax.ShapeDtypeStruct(mu_init.shape, F32),
                jax.ShapeDtypeStruct(logpi_init.shape, F32),
                jax.ShapeDtypeStruct((2, x_local.shape[0]), F32)]
        res = pl.pallas_call(
            body,
            out_shape=tuple(pltpu.VMEM(o.shape, o.dtype) for o in outs),
            in_specs=[hbm] * 4,
            out_specs=(vmem, vmem, vmem),
            scratch_shapes=[
                pltpu.VMEM((ROWS, HALF), BF16),
                pltpu.VMEM((NBLK // 2, HALF, 2 * BLK), BF16),
                pltpu.VMEM((NBLK, KC, BLK), F32),
                pltpu.VMEM((2, KC, GRP * BLK), BF16),
                pltpu.VMEM((PRE * Z, HALF), BF16),
                pltpu.VMEM((2, 2 * KC), F32),
                pltpu.SMEM((SWEEPS,), F32),
                pltpu.VMEM((KC, HALF), F32),
                pltpu.VMEM((KC, 128), F32),
                pltpu.VMEM((KC, HALF), F32),
                pltpu.VMEM((KC, HALF), BF16),
                pltpu.VMEM((KC, 128), F32),
                pltpu.VMEM((KC, 128), F32),
                pltpu.VMEM((NBLK, 1, BLK), F32),
                pltpu.VMEM((NBLK, 1, BLK), F32),
                pltpu.VMEM((1, ROWS), F32),
                pltpu.VMEM((2, NGRP, GRP, 1, BLK), F32),
                pltpu.VMEM((2, 3, NGRP, GRP, 1, BLK), F32),
                pltpu.VMEM((4, 1, KC), F32),
                pltpu.VMEM((1, SHARD), F32),
                pltpu.VMEM((1, SHARD), F32),
                dma((5,)),
                dma, dma((NCH + 1,)),
                dma, dma((NCH - 1,)),
                dma, dma((NCH,)),
                dma, dma((NOWN,)),
                dma, dma((2, NGRP)),
                dma, dma,
                dma, dma,
                dma, dma((NQ,)),
            ],
            compiler_params=pltpu.CompilerParams(
                collective_id=0, has_side_effects=True,
                vmem_limit_bytes=56 * 1024 * 1024),
        )(x_local, mu_init, logpi_init, inv_temp)
        return pl.pallas_call(
            write_out,
            out_shape=tuple(outs),
            in_specs=[vmem] * 3,
            out_specs=(hbm,) * 3,
            scratch_shapes=[dma((6,))],
        )(*[pltpu.with_memory_space_constraint(r, pltpu.VMEM) for r in res])

    return jax.shard_map(
        local_fit,
        mesh=mesh,
        in_specs=(P(("grp", "row"), None), P(None, ("grp", "comp"), None), P(None, ("grp", "comp")), P()),
        out_specs=(P(None, ("grp", "comp"), None), P(None, ("grp", "comp")), P(None, ("grp", "row"))),
        check_vma=False,
    )
```
